128 devices in a mesh: gx: 8 (over x, core), yz: 16 (over z, y).
Axes of the slice: x: 4, y: 4, z: 4, core: 2. Of those that a mesh axis runs over, the one named last changes fastest.
Arguments:
- pressure: bfloat16 [32768, 4096], P(('gx', 'yz')), may hold values from -6 to 6
- face_block: int32 [524288], P(('gx', 'yz')), may hold values from 0 to 255
- stencil_local: int32 [32, 524288], P(None, ('gx', 'yz')), may hold values from 0 to 4095
- stencil_weight: float32 [32, 524288], P(None, ('gx', 'yz')), may hold values from 0 to 0.25
- area_normal: float32 [12, 524288], P(None, ('gx', 'yz')), may hold values from -6 to 6
- face_part: int32 [524288, 1], P(('gx', 'yz')), may hold values from 0 to 127; in each aligned block of 4096 rows (0 to 4095, 4096 to 8191, ...) at most 64 rows name the same one
- face_nodes: int32 [8, 524288], P(None, ('gx', 'yz')), may hold values from 0 to 1023
- stiffness: float32 [60, 60, 32768], P(None, None, ('gx', 'yz')), may hold values from -0.075 to 6, as said below
- connect: int32 [20, 32768], P(None, ('gx', 'yz')), may hold values from 0 to 1279
- halo_nodes: int32 [2, 16384], P(None, ('gx', 'yz')), may hold values from 0 to 1023
- node_mass: float32 [131072], P(('gx', 'yz')), may hold values from 24 to 160
- displacement: float32 [3, 131072], P(None, ('gx', 'yz')), may hold values from -6 to 6
- velocity: float32 [3, 131072], P(None, ('gx', 'yz')), may hold values from -3 to 3
Outputs:
- node_disp: float32 [3, 131072], P(None, ('gx', 'yz'))
- face_disp: float32 [12, 524288], P(None, ('gx', 'yz'))
The draws below stay inside these ranges and needn't reach their ends.
Inputs may be any that keep to these rules, and one draw needn't show every extreme that they name: `face_part`: the faces of one device name no partition more than 64 times; in every draw some device names some partition exactly 64 times. `connect`: local node l of a partition: l < 1024 is owned, 1024 + g is entry g of the previous partition's row 1, 1152 + g entry g of the next partition's row 0 (along gx+yz). `halo_nodes`: each partition's 128 entries of row 0 are owned nodes held as ghosts by the previous partition, row 1 by the next; entries may repeat. `stiffness`: each element's matrix is symmetric positive definite.
All inputs are finite; a program needn't handle non-finite values.
Results may differ from the reference program's by a relative error of at most 0.0003.
Values sent between devices are 32-bit elements; how exact they have to be, the bound alone decides.
A program may use at most 256 MiB of HBM per device.

```python
import math
import jax
import jax.numpy as jnp
import numpy as np
from jax import lax

BLK_DEV = 256
BLOCK = 4096
FACE_DEV = 4096
ELEM_DEV = 256
SUBSTEPS = 4
NODE_DEV = 1024
GHOST = 128
CAP = 64
BLOCKS = 32768
FACES = 524288
ELEMS = 32768
NODES = 131072
GHOSTS = 16384
N_GX = 8
N_YZ = 16


def draw_stiffness(key, part):
    raw_entries = jax.random.uniform(key, (60, 60, ELEMS), jnp.float32, -0.05, 0.05)
    symmetric = 0.5 * (raw_entries + jnp.transpose(raw_entries, (1, 0, 2)))
    diag_mask = jnp.eye(60, dtype=jnp.float32)[:, :, None]
    off_part = symmetric * (1.0 - diag_mask)
    diagonal = 1.25 * jnp.sum(jnp.abs(off_part), axis=1) + 0.25
    matrix = off_part + diag_mask * diagonal[:, None, :]
    return matrix


def plant(values, stream_key, low, high):
    dims = values.shape
    index_at = [jax.random.randint(jax.random.fold_in(stream_key, axis), (), 0, dims[axis]) for axis in range(len(dims))]
    values = values.at[tuple(index_at)].set(low)
    longest = dims.index(max(dims))
    index_at[longest] = (index_at[longest] + 1) % dims[longest]
    return values.at[tuple(index_at)].set(high)


def shard_levels(stream_key, dims, pieces, low, largest):
    loudness, own = 1.0, jax.random.fold_in(stream_key, 6)
    for axis_at, shards_of in pieces:
        steps = jnp.exp(jax.random.uniform(jax.random.fold_in(own, axis_at), (shards_of,), jnp.float32, low / len(pieces), largest / len(pieces)))
        loudness = loudness * jnp.repeat(steps, dims[axis_at] // shards_of).reshape([-1 if axis == axis_at else 1 for axis in range(len(dims))])
    return loudness


def routed_block(stream_key, own, number, rows, amount, top, reach, skew):
    sequence = jax.random.permutation(stream_key, amount)
    heavy_load, common = shares(amount, rows * top, reach, skew, True), shares(amount, rows * top, reach, skew, False)
    places = jnp.arange(amount)

    def named(tallies, turn):
        used = int((tallies > 0).sum())
        fixed = max(1, used // 4)
        passed = fixed + (places - fixed + turn * (used - fixed)) % max(1, amount - fixed)
        return jnp.zeros((amount,), jnp.int32).at[sequence[jnp.where(places < fixed, places, passed)]].set(jnp.asarray(tallies, jnp.int32))

    tallies = jnp.where(number % 4 == 0, named(heavy_load, number // 4), named(common, number - number // 4 - 1))
    mixed = jax.random.permutation(jax.random.fold_in(own, 3), amount)
    giver, sink = mixed[0:amount // 2 * 2:2], mixed[1:amount // 2 * 2:2]
    slack = jnp.minimum(tallies[giver] - 1, reach - tallies[sink]) // 2
    slack = jnp.where((giver == sequence[0]) | (sink == sequence[0]) | (tallies[sink] == 0), 0, jnp.maximum(slack, 0))
    passed = jax.random.randint(jax.random.fold_in(own, 4), (amount // 2,), 0, 1 << 20) % (slack + 1)
    tallies = tallies.at[giver].add(-passed).at[sink].add(passed)
    labels = jnp.searchsorted(jnp.cumsum(tallies), jnp.arange(rows * top), side="right").astype(jnp.int32)
    table = labels.reshape(top, rows).T
    table = table[jax.random.permutation(jax.random.fold_in(own, 1), rows)]
    turn = jax.random.randint(jax.random.fold_in(own, 2), (rows, 1), 0, top)
    return jnp.take_along_axis(table, (jnp.arange(top)[None, :] + turn) % top, axis=1)


def shares(number_of, total, most, skew, full):
    loads = [(1 << 20) // math.isqrt(rank ** skew) + 1 for rank in range(1, number_of + 1)]
    largest = most if full else min(most, max(-(-total // number_of), total * loads[0] // sum(loads)))
    least = 1 if total - largest >= number_of - 1 else 0
    given, spare = [largest] + [least] * (number_of - 1), total - largest - least * (number_of - 1)
    while spare > 0:
        candidates = [i for i in range(1, number_of) if given[i] < largest] or [i for i in range(1, number_of) if given[i] < most]
        whole, left = sum([loads[i] for i in candidates]), spare
        for i in candidates:
            extra = min(most - given[i], max(1, left * loads[i] // whole), spare)
            given[i] = given[i] + extra
            spare = spare - extra
    return np.array(given)


def centred(key, extent, width, reach, pieces=(), kind=jnp.bfloat16):
    loudness = shard_levels(key, extent, pieces, -0.22, 0.18) if pieces else 1.0
    values = jax.random.normal(key, extent, jnp.float32) * width * loudness
    return jnp.minimum(jnp.maximum(values, -reach), reach).astype(kind)


def setup_inputs(seed: int = 0) -> dict:
    streams_of = jax.random.split(jax.random.key(seed), 14)
    pressure = centred(streams_of[0], (BLOCKS, BLOCK), 1.0, 6.0, ((0, 128),))
    face_block = plant(jax.random.randint(streams_of[1], (FACES,), 0, BLK_DEV), jax.random.fold_in(streams_of[1], 1), 0, BLK_DEV - 1).astype(jnp.int32)
    stencil_local = plant(jax.random.randint(streams_of[2], (32, FACES), 0, BLOCK), jax.random.fold_in(streams_of[2], 1), 0, BLOCK - 1).astype(jnp.int32)
    stencil_weight = jnp.clip(0.25 * jax.random.uniform(streams_of[3], (32, FACES), jnp.float32) ** shard_levels(streams_of[3], (32, FACES), ((1, 128),), -0.2, 0.2), 0.0, 0.25)
    area_normal = centred(streams_of[4], (12, FACES), 1.0, 6.0, ((1, 128),), jnp.float32)
    face_part_keys = jax.random.split(jax.random.fold_in(streams_of[5], 1), FACES // FACE_DEV)
    face_part_turns = jax.random.permutation(jax.random.fold_in(streams_of[5], 3), FACES // FACE_DEV)
    face_part = jax.vmap(lambda own, number: routed_block(jax.random.fold_in(streams_of[5], 2), own, number, FACE_DEV, N_GX * N_YZ, 1, CAP, 2))(face_part_keys, face_part_turns).reshape((FACES, 1))
    face_nodes = plant(jax.random.randint(streams_of[6], (8, FACES), 0, NODE_DEV), jax.random.fold_in(streams_of[6], 1), 0, NODE_DEV - 1).astype(jnp.int32)
    stiffness = draw_stiffness(jax.random.fold_in(streams_of[13], 71), 0)
    connect = plant(jax.random.randint(streams_of[8], (20, ELEMS), 0, NODE_DEV + 2 * GHOST), jax.random.fold_in(streams_of[8], 1), 0, (NODE_DEV + 2 * GHOST) - 1).astype(jnp.int32)
    halo_nodes = plant(jax.random.randint(streams_of[9], (2, GHOSTS), 0, NODE_DEV), jax.random.fold_in(streams_of[9], 1), 0, NODE_DEV - 1).astype(jnp.int32)
    node_mass = jnp.clip(jnp.exp(math.log(160.0) - 1.89712 * jax.random.uniform(streams_of[10], (NODES,), jnp.float32) ** shard_levels(streams_of[10], (NODES,), ((0, 128),), -0.2, 0.2)), 24.0, 160.0)
    displacement = centred(streams_of[11], (3, NODES), 1.0, 6.0, ((1, 128),), jnp.float32)
    velocity = centred(streams_of[12], (3, NODES), 0.5, 3.0, ((1, 128),), jnp.float32)
    return dict(pressure=pressure, face_block=face_block, stencil_local=stencil_local, stencil_weight=stencil_weight, area_normal=area_normal, face_part=face_part, face_nodes=face_nodes, stiffness=stiffness, connect=connect, halo_nodes=halo_nodes, node_mass=node_mass, displacement=displacement, velocity=velocity)


def shape_table():
    corner_u = [-1, 1, 1, -1, 0, 1, 0, -1]
    corner_v = [-1, -1, 1, 1, -1, 0, 1, 0]
    gauss_point = 1.0 / math.sqrt(3.0)
    points = [(-gauss_point, -gauss_point), (gauss_point, -gauss_point), (gauss_point, gauss_point), (-gauss_point, gauss_point)]
    shape_values = np.zeros((4, 8), np.float32)
    for position, (coord_u, coord_v) in enumerate(points):
        for corner in range(8):
            node_u = corner_u[corner]
            node_v = corner_v[corner]
            if corner < 4:
                entry_value = 0.25 * (1 + coord_u * node_u) * (1 + coord_v * node_v) * (coord_u * node_u + coord_v * node_v - 1)
            elif node_u == 0:
                entry_value = 0.5 * (1 - coord_u * coord_u) * (1 + coord_v * node_v)
            else:
                entry_value = 0.5 * (1 + coord_u * node_u) * (1 - coord_v * coord_v)
            shape_values[position, corner] = entry_value
    return shape_values

def reference(pressure, face_block, stencil_local, stencil_weight, area_normal, face_part, face_nodes, stiffness, connect, halo_nodes, node_mass, displacement, velocity):
    highest = lax.Precision.HIGHEST
    devices = N_GX * N_YZ
    shapes = jnp.asarray(shape_table(), dtype=jnp.float32)
    faces = FACE_DEV * devices
    owner = jnp.arange(faces, dtype=jnp.int32) // FACE_DEV
    block_index = owner * BLK_DEV + face_block
    cell_index = block_index[None, :] * BLOCK + stencil_local
    cell_values = pressure.reshape(-1)[cell_index].astype(jnp.float32)
    face_pressure = lax.optimization_barrier(jnp.sum((stencil_weight * cell_values).reshape(4, 8, faces), axis=1))
    traction = -(area_normal.reshape(3, 4, faces) * face_pressure[None])
    face_global = face_part[:, 0][None, :] * NODE_DEV + face_nodes
    total_nodes = NODE_DEV * devices
    load = jnp.einsum('qa,cqf->caf', shapes, traction, precision=highest)
    external = jnp.zeros((3, total_nodes), jnp.float32).at[:, face_global.reshape(-1)].add(load.reshape(3, -1))
    span = NODE_DEV + 2 * GHOST
    device_ids = jnp.arange(devices, dtype=jnp.int32)[:, None]
    owned = device_ids * NODE_DEV + jnp.arange(NODE_DEV, dtype=jnp.int32)[None, :]
    halo_grid = halo_nodes.reshape(2, devices, GHOST)
    from_prev = jnp.where(device_ids >= 1, (device_ids - 1) * NODE_DEV + jnp.roll(halo_grid[1], 1, axis=0), total_nodes).astype(jnp.int32)
    from_next = jnp.where(device_ids < devices - 1, (device_ids + 1) * NODE_DEV + jnp.roll(halo_grid[0], -1, axis=0), total_nodes).astype(jnp.int32)
    local_global = jnp.concatenate([owned, from_prev, from_next], axis=1).reshape(-1)
    elem_owner = jnp.arange(ELEM_DEV * devices, dtype=jnp.int32) // ELEM_DEV
    element_global = local_global[elem_owner[None, :] * span + connect]
    flat_index = element_global.reshape(-1)
    node_disp = displacement
    node_vel = velocity
    for substep in range(SUBSTEPS):
        padded = jnp.concatenate([node_disp, jnp.zeros((3, 1), jnp.float32)], axis=1)
        element_disp = padded[:, element_global].reshape(60, -1)
        element_force = lax.map(lambda stiff_row: lax.optimization_barrier(jnp.sum(stiff_row * element_disp, axis=0)), stiffness)
        internal = jnp.zeros((3, total_nodes + 1), jnp.float32).at[:, flat_index].add(element_force.reshape(3, -1))[:, :total_nodes]
        node_vel = node_vel + (external - internal) / node_mass[None, :]
        node_disp = node_disp + node_vel
    gathered = node_disp[:, face_global]
    face_disp = jnp.einsum('qa,caf->cqf', shapes, gathered, precision=highest).reshape(12, faces)
    return (node_disp, face_disp)
```

```python
import math

import jax
import jax.numpy as jnp
import numpy as np
from jax import lax
from jax.experimental import pallas as pl
from jax.experimental.pallas import tpu as pltpu
from jax.sharding import PartitionSpec as P

SUBSTEPS = 4
STRIDE = 40

def lane_take(x, idx):
    return jnp.take_along_axis(x, idx, axis=1, mode="promise_in_bounds")

def stencil_kernel(fb_ref, pr_ref, loc_ref, w_ref, an_ref, out_ref, tab, idxt, wt, res):
    def relayout(b, _):
        r0 = pl.multiple_of(b * 16, 16)
        for t in range(32):
            x = pr_ref[pl.ds(r0, 16), 128 * t:128 * t + 128].astype(jnp.float32)
            tab[pl.ds(r0 * STRIDE + t, 8, stride=STRIDE), :] = x[:8]
            tab[pl.ds((r0 + 8) * STRIDE + t, 8, stride=STRIDE), :] = x[8:]
        return 0
    lax.fori_loop(0, 16, relayout, 0)
    for i in range(8):
        idxt[128 * i:128 * i + 128, :] = jnp.concatenate(
            [loc_ref[:, a * 1024 + 128 * i:a * 1024 + 128 * i + 128] for a in range(4)], axis=0).T
        wt[128 * i:128 * i + 128, :] = jnp.concatenate(
            [w_ref[:, a * 1024 + 128 * i:a * 1024 + 128 * i + 128] for a in range(4)], axis=0).T
    lane = lax.broadcasted_iota(jnp.int32, (8, 128), 1)
    sub = lax.broadcasted_iota(jnp.int32, (8, 128), 0)
    grp = lane // 32
    m_lo = grp < 2
    m0 = grp == 0
    m2 = grp == 2

    def main(gg, _):
        base = pl.multiple_of(gg * 8, 8)
        rows = []
        for u in range(8):
            g = base + u
            idx = jnp.broadcast_to(idxt[pl.ds(g, 1), :], (8, 128))
            lo = idx & 127
            hi = idx >> 7
            j = hi >> 3
            c0 = j == 0
            c2 = j == 2
            cl = j < 2
            xs = []
            for a in range(4):
                b = fb_ref[a * 1024 + g]
                off = pl.multiple_of(b * STRIDE, 8)
                gs = [lane_take(tab[pl.ds(off + 8 * v, 8), :], lo) for v in range(4)]
                xs.append(jnp.where(cl, jnp.where(c0, gs[0], gs[1]), jnp.where(c2, gs[2], gs[3])))
            x = jnp.where(m_lo, jnp.where(m0, xs[0], xs[1]), jnp.where(m2, xs[2], xs[3]))
            x = jnp.where((hi & 7) == sub, x, 0.0)
            rows.append(jnp.sum(x, axis=0, keepdims=True))
        res[pl.ds(base, 8), :] = jnp.concatenate(rows, axis=0) * wt[pl.ds(base, 8), :]
        return 0
    lax.fori_loop(0, 128, main, 0)
    for i in range(8):
        rt = res[128 * i:128 * i + 128, :].T
        for a in range(4):
            f0 = a * 1024 + 128 * i
            fp = jnp.concatenate([jnp.sum(rt[a * 32 + 8 * q:a * 32 + 8 * q + 8], axis=0, keepdims=True) for q in range(4)], axis=0)
            fp3 = jnp.concatenate([fp, fp, fp], axis=0)
            out_ref[:, f0:f0 + 128] = -(an_ref[:, f0:f0 + 128] * fp3)

def stencil(face_block, pressure, local, weight, area):
    V = pl.BlockSpec(memory_space=pltpu.VMEM)
    return pl.pallas_call(
        stencil_kernel,
        out_shape=jax.ShapeDtypeStruct((12, 4096), jnp.float32),
        in_specs=[pl.BlockSpec(memory_space=pltpu.SMEM), V, V, V, V],
        out_specs=V,
        scratch_shapes=[pltpu.VMEM((256 * STRIDE, 128), jnp.float32), pltpu.VMEM((1024, 128), jnp.int32),
                        pltpu.VMEM((1024, 128), jnp.float32), pltpu.VMEM((1024, 128), jnp.float32)],
        compiler_params=pltpu.CompilerParams(vmem_limit_bytes=40 * 2**20),
        name="stencil",
    )(face_block, pressure, local, weight, area)


def in_one_piece(arrays, axis, split_dim, concat_dim, along):
    both = jnp.concatenate(arrays, axis=along)
    whole, at, done = (
        lax.all_to_all(both, axis, split_axis=split_dim, concat_axis=concat_dim, tiled=True),
        0,
        [],
    )
    for a in arrays:
        done.append(lax.slice_in_dim(whole, at, at + a.shape[along], axis=along))
        at += a.shape[along]
    return tuple(done)


def with_halo(value, sides, width):
    edges = {}
    for axis, dim in sides:
        peers, length = (lax.axis_size(axis), value.shape[dim])
        up = [(i, (i + 1) % peers) for i in range(peers - 1)]
        last = lax.slice_in_dim(value, length - width, length, axis=dim)
        first = lax.slice_in_dim(value, 0, width, axis=dim)
        edges[dim] = (
            lax.ppermute(last, axis, up),
            lax.ppermute(first, axis, [(b, a) for a, b in up]),
        )
    done = []
    for _, dim in sides:
        low, high = edges[dim]
        around = [(width, width) if d in done else (0, 0) for d in range(value.ndim)]
        value = jnp.concatenate([jnp.pad(low, around), value, jnp.pad(high, around)], axis=dim)
        done.append(dim)
    return value


def with_halo_2(cells, sides, width):
    for axis, dim in sides:
        count = lax.axis_size(axis)
        ends = count - 1
        head = lax.slice_in_dim(cells, 0, width, axis=dim)
        tail = lax.slice_in_dim(cells, cells.shape[dim] - width, cells.shape[dim], axis=dim)
        cells = jnp.concatenate(
            [
                lax.ppermute(tail, axis, [(i, (i + 1) % count) for i in range(ends)]),
                cells,
                lax.ppermute(head, axis, [((i + 1) % count, i) for i in range(ends)]),
            ],
            axis=dim,
        )
    return cells


def shape_table():
    corner_u = [-1, 1, 1, -1, 0, 1, 0, -1]
    corner_v = [-1, -1, 1, 1, -1, 0, 1, 0]
    gauss_point = 1.0 / math.sqrt(3.0)
    points = [
        (-gauss_point, -gauss_point),
        (gauss_point, -gauss_point),
        (gauss_point, gauss_point),
        (-gauss_point, gauss_point),
    ]
    shape_values = np.zeros((4, 8), np.float32)
    for position, (coord_u, coord_v) in enumerate(points):
        for corner in range(8):
            node_u = corner_u[corner]
            node_v = corner_v[corner]
            if corner < 4:
                entry_value = (
                    0.25
                    * (1 + coord_u * node_u)
                    * (1 + coord_v * node_v)
                    * (coord_u * node_u + coord_v * node_v - 1)
                )
            elif node_u == 0:
                entry_value = 0.5 * (1 - coord_u * coord_u) * (1 + coord_v * node_v)
            else:
                entry_value = 0.5 * (1 + coord_u * node_u) * (1 - coord_v * coord_v)
            shape_values[position, corner] = entry_value
    return shape_values


def hot_pair(indices, extent):
    lanes_width = 32
    upper_count = -(-extent // lanes_width)
    upper_hot = (
        indices[None, :] // lanes_width == lax.broadcasted_iota(jnp.int32, (upper_count, 1), 0)
    ).astype(jnp.float32)
    lower_hot = (
        indices[None, :] % lanes_width == lax.broadcasted_iota(jnp.int32, (lanes_width, 1), 0)
    ).astype(jnp.float32)
    return (upper_hot, lower_hot)


def pick_cols(table, hots):
    upper_hot, lower_hot = hots
    lanes_width = lower_hot.shape[0]
    upper_count = upper_hot.shape[0]
    comps, extent = table.shape
    grid = (
        table.reshape(comps, upper_count, lanes_width)
        .transpose(1, 0, 2)
        .reshape(upper_count, comps * lanes_width)
    )
    rows_out = lax.dot_general(
        grid,
        upper_hot,
        (((0,), (0,)), ((), ())),
        precision=lax.Precision.HIGHEST,
        preferred_element_type=jnp.float32,
    )
    return jnp.sum(rows_out.reshape(comps, lanes_width, -1) * lower_hot[None], axis=1)


def spread_cols(values, hots):
    upper_hot, lower_hot = hots
    lanes_width = lower_hot.shape[0]
    upper_count = upper_hot.shape[0]
    comps = values.shape[0]
    masked = (values[:, None, :] * lower_hot[None]).reshape(comps * lanes_width, -1)
    summed = lax.dot_general(
        masked,
        upper_hot,
        (((1,), (1,)), ((), ())),
        precision=lax.Precision.HIGHEST,
        preferred_element_type=jnp.float32,
    )
    return (
        summed.reshape(comps, lanes_width, upper_count)
        .transpose(0, 2, 1)
        .reshape(comps, upper_count * lanes_width)
    )


def arrival_order(target, devices):
    row_count = target.shape[0]
    group_rows = min(512, row_count)
    groups = row_count // group_rows
    onehot = (target[:, None] == jnp.arange(devices, dtype=jnp.int32)[None, :]).astype(jnp.bfloat16)
    onehot = onehot.reshape(groups, group_rows, devices)
    lower_ones = (
        lax.broadcasted_iota(jnp.int32, (group_rows, group_rows), 0)
        > lax.broadcasted_iota(jnp.int32, (group_rows, group_rows), 1)
    ).astype(jnp.bfloat16)
    before = jnp.einsum("ij,gjd->gid", lower_ones, onehot, preferred_element_type=jnp.float32)
    onehot_float = onehot.astype(jnp.float32)
    totals = jnp.sum(onehot_float, axis=1)
    offsets = jnp.cumsum(totals, axis=0) - totals
    placed = jnp.sum((before + offsets[:, None, :]) * onehot_float, axis=2)
    return placed.reshape(row_count).astype(jnp.int32)


def send_back(outgoing):
    returned = lax.all_to_all(outgoing, ("gx", "yz"), split_axis=1, concat_axis=1, tiled=True)
    return returned


def shards(
    pressure,
    face_block,
    stencil_local,
    stencil_weight,
    area_normal,
    face_part,
    face_nodes,
    stiffness,
    connect,
    halo_nodes,
    node_mass,
    displacement,
    velocity,
):
    highest = lax.Precision.HIGHEST
    gx_size = lax.axis_size("gx")
    yz_size = lax.axis_size("yz")
    devices = gx_size * yz_size
    shapes = jnp.asarray(shape_table(), dtype=jnp.float32)
    face_count = face_block.shape[0]
    capacity = max(2, 2 * face_count // devices)
    slot_total = devices * capacity
    traction = stencil(face_block, pressure, stencil_local, stencil_weight, area_normal)
    target = face_part[:, 0]
    slots = target * capacity + arrival_order(target, devices)
    slot_hots = hot_pair(slots, slot_total)
    packed = spread_cols(
        jnp.concatenate([traction, face_nodes.astype(jnp.float32)], axis=0), slot_hots
    )
    load_buffer = packed[:12].reshape(12, devices, capacity)
    node_buffer = packed[12:].reshape(8, devices, capacity)
    arrived_load, arrived_nodes = in_one_piece((load_buffer, node_buffer), ("gx", "yz"), 1, 1, 0)
    received = arrived_load.reshape(3, 4, slot_total)
    node_ids = arrived_nodes.reshape(8 * slot_total).astype(jnp.int32)
    owned_count = displacement.shape[1]
    ghost_count = halo_nodes.shape[1]
    span = owned_count + 2 * ghost_count
    node_hots = hot_pair(node_ids, owned_count)
    load = jnp.einsum("qa,cqs->cas", shapes, received, precision=highest)
    external = spread_cols(load.reshape(3, -1), node_hots)
    element_count = connect.shape[1]
    elem_hots = hot_pair(connect.reshape(-1), span)
    halo_hots = hot_pair(halo_nodes.reshape(-1), owned_count)
    node_disp = displacement
    node_vel = velocity
    for substep in range(SUBSTEPS):
        outgoing = pick_cols(node_disp, halo_hots).reshape(3, 2, ghost_count)
        bordered = with_halo(outgoing, ((("gx", "yz"), 1),), 1)
        local_disp = jnp.concatenate([node_disp, bordered[:, 0], bordered[:, 3]], axis=1)
        element_disp = pick_cols(local_disp, elem_hots).reshape(60, element_count)
        element_force = jnp.sum(stiffness * element_disp[None], axis=1)
        spread = spread_cols(element_force.reshape(3, -1), elem_hots)
        ghost_terms = jnp.stack(
            [
                spread[:, owned_count : owned_count + ghost_count],
                spread[:, owned_count + ghost_count :],
            ],
            axis=1,
        )
        arriving = with_halo_2(ghost_terms, ((("gx", "yz"), 1),), 1)
        incoming = jnp.concatenate([arriving[:, 0], arriving[:, 3]], axis=1)
        internal = spread[:, :owned_count] + spread_cols(incoming, halo_hots)
        node_vel = node_vel + (external - internal) / node_mass[None, :]
        node_disp = node_disp + node_vel
    at_nodes = pick_cols(node_disp, node_hots).reshape(3, 8, slot_total)
    at_points = jnp.einsum("qa,cas->cqs", shapes, at_nodes, precision=highest).reshape(
        12, devices, capacity
    )
    returned = send_back(at_points)
    face_disp = pick_cols(returned.reshape(12, slot_total), slot_hots)
    return (node_disp, face_disp)


def solution(mesh):
    in_specs = (
        P(("gx", "yz"), None),
        P(("gx", "yz")),
        P(None, ("gx", "yz")),
        P(None, ("gx", "yz")),
        P(None, ("gx", "yz")),
        P(("gx", "yz"), None),
        P(None, ("gx", "yz")),
        P(None, None, ("gx", "yz")),
        P(None, ("gx", "yz")),
        P(None, ("gx", "yz")),
        P(("gx", "yz")),
        P(None, ("gx", "yz")),
        P(None, ("gx", "yz")),
    )
    out_specs = (P(None, ("gx", "yz")), P(None, ("gx", "yz")))
    return jax.shard_map(shards, mesh=mesh, in_specs=in_specs, out_specs=out_specs, check_vma=False)
```

```python
import functools
import math

import jax
import jax.numpy as jnp
import numpy as np
from jax import lax
from jax.experimental import pallas as pl
from jax.experimental.pallas import tpu as pltpu
from jax.sharding import PartitionSpec as P

MESH = pl.DeviceIdType.MESH
F32 = jnp.float32
BF16 = jnp.bfloat16
SUBSTEPS = 4

def half_lanes(left, right):
    lane = lax.broadcasted_iota(jnp.int32, (8, 128), 1)
    return jnp.where(lane < 64, F32(left), F32(right))

def mix_weights(shapes):
    pick = lambda q, a: float(shapes[q, a])
    out = []
    for j in range(4):
        e, o = 2 * j, 2 * j + 1
        out.append((
            half_lanes(pick(0, e), pick(1, o)), half_lanes(pick(1, e), pick(0, o)),
            half_lanes(pick(2, e), pick(3, o)), half_lanes(pick(3, e), pick(2, o))))
    return out

def solid_kernel(nx, ny, shapes, s_ref, k_hbm, con_ref, halo_ref, mass_ref, disp_ref, vel_ref,
                 nd_ref, ret_ref,
                 recv, outb, kmat, ids, con_lo, con_hi, u_s, fh_s, fl_s, v_s, oh_e, oh_h, oh_x, v_x,
                 dsend, drecv, fsend, frecv,
                 k_sem, fs_sem, fr_sem, rs_sem, rr_sem, ds_sem, dr_sem, gs_sem, gr_sem):
    n = nx * ny
    gx = lax.axis_index("gx")
    yz = lax.axis_index("yz")
    me = gx * ny + yz
    dev = lambda t: (t // ny, lax.rem(t, ny))
    nxt = lax.rem(me + 1, n)
    prv = lax.rem(me + n - 1, n)
    kcopy = pltpu.make_async_copy(k_hbm, kmat, k_sem)
    kcopy.start()
    barrier = pltpu.get_barrier_semaphore()

    def greet(i, _):
        pl.semaphore_signal(barrier, inc=1, device_id=dev(lax.rem(me + i, n)), device_id_type=MESH)
        return 0
    lax.fori_loop(1, n, greet, 0)

    sub8 = lax.broadcasted_iota(jnp.int32, (8, 128), 0)
    sub128 = lax.broadcasted_iota(jnp.int32, (128, 128), 0)
    weights = mix_weights(shapes)

    con_lo[...] = con_ref[...] & 127
    con_hi[...] = con_ref[...] >> 7
    for a in range(20):
        for e in range(2):
            row = jnp.broadcast_to(con_lo[a:a + 1, 128 * e:128 * e + 128], (128, 128))
            oh_e[a * 256 + 128 * e:a * 256 + 128 * e + 128, :] = jnp.where(row == sub128, F32(1), F32(0)).T.astype(BF16)
    halo_lo = [jnp.broadcast_to(halo_ref[r:r + 1, :] & 127, (8, 128)) for r in range(2)]
    halo_hi = [jnp.broadcast_to(halo_ref[r:r + 1, :] >> 7, (8, 128)) for r in range(2)]
    for r in range(2):
        row = jnp.broadcast_to(halo_ref[r:r + 1, :] & 127, (128, 128))
        oh_h[128 * r:128 * r + 128, :] = jnp.where(row == sub128, F32(1), F32(0)).T.astype(BF16)
    stack = lambda ref, c: jnp.concatenate([ref[c:c + 1, 128 * h:128 * h + 128] for h in range(8)], axis=0)
    disp = [stack(disp_ref, c) for c in range(3)]
    vel = [stack(vel_ref, c) for c in range(3)]
    mass = stack(mass_ref, 0)

    pl.semaphore_wait(barrier, n - 1)

    def near(src, dst, ss, rs, t):
        return pltpu.make_async_remote_copy(src_ref=src, dst_ref=dst, send_sem=ss, recv_sem=rs, device_id=dev(t), device_id_type=MESH)

    def disp_copies(step):
        return [near(dsend.at[step, 1], drecv.at[step, 0], ds_sem.at[step, 1], dr_sem.at[step, 0], nxt),
                near(dsend.at[step, 0], drecv.at[step, 1], ds_sem.at[step, 0], dr_sem.at[step, 1], prv)]

    def force_copies(step):
        return [near(fsend.at[step, 0], frecv.at[step, 1], gs_sem.at[step, 0], gr_sem.at[step, 1], prv),
                near(fsend.at[step, 1], frecv.at[step, 0], gs_sem.at[step, 1], gr_sem.at[step, 0], nxt)]

    def send_disp(step, disp):
        for r in range(2):
            for c in range(3):
                g = jnp.where(halo_hi[r] == sub8, lane_take(disp[c], halo_lo[r]), F32(0))
                dsend[step, r, c:c + 1, :] = jnp.sum(g, axis=0, keepdims=True)
        for cp in disp_copies(step):
            cp.start()

    def internal(step, disp):
        cps = disp_copies(step)
        for cp in cps:
            cp.wait()
        ghost = [jnp.where(me > 0, drecv[step, 0, 0:3, :], F32(0)), jnp.where(me < n - 1, drecv[step, 1, 0:3, :], F32(0))]
        for c in range(3):
            rows = [disp[c][h:h + 1, :] for h in range(8)] + [ghost[0][c:c + 1, :], ghost[1][c:c + 1, :]]
            rows = [jnp.broadcast_to(r, (8, 128)) for r in rows]
            for at in range(3):
                for e in range(2):
                    lo = con_lo[8 * at:8 * at + 8, 128 * e:128 * e + 128]
                    hi = con_hi[8 * at:8 * at + 8, 128 * e:128 * e + 128]
                    acc = lane_take(rows[0], lo)
                    for h in range(1, 10):
                        acc = jnp.where(hi == h, lane_take(rows[h], lo), acc)
                    u_s[c, 8 * at:8 * at + 8, 128 * e:128 * e + 128] = acc

        def multiply(a, acc):
            for c in range(3):
                acc = acc + kmat[c * 20 + a] * u_s[c, pl.ds(a, 1), :]
            return acc
        force = lax.fori_loop(0, 20, multiply, jnp.zeros((60, 256), F32))
        fh = force.astype(BF16).astype(F32)
        fh_s[...] = fh
        fl_s[...] = force - fh
        sub16 = lax.broadcasted_iota(jnp.int32, (16, 256), 0)
        for a in range(20):
            mask = jnp.broadcast_to(con_hi[a:a + 1, :], (16, 256)) == sub16
            for c in range(3):
                for k, part in enumerate((fh_s, fl_s)):
                    row = jnp.broadcast_to(part[20 * c + a:20 * c + a + 1, :], (16, 256))
                    v_s[48 * k + 16 * c:48 * k + 16 * c + 16, a * 256:a * 256 + 256] = jnp.where(mask, row, F32(0)).astype(BF16)
        both = jnp.dot(v_s[...], oh_e[...], preferred_element_type=F32)
        total = both[:48] + both[48:]
        for k in range(2):
            for c in range(3):
                fsend[step, k, c:c + 1, :] = total[16 * c + 8 + k:16 * c + 9 + k, :]
        for cp in force_copies(step):
            cp.start()
        return [total[16 * c:16 * c + 8, :] for c in range(3)]

    def advance(step, own, ext, disp, vel):
        for cp in force_copies(step):
            cp.wait()
        got = [jnp.where(me > 0, frecv[step, 0, 0:3, :], F32(0)), jnp.where(me < n - 1, frecv[step, 1, 0:3, :], F32(0))]
        parts = []
        for c in range(3):
            cols = []
            for r in range(2):
                x = jnp.where(halo_hi[r] == sub8, jnp.broadcast_to(got[r][c:c + 1, :], (8, 128)), F32(0))
                cols.append(x)
            parts.append(jnp.concatenate(cols, axis=1))
        x = jnp.concatenate(parts, axis=0)
        xh = x.astype(BF16).astype(F32)
        lhs = jnp.concatenate([xh, x - xh], axis=0).astype(BF16)
        both = jnp.dot(lhs, oh_h[...], preferred_element_type=F32)
        add = both[:24] + both[24:]
        vel = [vel[c] + (ext[c] - (own[c] + add[8 * c:8 * c + 8, :])) / mass for c in range(3)]
        disp = [disp[c] + vel[c] for c in range(3)]
        return disp, vel

    send_disp(0, disp)

    def fwd(i):
        t = lax.rem(me + i, n)
        return near(s_ref.at[t], recv.at[me], fs_sem.at[i], fr_sem.at[i], t)

    def fwd_start(i, _):
        fwd(i).start()
        return 0
    lax.fori_loop(1, n, fwd_start, 0)
    recv[me] = s_ref[me]
    kcopy.wait()
    own = internal(0, disp)

    def fwd_wait(i, _):
        fwd(i).wait()
        return 0
    lax.fori_loop(1, n, fwd_wait, 0)

    sub128h = lax.broadcasted_iota(jnp.int32, (128, 128), 0).astype(jnp.int16)

    def gather_load(t, acc):
        base = pl.multiple_of(t * 8, 8)
        get = lambda r: recv[pl.ds(base, 8), r, :]
        loads = []
        for c in range(3):
            t0, t1 = get(2 * c), get(2 * c + 1)
            r0, r1 = pltpu.roll(t0, 64, 1), pltpu.roll(t1, 64, 1)
            loads.append([weights[j][0] * t0 + weights[j][1] * r0 + weights[j][2] * t1 + weights[j][3] * r1 for j in range(4)])
        for j in range(4):
            idx = get(6 + j).astype(jnp.int32)
            ids[j, pl.ds(base, 8), :] = idx
            lo, hi = idx & 127, idx >> 7
            highs = [loads[c][j].astype(BF16).astype(F32) for c in range(3)]
            lows = [loads[c][j] - highs[c] for c in range(3)]
            for s in range(8):
                at = (j * 8 + s) * 128
                row = jnp.broadcast_to(lo[s:s + 1, :], (128, 128)).astype(jnp.int16)
                oh_x[:, at:at + 128] = jnp.where(row == sub128h, BF16(1), BF16(0))
                mask = jnp.broadcast_to(hi[s:s + 1, :], (8, 128)) == sub8
                v_x[:, at:at + 128] = jnp.concatenate(
                    [jnp.where(mask, jnp.broadcast_to(p[s:s + 1, :], (8, 128)), F32(0)) for p in highs + lows], axis=0).astype(BF16)
        return acc + lax.dot_general(v_x[...], oh_x[...], (((1,), (1,)), ((), ())), preferred_element_type=F32)
    both = lax.fori_loop(0, n // 8, gather_load, jnp.zeros((48, 128), F32))
    ext = [both[8 * c:8 * c + 8] + both[24 + 8 * c:32 + 8 * c] for c in range(3)]

    disp, vel = advance(0, own, ext, disp, vel)
    for step in range(1, SUBSTEPS):
        send_disp(step, disp)
        own = internal(step, disp)
        disp, vel = advance(step, own, ext, disp, vel)
    for c in range(3):
        for h in range(8):
            nd_ref[c:c + 1, 128 * h:128 * h + 128] = disp[c][h:h + 1, :]
            u_s[c, h:h + 1, 0:128] = disp[c][h:h + 1, :]

    def back(t):
        base = pl.multiple_of(t * 8, 8)
        idx = [ids[j, pl.ds(base, 8), :] for j in range(4)]
        for c in range(3):
            p0 = p1 = q0 = q1 = jnp.zeros((8, 128), F32)
            for j in range(4):
                lo, hi = idx[j] & 127, idx[j] >> 7
                acc = lane_take(jnp.broadcast_to(u_s[c, 0:1, 0:128], (8, 128)), lo)
                for h in range(1, 8):
                    acc = jnp.where(hi == h, lane_take(jnp.broadcast_to(u_s[c, h:h + 1, 0:128], (8, 128)), lo), acc)
                p0 = p0 + weights[j][0] * acc
                q0 = q0 + weights[j][1] * acc
                p1 = p1 + weights[j][2] * acc
                q1 = q1 + weights[j][3] * acc
            outb[pl.ds(base, 8), 2 * c, :] = p0 + pltpu.roll(q0, 64, 1)
            outb[pl.ds(base, 8), 2 * c + 1, :] = p1 + pltpu.roll(q1, 64, 1)

    def back_loop(t, _):
        back(t)
        return 0
    lax.fori_loop(0, n // 8, back_loop, 0)

    def ret(i):
        t = lax.rem(me + i, n)
        return near(outb.at[t], ret_ref.at[me], rs_sem.at[i], rr_sem.at[i], t)

    def ret_start(i, _):
        ret(i).start()
        return 0
    lax.fori_loop(1, n, ret_start, 0)
    ret_ref[me] = outb[me]

    def ret_wait(i, _):
        ret(i).wait()
        return 0
    lax.fori_loop(1, n, ret_wait, 0)


def solid(send, stiffness, connect, halo, mass, disp, vel, nx, ny, shapes):
    n = nx * ny
    V = pl.BlockSpec(memory_space=pltpu.VMEM)
    A = pl.BlockSpec(memory_space=pl.ANY)
    D = pltpu.SemaphoreType.DMA
    connect = jnp.pad(connect, ((0, 4), (0, 0)))
    return pl.pallas_call(
        functools.partial(solid_kernel, nx, ny, shapes),
        out_shape=(jax.ShapeDtypeStruct(disp.shape, F32), jax.ShapeDtypeStruct((n, 6, 128), F32)),
        in_specs=[V, A, V, V, V, V, V],
        out_specs=(V, V),
        scratch_shapes=[
            pltpu.VMEM((n, 10, 128), F32), pltpu.VMEM((n, 6, 128), F32), pltpu.VMEM((60, 60, 256), F32),
            pltpu.VMEM((4, n, 128), jnp.int32), pltpu.VMEM((24, 256), jnp.int32), pltpu.VMEM((24, 256), jnp.int32),
            pltpu.VMEM((3, 24, 256), F32), pltpu.VMEM((60, 256), F32), pltpu.VMEM((60, 256), F32),
            pltpu.VMEM((96, 5120), BF16), pltpu.VMEM((5120, 128), BF16), pltpu.VMEM((256, 128), BF16),
            pltpu.VMEM((128, 4096), BF16), pltpu.VMEM((48, 4096), BF16),
            pltpu.VMEM((SUBSTEPS, 2, 8, 128), F32), pltpu.VMEM((SUBSTEPS, 2, 8, 128), F32),
            pltpu.VMEM((SUBSTEPS, 2, 8, 128), F32), pltpu.VMEM((SUBSTEPS, 2, 8, 128), F32),
            D, D((n,)), D((n,)), D((n,)), D((n,)), D((SUBSTEPS, 2)), D((SUBSTEPS, 2)), D((SUBSTEPS, 2)), D((SUBSTEPS, 2))],
        compiler_params=pltpu.CompilerParams(collective_id=0, has_side_effects=True, vmem_limit_bytes=48 * 2**20),
        name="solid",
    )(send, stiffness, connect, halo, mass.reshape(1, -1), disp, vel)


STRIDE = 40
UNR = 32
TAKE = lax.GatherDimensionNumbers(
    offset_dims=(), collapsed_slice_dims=(1,), start_index_map=(1,), operand_batching_dims=(0,), start_indices_batching_dims=(0,)
)

def lane_take(x, idx):
    return lax.gather(x, idx[..., None], TAKE, slice_sizes=(1, 1), mode=lax.GatherScatterMode.PROMISE_IN_BOUNDS)

def stencil_kernel(fb_ref, pr_ref, loc_ref, w_ref, an_ref, out_ref, tab32, tab, idxt, wt, res):
    def relayout(b, _):
        r0 = pl.multiple_of(b * 16, 16)
        for t in range(32):
            x = pr_ref[pl.ds(r0, 16), 128 * t:128 * t + 128].astype(jnp.float32)
            tab32[pl.ds(t, 8, stride=STRIDE), :] = x[:8]
            tab32[pl.ds(8 * STRIDE + t, 8, stride=STRIDE), :] = x[8:]
        for n in range(16):
            tab[pl.ds(pl.multiple_of((r0 + n) * 32, 32), 32), :] = tab32[n * STRIDE:n * STRIDE + 32, :].astype(jnp.bfloat16)
        return 0
    lax.fori_loop(0, 16, relayout, 0)
    for i in range(8):
        idxt[128 * i:128 * i + 128, :] = jnp.concatenate(
            [loc_ref[:, a * 1024 + 128 * i:a * 1024 + 128 * i + 128] for a in range(4)], axis=0).T
        wt[128 * i:128 * i + 128, :] = jnp.concatenate(
            [w_ref[:, a * 1024 + 128 * i:a * 1024 + 128 * i + 128] for a in range(4)], axis=0).T
    lane = lax.broadcasted_iota(jnp.int32, (16, 128), 1)
    sub = lax.broadcasted_iota(jnp.int32, (16, 128), 0).astype(jnp.int16)
    grp = (lane // 32).astype(jnp.int16)
    m_lo = grp < 2
    m0 = grp == 0
    m2 = grp == 2

    def main(gg, _):
        for uu in range(UNR // 8):
            base = pl.multiple_of(gg * UNR + 8 * uu, 8)
            rows = []
            for u in range(8):
                g = base + u
                row = jnp.broadcast_to(idxt[pl.ds(g, 1), :], (16, 128))
                lo = (row & 127).astype(jnp.int16)
                hi = (row >> 7).astype(jnp.int16)
                cl = hi < 16
                mine = (hi & 15) == sub
                xs = []
                for a in range(4):
                    off = pl.multiple_of(fb_ref[a * 1024 + g] * 32, 32)
                    xs.append(jnp.where(cl, lane_take(tab[pl.ds(off, 16), :], lo), lane_take(tab[pl.ds(off + 16, 16), :], lo)))
                x = jnp.where(m_lo, jnp.where(m0, xs[0], xs[1]), jnp.where(m2, xs[2], xs[3]))
                x = jnp.where(mine, x, jnp.bfloat16(0)).astype(jnp.float32)
                rows.append(jnp.sum(x[:8] + x[8:], axis=0, keepdims=True))
            res[pl.ds(base, 8), :] = jnp.concatenate(rows, axis=0) * wt[pl.ds(base, 8), :]
        return 0
    lax.fori_loop(0, 1024 // UNR, main, 0)
    for i in range(8):
        rt = res[128 * i:128 * i + 128, :].T
        for a in range(4):
            f0 = a * 1024 + 128 * i
            fp = jnp.concatenate([jnp.sum(rt[a * 32 + 8 * q:a * 32 + 8 * q + 8], axis=0, keepdims=True) for q in range(4)], axis=0)
            fp3 = jnp.concatenate([fp, fp, fp], axis=0)
            out_ref[:, f0:f0 + 128] = -(an_ref[:, f0:f0 + 128] * fp3)

def stencil(face_block, pressure, local, weight, area):
    V = pl.BlockSpec(memory_space=pltpu.VMEM)
    return pl.pallas_call(
        stencil_kernel,
        out_shape=jax.ShapeDtypeStruct((12, 4096), jnp.float32),
        in_specs=[pl.BlockSpec(memory_space=pltpu.SMEM), V, V, V, V],
        out_specs=V,
        scratch_shapes=[pltpu.VMEM((16 * STRIDE, 128), jnp.float32), pltpu.VMEM((8192, 128), jnp.bfloat16), pltpu.VMEM((1024, 128), jnp.int32),
                        pltpu.VMEM((1024, 128), jnp.float32), pltpu.VMEM((1024, 128), jnp.float32)],
        compiler_params=pltpu.CompilerParams(vmem_limit_bytes=40 * 2**20),
        name="stencil",
    )(face_block, pressure, local, weight, area)


def shape_table():
    corner_u = [-1, 1, 1, -1, 0, 1, 0, -1]
    corner_v = [-1, -1, 1, 1, -1, 0, 1, 0]
    gauss_point = 1.0 / math.sqrt(3.0)
    points = [
        (-gauss_point, -gauss_point),
        (gauss_point, -gauss_point),
        (gauss_point, gauss_point),
        (-gauss_point, gauss_point),
    ]
    shape_values = np.zeros((4, 8), np.float32)
    for position, (coord_u, coord_v) in enumerate(points):
        for corner in range(8):
            node_u = corner_u[corner]
            node_v = corner_v[corner]
            if corner < 4:
                entry_value = (
                    0.25
                    * (1 + coord_u * node_u)
                    * (1 + coord_v * node_v)
                    * (coord_u * node_u + coord_v * node_v - 1)
                )
            elif node_u == 0:
                entry_value = 0.5 * (1 - coord_u * coord_u) * (1 + coord_v * node_v)
            else:
                entry_value = 0.5 * (1 + coord_u * node_u) * (1 - coord_v * coord_v)
            shape_values[position, corner] = entry_value
    return shape_values


def hot_pair(indices, extent):
    lanes_width = 32
    upper_count = -(-extent // lanes_width)
    upper_hot = (
        indices[None, :] // lanes_width == lax.broadcasted_iota(jnp.int32, (upper_count, 1), 0)
    ).astype(jnp.float32)
    lower_hot = (
        indices[None, :] % lanes_width == lax.broadcasted_iota(jnp.int32, (lanes_width, 1), 0)
    ).astype(jnp.float32)
    return (upper_hot, lower_hot)


def pick_cols(table, hots):
    upper_hot, lower_hot = hots
    lanes_width = lower_hot.shape[0]
    upper_count = upper_hot.shape[0]
    comps, extent = table.shape
    grid = (
        table.reshape(comps, upper_count, lanes_width)
        .transpose(1, 0, 2)
        .reshape(upper_count, comps * lanes_width)
    )
    rows_out = lax.dot_general(
        grid,
        upper_hot,
        (((0,), (0,)), ((), ())),
        precision=lax.Precision.HIGHEST,
        preferred_element_type=jnp.float32,
    )
    return jnp.sum(rows_out.reshape(comps, lanes_width, -1) * lower_hot[None], axis=1)


def spread_cols(values, hots):
    upper_hot, lower_hot = hots
    lanes_width = lower_hot.shape[0]
    upper_count = upper_hot.shape[0]
    comps = values.shape[0]
    masked = (values[:, None, :] * lower_hot[None]).reshape(comps * lanes_width, -1)
    summed = lax.dot_general(
        masked,
        upper_hot,
        (((1,), (1,)), ((), ())),
        precision=lax.Precision.HIGHEST,
        preferred_element_type=jnp.float32,
    )
    return (
        summed.reshape(comps, lanes_width, upper_count)
        .transpose(0, 2, 1)
        .reshape(comps, upper_count * lanes_width)
    )


def arrival_order(target, devices):
    row_count = target.shape[0]
    group_rows = min(512, row_count)
    groups = row_count // group_rows
    onehot = (target[:, None] == jnp.arange(devices, dtype=jnp.int32)[None, :]).astype(jnp.bfloat16)
    onehot = onehot.reshape(groups, group_rows, devices)
    lower_ones = (
        lax.broadcasted_iota(jnp.int32, (group_rows, group_rows), 0)
        > lax.broadcasted_iota(jnp.int32, (group_rows, group_rows), 1)
    ).astype(jnp.bfloat16)
    before = jnp.einsum("ij,gjd->gid", lower_ones, onehot, preferred_element_type=jnp.float32)
    onehot_float = onehot.astype(jnp.float32)
    totals = jnp.sum(onehot_float, axis=1)
    offsets = jnp.cumsum(totals, axis=0) - totals
    placed = jnp.sum((before + offsets[:, None, :]) * onehot_float, axis=2)
    return placed.reshape(row_count).astype(jnp.int32)


def shards(
    pressure,
    face_block,
    stencil_local,
    stencil_weight,
    area_normal,
    face_part,
    face_nodes,
    stiffness,
    connect,
    halo_nodes,
    node_mass,
    displacement,
    velocity,
):
    gx_size = lax.axis_size("gx")
    yz_size = lax.axis_size("yz")
    devices = gx_size * yz_size
    face_count = face_block.shape[0]
    capacity = 2 * face_count // devices
    slot_total = devices * capacity
    traction = stencil(face_block, pressure, stencil_local, stencil_weight, area_normal)
    target = face_part[:, 0]
    slots = target * capacity + arrival_order(target, devices)
    slot_hots = hot_pair(slots, slot_total)
    packed = spread_cols(
        jnp.concatenate([traction, face_nodes.astype(jnp.float32)], axis=0), slot_hots
    )
    send = packed.reshape(10, 2, devices, capacity).transpose(2, 0, 1, 3).reshape(devices, 10, 2 * capacity)
    node_disp, returned = solid(
        send, stiffness, connect, halo_nodes, node_mass, displacement, velocity, gx_size, yz_size, shape_table()
    )
    returned = returned.reshape(devices, 6, 2, capacity).transpose(1, 2, 0, 3).reshape(12, slot_total)
    face_disp = pick_cols(returned, slot_hots)
    return (node_disp, face_disp)


def solution(mesh):
    in_specs = (
        P(("gx", "yz"), None),
        P(("gx", "yz")),
        P(None, ("gx", "yz")),
        P(None, ("gx", "yz")),
        P(None, ("gx", "yz")),
        P(("gx", "yz"), None),
        P(None, ("gx", "yz")),
        P(None, None, ("gx", "yz")),
        P(None, ("gx", "yz")),
        P(None, ("gx", "yz")),
        P(("gx", "yz")),
        P(None, ("gx", "yz")),
        P(None, ("gx", "yz")),
    )
    out_specs = (P(None, ("gx", "yz")), P(None, ("gx", "yz")))
    return jax.shard_map(shards, mesh=mesh, in_specs=in_specs, out_specs=out_specs, check_vma=False)
```

```python
import functools
import math

import jax
import jax.numpy as jnp
import numpy as np
from jax import lax
from jax.experimental import pallas as pl
from jax.experimental.pallas import tpu as pltpu
from jax.sharding import PartitionSpec as P

MESH = pl.DeviceIdType.MESH
F32 = jnp.float32
BF16 = jnp.bfloat16
SUBSTEPS = 4

def half_lanes(left, right):
    lane = lax.broadcasted_iota(jnp.int32, (8, 128), 1)
    return jnp.where(lane < 64, F32(left), F32(right))

def mix_weights(shapes):
    pick = lambda q, a: float(shapes[q, a])
    out = []
    for j in range(4):
        e, o = 2 * j, 2 * j + 1
        out.append((
            half_lanes(pick(0, e), pick(1, o)), half_lanes(pick(1, e), pick(0, o)),
            half_lanes(pick(2, e), pick(3, o)), half_lanes(pick(3, e), pick(2, o))))
    return out

def solid_kernel(nx, ny, shapes, s_ref, k_hbm, con_ref, halo_ref, mass_ref, disp_ref, vel_ref,
                 nd_ref, ret_ref,
                 recv, outb, kmat, ids, con_lo, con_hi, u_s, fh_s, fl_s, v_s, oh_e, oh_h, oh_x, v_x,
                 dsend, drecv, fsend, frecv,
                 k_sem, fs_sem, fr_sem, rs_sem, rr_sem, ds_sem, dr_sem, gs_sem, gr_sem):
    n = nx * ny
    gx = lax.axis_index("gx")
    yz = lax.axis_index("yz")
    me = gx * ny + yz
    dev = lambda t: (t // ny, lax.rem(t, ny))
    nxt = lax.rem(me + 1, n)
    prv = lax.rem(me + n - 1, n)
    kcopy = pltpu.make_async_copy(k_hbm, kmat, k_sem)
    kcopy.start()
    barrier = pltpu.get_barrier_semaphore()

    def greet(i, _):
        pl.semaphore_signal(barrier, inc=1, device_id=dev(lax.rem(me + i, n)), device_id_type=MESH)
        return 0
    lax.fori_loop(1, n, greet, 0)

    sub8 = lax.broadcasted_iota(jnp.int32, (8, 128), 0)
    sub128 = lax.broadcasted_iota(jnp.int32, (128, 128), 0)
    weights = mix_weights(shapes)

    con_lo[...] = con_ref[...] & 127
    con_hi[...] = con_ref[...] >> 7
    for a in range(20):
        for e in range(2):
            row = jnp.broadcast_to(con_lo[a:a + 1, 128 * e:128 * e + 128], (128, 128))
            oh_e[a * 256 + 128 * e:a * 256 + 128 * e + 128, :] = jnp.where(row == sub128, F32(1), F32(0)).T.astype(BF16)
    halo_lo = [jnp.broadcast_to(halo_ref[r:r + 1, :] & 127, (8, 128)) for r in range(2)]
    halo_hi = [jnp.broadcast_to(halo_ref[r:r + 1, :] >> 7, (8, 128)) for r in range(2)]
    for r in range(2):
        row = jnp.broadcast_to(halo_ref[r:r + 1, :] & 127, (128, 128))
        oh_h[128 * r:128 * r + 128, :] = jnp.where(row == sub128, F32(1), F32(0)).T.astype(BF16)
    stack = lambda ref, c: jnp.concatenate([ref[c:c + 1, 128 * h:128 * h + 128] for h in range(8)], axis=0)
    disp = [stack(disp_ref, c) for c in range(3)]
    vel = [stack(vel_ref, c) for c in range(3)]
    mass = stack(mass_ref, 0)

    pl.semaphore_wait(barrier, n - 1)

    def near(src, dst, ss, rs, t):
        return pltpu.make_async_remote_copy(src_ref=src, dst_ref=dst, send_sem=ss, recv_sem=rs, device_id=dev(t), device_id_type=MESH)

    def disp_copies(step):
        return [near(dsend.at[step, 1], drecv.at[step, 0], ds_sem.at[step, 1], dr_sem.at[step, 0], nxt),
                near(dsend.at[step, 0], drecv.at[step, 1], ds_sem.at[step, 0], dr_sem.at[step, 1], prv)]

    def force_copies(step):
        return [near(fsend.at[step, 0], frecv.at[step, 1], gs_sem.at[step, 0], gr_sem.at[step, 1], prv),
                near(fsend.at[step, 1], frecv.at[step, 0], gs_sem.at[step, 1], gr_sem.at[step, 0], nxt)]

    def start_both(copies):
        up, down = copies

        @pl.when(me < n - 1)
        def _():
            up.start()

        @pl.when(me > 0)
        def _():
            down.start()

    def wait_both(copies):
        up, down = copies

        @pl.when(me < n - 1)
        def _():
            up.wait_send()
            down.wait_recv()

        @pl.when(me > 0)
        def _():
            down.wait_send()
            up.wait_recv()

    def send_disp(step, disp):
        for r in range(2):
            for c in range(3):
                g = jnp.where(halo_hi[r] == sub8, lane_take(disp[c], halo_lo[r]), F32(0))
                dsend[step, r, c:c + 1, :] = jnp.sum(g, axis=0, keepdims=True)
        start_both(disp_copies(step))

    def internal(step, disp):
        wait_both(disp_copies(step))
        ghost = [jnp.where(me > 0, drecv[step, 0, 0:3, :], F32(0)), jnp.where(me < n - 1, drecv[step, 1, 0:3, :], F32(0))]
        for c in range(3):
            rows = [disp[c][h:h + 1, :] for h in range(8)] + [ghost[0][c:c + 1, :], ghost[1][c:c + 1, :]]
            rows = [jnp.broadcast_to(r, (8, 128)) for r in rows]
            for at in range(3):
                for e in range(2):
                    lo = con_lo[8 * at:8 * at + 8, 128 * e:128 * e + 128]
                    hi = con_hi[8 * at:8 * at + 8, 128 * e:128 * e + 128]
                    acc = lane_take(rows[0], lo)
                    for h in range(1, 10):
                        acc = jnp.where(hi == h, lane_take(rows[h], lo), acc)
                    u_s[c, 8 * at:8 * at + 8, 128 * e:128 * e + 128] = acc

        def multiply(a, acc):
            for c in range(3):
                acc = acc + kmat[c * 20 + a] * u_s[c, pl.ds(a, 1), :]
            return acc
        force = lax.fori_loop(0, 20, multiply, jnp.zeros((60, 256), F32))
        fh = force.astype(BF16).astype(F32)
        fh_s[...] = fh
        fl_s[...] = force - fh
        sub16 = lax.broadcasted_iota(jnp.int32, (16, 256), 0)
        for a in range(20):
            mask = jnp.broadcast_to(con_hi[a:a + 1, :], (16, 256)) == sub16
            for c in range(3):
                for k, part in enumerate((fh_s, fl_s)):
                    row = jnp.broadcast_to(part[20 * c + a:20 * c + a + 1, :], (16, 256))
                    v_s[48 * k + 16 * c:48 * k + 16 * c + 16, a * 256:a * 256 + 256] = jnp.where(mask, row, F32(0)).astype(BF16)
        both = jnp.dot(v_s[...], oh_e[...], preferred_element_type=F32)
        total = both[:48] + both[48:]
        for k in range(2):
            for c in range(3):
                fsend[step, k, c:c + 1, :] = total[16 * c + 8 + k:16 * c + 9 + k, :]
        start_both(force_copies(step)[::-1])
        return [total[16 * c:16 * c + 8, :] for c in range(3)]

    def advance(step, own, ext, disp, vel):
        wait_both(force_copies(step)[::-1])
        got = [jnp.where(me > 0, frecv[step, 0, 0:3, :], F32(0)), jnp.where(me < n - 1, frecv[step, 1, 0:3, :], F32(0))]
        parts = []
        for c in range(3):
            cols = []
            for r in range(2):
                x = jnp.where(halo_hi[r] == sub8, jnp.broadcast_to(got[r][c:c + 1, :], (8, 128)), F32(0))
                cols.append(x)
            parts.append(jnp.concatenate(cols, axis=1))
        x = jnp.concatenate(parts, axis=0)
        xh = x.astype(BF16).astype(F32)
        lhs = jnp.concatenate([xh, x - xh], axis=0).astype(BF16)
        both = jnp.dot(lhs, oh_h[...], preferred_element_type=F32)
        add = both[:24] + both[24:]
        vel = [vel[c] + (ext[c] - (own[c] + add[8 * c:8 * c + 8, :])) / mass for c in range(3)]
        disp = [disp[c] + vel[c] for c in range(3)]
        return disp, vel

    send_disp(0, disp)

    def fwd(i):
        t = lax.rem(me + i, n)
        return near(s_ref.at[t], recv.at[me], fs_sem.at[i], fr_sem.at[i], t)

    def fwd_start(i, _):
        fwd(i).start()
        return 0
    lax.fori_loop(1, n, fwd_start, 0)
    recv[me] = s_ref[me]
    kcopy.wait()
    own = internal(0, disp)


    sub128h = lax.broadcasted_iota(jnp.int32, (128, 128), 0).astype(jnp.int16)

    tiles = n // 8
    mine = me // 8

    def gather_load(k, acc):
        base = pl.multiple_of(lax.rem(mine + tiles - k, tiles) * 8, 8)
        for s in range(8):
            i = lax.rem(me + n - (base + s), n)

            @pl.when(i != 0)
            def _():
                fwd(i).wait_recv()
        get = lambda r: recv[pl.ds(base, 8), r, :]
        loads = []
        for c in range(3):
            t0, t1 = get(2 * c), get(2 * c + 1)
            r0, r1 = pltpu.roll(t0, 64, 1), pltpu.roll(t1, 64, 1)
            loads.append([weights[j][0] * t0 + weights[j][1] * r0 + weights[j][2] * t1 + weights[j][3] * r1 for j in range(4)])
        for j in range(4):
            idx = get(6 + j).astype(jnp.int32)
            ids[j, pl.ds(base, 8), :] = idx
            lo, hi = idx & 127, idx >> 7
            highs = [loads[c][j].astype(BF16).astype(F32) for c in range(3)]
            lows = [loads[c][j] - highs[c] for c in range(3)]
            for s in range(8):
                at = (j * 8 + s) * 128
                row = jnp.broadcast_to(lo[s:s + 1, :], (128, 128)).astype(jnp.int16)
                oh_x[:, at:at + 128] = jnp.where(row == sub128h, BF16(1), BF16(0))
                mask = jnp.broadcast_to(hi[s:s + 1, :], (8, 128)) == sub8
                v_x[:, at:at + 128] = jnp.concatenate(
                    [jnp.where(mask, jnp.broadcast_to(p[s:s + 1, :], (8, 128)), F32(0)) for p in highs + lows], axis=0).astype(BF16)
        return acc + lax.dot_general(v_x[...], oh_x[...], (((1,), (1,)), ((), ())), preferred_element_type=F32)
    both = lax.fori_loop(0, tiles, gather_load, jnp.zeros((48, 128), F32))
    ext = [both[8 * c:8 * c + 8] + both[24 + 8 * c:32 + 8 * c] for c in range(3)]

    disp, vel = advance(0, own, ext, disp, vel)
    for step in range(1, SUBSTEPS):
        send_disp(step, disp)
        own = internal(step, disp)
        disp, vel = advance(step, own, ext, disp, vel)
    for c in range(3):
        for h in range(8):
            nd_ref[c:c + 1, 128 * h:128 * h + 128] = disp[c][h:h + 1, :]
            u_s[c, h:h + 1, 0:128] = disp[c][h:h + 1, :]

    def ret(i):
        t = lax.rem(me + i, n)
        return near(outb.at[t], ret_ref.at[me], rs_sem.at[i], rr_sem.at[i], t)

    def back(k, _):
        base = pl.multiple_of(lax.rem(mine + k, tiles) * 8, 8)
        sums = [[jnp.zeros((8, 128), F32)] * 4 for c in range(3)]
        for j in range(4):
            idx = ids[j, pl.ds(base, 8), :]
            lo, hi = idx & 127, idx >> 7
            masks = [hi == h for h in range(1, 8)]
            for c in range(3):
                acc = lane_take(jnp.broadcast_to(u_s[c, 0:1, 0:128], (8, 128)), lo)
                for h in range(1, 8):
                    acc = jnp.where(masks[h - 1], lane_take(jnp.broadcast_to(u_s[c, h:h + 1, 0:128], (8, 128)), lo), acc)
                sums[c] = [sums[c][m] + weights[j][m] * acc for m in range(4)]
        for c in range(3):
            p0, q0, p1, q1 = sums[c]
            outb[pl.ds(base, 8), 2 * c, :] = p0 + pltpu.roll(q0, 64, 1)
            outb[pl.ds(base, 8), 2 * c + 1, :] = p1 + pltpu.roll(q1, 64, 1)
        for s in range(8):
            i = lax.rem(base + s + n - me, n)

            @pl.when(i != 0)
            def _():
                ret(i).start()
        return 0
    lax.fori_loop(0, tiles, back, 0)
    ret_ref[me] = outb[me]

    def drain(i, _):
        fwd(i).wait_send()
        ret(i).wait()
        return 0
    lax.fori_loop(1, n, drain, 0)


def solid(send, stiffness, connect, halo, mass, disp, vel, nx, ny, shapes):
    n = nx * ny
    V = pl.BlockSpec(memory_space=pltpu.VMEM)
    A = pl.BlockSpec(memory_space=pl.ANY)
    D = pltpu.SemaphoreType.DMA
    connect = jnp.pad(connect, ((0, 4), (0, 0)))
    return pl.pallas_call(
        functools.partial(solid_kernel, nx, ny, shapes),
        out_shape=(jax.ShapeDtypeStruct(disp.shape, F32), jax.ShapeDtypeStruct((n, 6, 128), F32)),
        in_specs=[V, A, V, V, V, V, V],
        out_specs=(V, V),
        scratch_shapes=[
            pltpu.VMEM((n, 10, 128), F32), pltpu.VMEM((n, 6, 128), F32), pltpu.VMEM((60, 60, 256), F32),
            pltpu.VMEM((4, n, 128), jnp.int32), pltpu.VMEM((24, 256), jnp.int32), pltpu.VMEM((24, 256), jnp.int32),
            pltpu.VMEM((3, 24, 256), F32), pltpu.VMEM((60, 256), F32), pltpu.VMEM((60, 256), F32),
            pltpu.VMEM((96, 5120), BF16), pltpu.VMEM((5120, 128), BF16), pltpu.VMEM((256, 128), BF16),
            pltpu.VMEM((128, 4096), BF16), pltpu.VMEM((48, 4096), BF16),
            pltpu.VMEM((SUBSTEPS, 2, 8, 128), F32), pltpu.VMEM((SUBSTEPS, 2, 8, 128), F32),
            pltpu.VMEM((SUBSTEPS, 2, 8, 128), F32), pltpu.VMEM((SUBSTEPS, 2, 8, 128), F32),
            D, D((n,)), D((n,)), D((n,)), D((n,)), D((SUBSTEPS, 2)), D((SUBSTEPS, 2)), D((SUBSTEPS, 2)), D((SUBSTEPS, 2))],
        compiler_params=pltpu.CompilerParams(collective_id=0, has_side_effects=True, vmem_limit_bytes=48 * 2**20),
        name="solid",
    )(send, stiffness, connect, halo, mass.reshape(1, -1), disp, vel)


STRIDE = 40
UNR = 32
TAKE = lax.GatherDimensionNumbers(
    offset_dims=(), collapsed_slice_dims=(1,), start_index_map=(1,), operand_batching_dims=(0,), start_indices_batching_dims=(0,)
)

def lane_take(x, idx):
    return lax.gather(x, idx[..., None], TAKE, slice_sizes=(1, 1), mode=lax.GatherScatterMode.PROMISE_IN_BOUNDS)

def stencil_kernel(fb_ref, pr_ref, loc_ref, w_ref, an_ref, out_ref, tab32, tab, idxt, wt, res):
    def relayout(b, _):
        r0 = pl.multiple_of(b * 16, 16)
        for t in range(32):
            x = pr_ref[pl.ds(r0, 16), 128 * t:128 * t + 128].astype(jnp.float32)
            tab32[pl.ds(t, 8, stride=STRIDE), :] = x[:8]
            tab32[pl.ds(8 * STRIDE + t, 8, stride=STRIDE), :] = x[8:]
        for n in range(16):
            tab[pl.ds(pl.multiple_of((r0 + n) * 32, 32), 32), :] = tab32[n * STRIDE:n * STRIDE + 32, :].astype(jnp.bfloat16)
        return 0
    lax.fori_loop(0, 16, relayout, 0)
    for i in range(8):
        idxt[128 * i:128 * i + 128, :] = jnp.concatenate(
            [loc_ref[:, a * 1024 + 128 * i:a * 1024 + 128 * i + 128] for a in range(4)], axis=0).T
        wt[128 * i:128 * i + 128, :] = jnp.concatenate(
            [w_ref[:, a * 1024 + 128 * i:a * 1024 + 128 * i + 128] for a in range(4)], axis=0).T
    lane = lax.broadcasted_iota(jnp.int32, (16, 128), 1)
    sub = lax.broadcasted_iota(jnp.int32, (16, 128), 0).astype(jnp.int16)
    grp = (lane // 32).astype(jnp.int16)
    m_lo = grp < 2
    m0 = grp == 0
    m2 = grp == 2

    def main(gg, _):
        for uu in range(UNR // 8):
            base = pl.multiple_of(gg * UNR + 8 * uu, 8)
            rows = []
            for u in range(8):
                g = base + u
                row = jnp.broadcast_to(idxt[pl.ds(g, 1), :], (16, 128))
                lo = (row & 127).astype(jnp.int16)
                hi = (row >> 7).astype(jnp.int16)
                cl = hi < 16
                mine = (hi & 15) == sub
                xs = []
                for a in range(4):
                    off = pl.multiple_of(fb_ref[a * 1024 + g] * 32, 32)
                    xs.append(jnp.where(cl, lane_take(tab[pl.ds(off, 16), :], lo), lane_take(tab[pl.ds(off + 16, 16), :], lo)))
                x = jnp.where(m_lo, jnp.where(m0, xs[0], xs[1]), jnp.where(m2, xs[2], xs[3]))
                x = jnp.where(mine, x, jnp.bfloat16(0)).astype(jnp.float32)
                rows.append(jnp.sum(x[:8] + x[8:], axis=0, keepdims=True))
            res[pl.ds(base, 8), :] = jnp.concatenate(rows, axis=0) * wt[pl.ds(base, 8), :]
        return 0
    lax.fori_loop(0, 1024 // UNR, main, 0)
    for i in range(8):
        rt = res[128 * i:128 * i + 128, :].T
        for a in range(4):
            f0 = a * 1024 + 128 * i
            fp = jnp.concatenate([jnp.sum(rt[a * 32 + 8 * q:a * 32 + 8 * q + 8], axis=0, keepdims=True) for q in range(4)], axis=0)
            fp3 = jnp.concatenate([fp, fp, fp], axis=0)
            out_ref[:, f0:f0 + 128] = -(an_ref[:, f0:f0 + 128] * fp3)

def stencil(face_block, pressure, local, weight, area):
    V = pl.BlockSpec(memory_space=pltpu.VMEM)
    return pl.pallas_call(
        stencil_kernel,
        out_shape=jax.ShapeDtypeStruct((12, 4096), jnp.float32),
        in_specs=[pl.BlockSpec(memory_space=pltpu.SMEM), V, V, V, V],
        out_specs=V,
        scratch_shapes=[pltpu.VMEM((16 * STRIDE, 128), jnp.float32), pltpu.VMEM((8192, 128), jnp.bfloat16), pltpu.VMEM((1024, 128), jnp.int32),
                        pltpu.VMEM((1024, 128), jnp.float32), pltpu.VMEM((1024, 128), jnp.float32)],
        compiler_params=pltpu.CompilerParams(vmem_limit_bytes=40 * 2**20),
        name="stencil",
    )(face_block, pressure, local, weight, area)


def shape_table():
    corner_u = [-1, 1, 1, -1, 0, 1, 0, -1]
    corner_v = [-1, -1, 1, 1, -1, 0, 1, 0]
    gauss_point = 1.0 / math.sqrt(3.0)
    points = [
        (-gauss_point, -gauss_point),
        (gauss_point, -gauss_point),
        (gauss_point, gauss_point),
        (-gauss_point, gauss_point),
    ]
    shape_values = np.zeros((4, 8), np.float32)
    for position, (coord_u, coord_v) in enumerate(points):
        for corner in range(8):
            node_u = corner_u[corner]
            node_v = corner_v[corner]
            if corner < 4:
                entry_value = (
                    0.25
                    * (1 + coord_u * node_u)
                    * (1 + coord_v * node_v)
                    * (coord_u * node_u + coord_v * node_v - 1)
                )
            elif node_u == 0:
                entry_value = 0.5 * (1 - coord_u * coord_u) * (1 + coord_v * node_v)
            else:
                entry_value = 0.5 * (1 + coord_u * node_u) * (1 - coord_v * coord_v)
            shape_values[position, corner] = entry_value
    return shape_values


def hot_pair(indices, extent):
    lanes_width = 32
    upper_count = -(-extent // lanes_width)
    upper_hot = (
        indices[None, :] // lanes_width == lax.broadcasted_iota(jnp.int32, (upper_count, 1), 0)
    ).astype(jnp.float32)
    lower_hot = (
        indices[None, :] % lanes_width == lax.broadcasted_iota(jnp.int32, (lanes_width, 1), 0)
    ).astype(jnp.float32)
    return (upper_hot, lower_hot)


def pick_cols(table, hots):
    upper_hot, lower_hot = hots
    lanes_width = lower_hot.shape[0]
    upper_count = upper_hot.shape[0]
    comps, extent = table.shape
    grid = (
        table.reshape(comps, upper_count, lanes_width)
        .transpose(1, 0, 2)
        .reshape(upper_count, comps * lanes_width)
    )
    rows_out = lax.dot_general(
        grid,
        upper_hot,
        (((0,), (0,)), ((), ())),
        precision=lax.Precision.HIGHEST,
        preferred_element_type=jnp.float32,
    )
    return jnp.sum(rows_out.reshape(comps, lanes_width, -1) * lower_hot[None], axis=1)


def spread_cols(values, hots):
    upper_hot, lower_hot = hots
    lanes_width = lower_hot.shape[0]
    upper_count = upper_hot.shape[0]
    comps = values.shape[0]
    masked = (values[:, None, :] * lower_hot[None]).reshape(comps * lanes_width, -1)
    summed = lax.dot_general(
        masked,
        upper_hot,
        (((1,), (1,)), ((), ())),
        precision=lax.Precision.HIGHEST,
        preferred_element_type=jnp.float32,
    )
    return (
        summed.reshape(comps, lanes_width, upper_count)
        .transpose(0, 2, 1)
        .reshape(comps, upper_count * lanes_width)
    )


def arrival_order(target, devices):
    row_count = target.shape[0]
    group_rows = min(512, row_count)
    groups = row_count // group_rows
    onehot = (target[:, None] == jnp.arange(devices, dtype=jnp.int32)[None, :]).astype(jnp.bfloat16)
    onehot = onehot.reshape(groups, group_rows, devices)
    lower_ones = (
        lax.broadcasted_iota(jnp.int32, (group_rows, group_rows), 0)
        > lax.broadcasted_iota(jnp.int32, (group_rows, group_rows), 1)
    ).astype(jnp.bfloat16)
    before = jnp.einsum("ij,gjd->gid", lower_ones, onehot, preferred_element_type=jnp.float32)
    onehot_float = onehot.astype(jnp.float32)
    totals = jnp.sum(onehot_float, axis=1)
    offsets = jnp.cumsum(totals, axis=0) - totals
    placed = jnp.sum((before + offsets[:, None, :]) * onehot_float, axis=2)
    return placed.reshape(row_count).astype(jnp.int32)


def shards(
    pressure,
    face_block,
    stencil_local,
    stencil_weight,
    area_normal,
    face_part,
    face_nodes,
    stiffness,
    connect,
    halo_nodes,
    node_mass,
    displacement,
    velocity,
):
    gx_size = lax.axis_size("gx")
    yz_size = lax.axis_size("yz")
    devices = gx_size * yz_size
    face_count = face_block.shape[0]
    capacity = 2 * face_count // devices
    slot_total = devices * capacity
    traction = stencil(face_block, pressure, stencil_local, stencil_weight, area_normal)
    target = face_part[:, 0]
    slots = target * capacity + arrival_order(target, devices)
    slot_hots = hot_pair(slots, slot_total)
    packed = spread_cols(
        jnp.concatenate([traction, face_nodes.astype(jnp.float32)], axis=0), slot_hots
    )
    send = packed.reshape(10, 2, devices, capacity).transpose(2, 0, 1, 3).reshape(devices, 10, 2 * capacity)
    node_disp, returned = solid(
        send, stiffness, connect, halo_nodes, node_mass, displacement, velocity, gx_size, yz_size, shape_table()
    )
    returned = returned.reshape(devices, 6, 2, capacity).transpose(1, 2, 0, 3).reshape(12, slot_total)
    face_disp = pick_cols(returned, slot_hots)
    return (node_disp, face_disp)


def solution(mesh):
    in_specs = (
        P(("gx", "yz"), None),
        P(("gx", "yz")),
        P(None, ("gx", "yz")),
        P(None, ("gx", "yz")),
        P(None, ("gx", "yz")),
        P(("gx", "yz"), None),
        P(None, ("gx", "yz")),
        P(None, None, ("gx", "yz")),
        P(None, ("gx", "yz")),
        P(None, ("gx", "yz")),
        P(("gx", "yz")),
        P(None, ("gx", "yz")),
        P(None, ("gx", "yz")),
    )
    out_specs = (P(None, ("gx", "yz")), P(None, ("gx", "yz")))
    return jax.shard_map(shards, mesh=mesh, in_specs=in_specs, out_specs=out_specs, check_vma=False)
```

```python
import functools
import math

import jax
import jax.numpy as jnp
import numpy as np
from jax import lax
from jax.experimental import pallas as pl
from jax.experimental.pallas import tpu as pltpu
from jax.sharding import PartitionSpec as P

MESH = pl.DeviceIdType.MESH
F32 = jnp.float32
BF16 = jnp.bfloat16
SUBSTEPS = 4

def half_lanes(left, right):
    lane = lax.broadcasted_iota(jnp.int32, (8, 128), 1)
    return jnp.where(lane < 64, F32(left), F32(right))

def mix_weights(shapes):
    pick = lambda q, a: float(shapes[q, a])
    out = []
    for j in range(4):
        e, o = 2 * j, 2 * j + 1
        out.append((
            half_lanes(pick(0, e), pick(1, o)), half_lanes(pick(1, e), pick(0, o)),
            half_lanes(pick(2, e), pick(3, o)), half_lanes(pick(3, e), pick(2, o))))
    return out

STRIDE = 40
UNR = 32
TAKE = lax.GatherDimensionNumbers(
    offset_dims=(), collapsed_slice_dims=(1,), start_index_map=(1,), operand_batching_dims=(0,), start_indices_batching_dims=(0,)
)

def lane_take(x, idx):
    return lax.gather(x, idx[..., None], TAKE, slice_sizes=(1, 1), mode=lax.GatherScatterMode.PROMISE_IN_BOUNDS)

def stencil_part(fb_ref, pr_ref, loc_ref, w_ref, an_ref, out_ref, tab32, tab, idxt, wt, res, arrive_lists, arrive_blocks):
    arrive_lists()
    for i in range(8):
        idxt[128 * i:128 * i + 128, :] = jnp.concatenate(
            [loc_ref[:, a * 1024 + 128 * i:a * 1024 + 128 * i + 128] for a in range(4)], axis=0).T
        wt[128 * i:128 * i + 128, :] = jnp.concatenate(
            [w_ref[:, a * 1024 + 128 * i:a * 1024 + 128 * i + 128] for a in range(4)], axis=0).T
    arrive_blocks()

    def relayout(b, _):
        r0 = pl.multiple_of(b * 16, 16)
        for t in range(32):
            x = pr_ref[pl.ds(r0, 16), 128 * t:128 * t + 128].astype(jnp.float32)
            tab32[pl.ds(t, 8, stride=STRIDE), :] = x[:8]
            tab32[pl.ds(8 * STRIDE + t, 8, stride=STRIDE), :] = x[8:]
        for n in range(16):
            tab[r0 + n] = tab32[n * STRIDE:n * STRIDE + 32, :].astype(jnp.bfloat16)
        return 0
    lax.fori_loop(0, 16, relayout, 0)
    lane = lax.broadcasted_iota(jnp.int32, (16, 128), 1)
    sub = lax.broadcasted_iota(jnp.int32, (16, 128), 0).astype(jnp.int16)
    grp = (lane // 32).astype(jnp.int16)
    m_lo = grp < 2
    m0 = grp == 0
    m2 = grp == 2

    def main(gg, _):
        for uu in range(UNR // 8):
            base = pl.multiple_of(gg * UNR + 8 * uu, 8)
            rows = []
            for u in range(8):
                g = base + u
                row = jnp.broadcast_to(idxt[pl.ds(g, 1), :], (16, 128))
                lo = (row & 127).astype(jnp.int16)
                hi = (row >> 7).astype(jnp.int16)
                cl = hi < 16
                mine = (hi & 15) == sub
                xs = []
                for a in range(4):
                    block = tab[fb_ref[a * 1024 + g]]
                    xs.append(jnp.where(cl, lane_take(block[:16], lo), lane_take(block[16:], lo)))
                x = jnp.where(m_lo, jnp.where(m0, xs[0], xs[1]), jnp.where(m2, xs[2], xs[3]))
                x = jnp.where(mine, x, jnp.bfloat16(0)).astype(jnp.float32)
                rows.append(jnp.sum(x[:8] + x[8:], axis=0, keepdims=True))
            res[pl.ds(base, 8), :] = jnp.concatenate(rows, axis=0) * wt[pl.ds(base, 8), :]
        return 0
    lax.fori_loop(0, 1024 // UNR, main, 0)
    for i in range(8):
        rt = res[128 * i:128 * i + 128, :].T
        for a in range(4):
            f0 = a * 1024 + 128 * i
            fp = jnp.concatenate([jnp.sum(rt[a * 32 + 8 * q:a * 32 + 8 * q + 8], axis=0, keepdims=True) for q in range(4)], axis=0)
            fp3 = jnp.concatenate([fp, fp, fp], axis=0)
            out_ref[:, f0:f0 + 128] = -(an_ref[:, f0:f0 + 128] * fp3)


def pack_part(tgt_ref, fn_ref, trac, slot_s, carry, acc, send_ref):
    rows128 = lax.broadcasted_iota(jnp.int32, (128, 256), 0)
    rows256 = lax.broadcasted_iota(jnp.int32, (256, 256), 0)
    cols256 = lax.broadcasted_iota(jnp.int32, (256, 256), 1)
    rows32 = lax.broadcasted_iota(jnp.int32, (32, 256), 0)
    one_if = lambda m: jnp.where(m, F32(1), F32(0)).astype(BF16)
    upper = one_if(rows256 < cols256)
    ones = jnp.ones((256, 256), BF16)
    carry[...] = jnp.zeros_like(carry)
    acc[...] = jnp.zeros_like(acc)

    def tile(kt, _):
        at = pl.ds(pl.multiple_of(kt * 256, 256), 256)
        target = tgt_ref[:, at]
        hit = jnp.broadcast_to(target, (128, 256)) == rows128
        hot = one_if(hit)
        before = jnp.dot(hot, upper, preferred_element_type=F32) + carry[...]
        carry[...] += jnp.dot(hot, ones, preferred_element_type=F32)
        slot = jnp.sum(jnp.where(hit, before, F32(0)), axis=0, keepdims=True).astype(jnp.int32)
        slot_s[:, at] = slot
        place = jnp.broadcast_to(target + 128 * (slot >> 5), (256, 256))
        weights = one_if(place == rows256)
        mask = jnp.broadcast_to(slot & 31, (32, 256)) == rows32
        values = [trac[:, at], fn_ref[:, at].astype(F32)]
        total = None
        highs = [v.astype(BF16).astype(F32) for v in values]
        for part in (highs, [v - h for v, h in zip(values, highs)]):
            x = [
                jnp.where(mask, jnp.broadcast_to(p[r:r + 1, :], (32, 256)), F32(0)).astype(BF16)
                for p in part
                for r in range(p.shape[0])
            ]
            y = lax.dot_general(jnp.concatenate(x, axis=0), weights, (((1,), (1,)), ((), ())), preferred_element_type=F32)
            total = y if total is None else total + y
        acc[...] += total
        return 0
    lax.fori_loop(0, 16, tile, 0)
    for r in range(10):
        block = [acc[32 * v:32 * v + 32, 128 * h:128 * h + 128] for v in (2 * r, 2 * r + 1) for h in range(2)]
        send_ref[:, r, :] = jnp.concatenate(block, axis=0).T


def unpack_part(tgt_ref, slot_s, ret_ref, lhs, fd_ref):
    rows128 = lax.broadcasted_iota(jnp.int32, (128, 256), 0)
    rows64 = lax.broadcasted_iota(jnp.int32, (64, 256), 0)
    for r in range(6):
        x = ret_ref[:, r, :].T
        xh = x.astype(BF16).astype(F32)
        lhs[128 * r:128 * r + 128, :] = jnp.concatenate([xh, x - xh], axis=1).astype(BF16)

    def tile(kt, _):
        at = pl.ds(pl.multiple_of(kt * 256, 256), 256)
        hot = jnp.where(jnp.broadcast_to(tgt_ref[:, at], (128, 256)) == rows128, F32(1), F32(0)).astype(BF16)
        y = jnp.dot(lhs[...], jnp.concatenate([hot, hot], axis=0), preferred_element_type=F32)
        mask = jnp.broadcast_to(slot_s[:, at], (64, 256)) == rows64
        fd_ref[:, at] = jnp.concatenate(
            [jnp.sum(jnp.where(mask, y[64 * v:64 * v + 64, :], F32(0)), axis=0, keepdims=True) for v in range(12)], axis=0
        )
        return 0
    lax.fori_loop(0, 16, tile, 0)


def solid_kernel(nx, ny, shapes, fb_ref, pr_hbm, loc_hbm, w_hbm, an_hbm, fn_hbm, tgt_ref, k_hbm, con_ref, halo_ref, mass_ref, disp_ref, vel_ref,
                 nd_ref, fd_ref,
                 pr_ref, loc_ref, w_ref, an_ref, fn_ref, trac, tab32, tab, idxt, wt, res, slot_s, carry, acc_s, s_ref, ret_ref, lhs,
                 recv, outb, kmat, ids, con_lo, con_hi, u_s, fh_s, fl_s, v_s, oh_e, oh_h, oh_x, v_x,
                 dsend, drecv, fsend, frecv,
                 in_sem, k_sem, fs_sem, fr_sem, rs_sem, rr_sem, ds_sem, dr_sem, gs_sem, gr_sem):
    n = nx * ny
    gx = lax.axis_index("gx")
    yz = lax.axis_index("yz")
    me = gx * ny + yz
    dev = lambda t: (t // ny, lax.rem(t, ny))
    nxt = lax.rem(me + 1, n)
    prv = lax.rem(me + n - 1, n)
    ins = [pltpu.make_async_copy(src, dst, in_sem.at[k]) for k, (src, dst) in enumerate(
        ((loc_hbm, loc_ref), (w_hbm, w_ref), (pr_hbm, pr_ref), (an_hbm, an_ref), (fn_hbm, fn_ref)))]
    for cp in ins:
        cp.start()
    kcopy = pltpu.make_async_copy(k_hbm, kmat, k_sem)
    kcopy.start()
    barrier = pltpu.get_barrier_semaphore()

    def greet(i, _):
        pl.semaphore_signal(barrier, inc=1, device_id=dev(lax.rem(me + i, n)), device_id_type=MESH)
        return 0
    lax.fori_loop(1, n, greet, 0)

    sub8 = lax.broadcasted_iota(jnp.int32, (8, 128), 0)
    sub128 = lax.broadcasted_iota(jnp.int32, (128, 128), 0)
    weights = mix_weights(shapes)

    halo_lo = [jnp.broadcast_to(halo_ref[r:r + 1, :] & 127, (8, 128)) for r in range(2)]
    halo_hi = [jnp.broadcast_to(halo_ref[r:r + 1, :] >> 7, (8, 128)) for r in range(2)]
    stack = lambda ref, c: jnp.concatenate([ref[c:c + 1, 128 * h:128 * h + 128] for h in range(8)], axis=0)
    disp = [stack(disp_ref, c) for c in range(3)]
    vel = [stack(vel_ref, c) for c in range(3)]
    mass = stack(mass_ref, 0)

    def arrive_lists():
        ins[0].wait()
        ins[1].wait()

    def arrive_blocks():
        for cp in ins[2:]:
            cp.wait()
    stencil_part(fb_ref, pr_ref, loc_ref, w_ref, an_ref, trac, tab32, tab, idxt, wt, res, arrive_lists, arrive_blocks)
    pack_part(tgt_ref, fn_ref, trac, slot_s, carry, acc_s, s_ref)
    pl.semaphore_wait(barrier, n - 1)

    def near(src, dst, ss, rs, t):
        return pltpu.make_async_remote_copy(src_ref=src, dst_ref=dst, send_sem=ss, recv_sem=rs, device_id=dev(t), device_id_type=MESH)

    def disp_copies(step):
        return [near(dsend.at[step, 1], drecv.at[step, 0], ds_sem.at[step, 1], dr_sem.at[step, 0], nxt),
                near(dsend.at[step, 0], drecv.at[step, 1], ds_sem.at[step, 0], dr_sem.at[step, 1], prv)]

    def force_copies(step):
        return [near(fsend.at[step, 0], frecv.at[step, 1], gs_sem.at[step, 0], gr_sem.at[step, 1], prv),
                near(fsend.at[step, 1], frecv.at[step, 0], gs_sem.at[step, 1], gr_sem.at[step, 0], nxt)]

    def start_both(copies):
        up, down = copies

        @pl.when(me < n - 1)
        def _():
            up.start()

        @pl.when(me > 0)
        def _():
            down.start()

    def wait_both(copies):
        up, down = copies

        @pl.when(me < n - 1)
        def _():
            up.wait_send()
            down.wait_recv()

        @pl.when(me > 0)
        def _():
            down.wait_send()
            up.wait_recv()

    def send_disp(step, disp):
        for r in range(2):
            for c in range(3):
                g = jnp.where(halo_hi[r] == sub8, lane_take(disp[c], halo_lo[r]), F32(0))
                dsend[step, r, c:c + 1, :] = jnp.sum(g, axis=0, keepdims=True)
        start_both(disp_copies(step))

    def internal(step, disp):
        wait_both(disp_copies(step))
        ghost = [jnp.where(me > 0, drecv[step, 0, 0:3, :], F32(0)), jnp.where(me < n - 1, drecv[step, 1, 0:3, :], F32(0))]
        for c in range(3):
            rows = [disp[c][h:h + 1, :] for h in range(8)] + [ghost[0][c:c + 1, :], ghost[1][c:c + 1, :]]
            rows = [jnp.broadcast_to(r, (8, 128)) for r in rows]
            for at in range(3):
                for e in range(2):
                    lo = con_lo[8 * at:8 * at + 8, 128 * e:128 * e + 128]
                    hi = con_hi[8 * at:8 * at + 8, 128 * e:128 * e + 128]
                    acc = lane_take(rows[0], lo)
                    for h in range(1, 10):
                        acc = jnp.where(hi == h, lane_take(rows[h], lo), acc)
                    u_s[c, 8 * at:8 * at + 8, 128 * e:128 * e + 128] = acc

        def multiply(a, acc):
            for c in range(3):
                acc = acc + kmat[c * 20 + a] * u_s[c, pl.ds(a, 1), :]
            return acc
        force = lax.fori_loop(0, 20, multiply, jnp.zeros((60, 256), F32))
        fh = force.astype(BF16).astype(F32)
        fh_s[...] = fh
        fl_s[...] = force - fh
        sub16 = lax.broadcasted_iota(jnp.int32, (16, 256), 0)
        for a in range(20):
            mask = jnp.broadcast_to(con_hi[a:a + 1, :], (16, 256)) == sub16
            for c in range(3):
                for k, part in enumerate((fh_s, fl_s)):
                    row = jnp.broadcast_to(part[20 * c + a:20 * c + a + 1, :], (16, 256))
                    v_s[48 * k + 16 * c:48 * k + 16 * c + 16, a * 256:a * 256 + 256] = jnp.where(mask, row, F32(0)).astype(BF16)
        both = jnp.dot(v_s[...], oh_e[...], preferred_element_type=F32)
        total = both[:48] + both[48:]
        for k in range(2):
            for c in range(3):
                fsend[step, k, c:c + 1, :] = total[16 * c + 8 + k:16 * c + 9 + k, :]
        start_both(force_copies(step)[::-1])
        return [total[16 * c:16 * c + 8, :] for c in range(3)]

    def advance(step, own, ext, disp, vel):
        wait_both(force_copies(step)[::-1])
        got = [jnp.where(me > 0, frecv[step, 0, 0:3, :], F32(0)), jnp.where(me < n - 1, frecv[step, 1, 0:3, :], F32(0))]
        parts = []
        for c in range(3):
            cols = []
            for r in range(2):
                x = jnp.where(halo_hi[r] == sub8, jnp.broadcast_to(got[r][c:c + 1, :], (8, 128)), F32(0))
                cols.append(x)
            parts.append(jnp.concatenate(cols, axis=1))
        x = jnp.concatenate(parts, axis=0)
        xh = x.astype(BF16).astype(F32)
        lhs = jnp.concatenate([xh, x - xh], axis=0).astype(BF16)
        both = jnp.dot(lhs, oh_h[...], preferred_element_type=F32)
        add = both[:24] + both[24:]
        vel = [vel[c] + (ext[c] - (own[c] + add[8 * c:8 * c + 8, :])) / mass for c in range(3)]
        disp = [disp[c] + vel[c] for c in range(3)]
        return disp, vel

    send_disp(0, disp)

    def fwd(i):
        t = lax.rem(me + i, n)
        return near(s_ref.at[t], recv.at[me], fs_sem.at[i], fr_sem.at[i], t)

    def fwd_start(i, _):
        fwd(i).start()
        return 0
    lax.fori_loop(1, n, fwd_start, 0)
    recv[me] = s_ref[me]
    for dst in (con_lo, con_hi):
        dst[16:24, :] = jnp.zeros((8, 256), jnp.int32)
    con_lo[0:20, :] = con_ref[...] & 127
    con_hi[0:20, :] = con_ref[...] >> 7
    for a in range(20):
        for e in range(2):
            row = jnp.broadcast_to(con_lo[a:a + 1, 128 * e:128 * e + 128], (128, 128))
            oh_e[a * 256 + 128 * e:a * 256 + 128 * e + 128, :] = jnp.where(row == sub128, F32(1), F32(0)).T.astype(BF16)
    for r in range(2):
        row = jnp.broadcast_to(halo_ref[r:r + 1, :] & 127, (128, 128))
        oh_h[128 * r:128 * r + 128, :] = jnp.where(row == sub128, F32(1), F32(0)).T.astype(BF16)
    kcopy.wait()
    own = internal(0, disp)


    sub128h = lax.broadcasted_iota(jnp.int32, (128, 128), 0).astype(jnp.int16)

    tiles = n // 8
    mine = me // 8

    def gather_load(k, acc):
        base = pl.multiple_of(lax.rem(mine + tiles - k, tiles) * 8, 8)
        for s in range(8):
            i = lax.rem(me + n - (base + s), n)

            @pl.when(i != 0)
            def _():
                fwd(i).wait_recv()
        get = lambda r: recv[pl.ds(base, 8), r, :]
        loads = []
        for c in range(3):
            t0, t1 = get(2 * c), get(2 * c + 1)
            r0, r1 = pltpu.roll(t0, 64, 1), pltpu.roll(t1, 64, 1)
            loads.append([weights[j][0] * t0 + weights[j][1] * r0 + weights[j][2] * t1 + weights[j][3] * r1 for j in range(4)])
        for j in range(4):
            idx = get(6 + j).astype(jnp.int32)
            ids[j, pl.ds(base, 8), :] = idx
            lo, hi = idx & 127, idx >> 7
            highs = [loads[c][j].astype(BF16).astype(F32) for c in range(3)]
            lows = [loads[c][j] - highs[c] for c in range(3)]
            for s in range(8):
                at = (j * 8 + s) * 128
                row = jnp.broadcast_to(lo[s:s + 1, :], (128, 128)).astype(jnp.int16)
                oh_x[:, at:at + 128] = jnp.where(row == sub128h, BF16(1), BF16(0))
                mask = jnp.broadcast_to(hi[s:s + 1, :], (8, 128)) == sub8
                v_x[:, at:at + 128] = jnp.concatenate(
                    [jnp.where(mask, jnp.broadcast_to(p[s:s + 1, :], (8, 128)), F32(0)) for p in highs + lows], axis=0).astype(BF16)
        return acc + lax.dot_general(v_x[...], oh_x[...], (((1,), (1,)), ((), ())), preferred_element_type=F32)
    both = lax.fori_loop(0, tiles, gather_load, jnp.zeros((48, 128), F32))
    ext = [both[8 * c:8 * c + 8] + both[24 + 8 * c:32 + 8 * c] for c in range(3)]

    disp, vel = advance(0, own, ext, disp, vel)
    for step in range(1, SUBSTEPS):
        send_disp(step, disp)
        own = internal(step, disp)
        disp, vel = advance(step, own, ext, disp, vel)
    for c in range(3):
        for h in range(8):
            nd_ref[c:c + 1, 128 * h:128 * h + 128] = disp[c][h:h + 1, :]
            u_s[c, h:h + 1, 0:128] = disp[c][h:h + 1, :]

    def ret(i):
        t = lax.rem(me + i, n)
        return near(outb.at[t], ret_ref.at[me], rs_sem.at[i], rr_sem.at[i], t)

    def back(k, _):
        base = pl.multiple_of(lax.rem(mine + k, tiles) * 8, 8)
        sums = [[jnp.zeros((8, 128), F32)] * 4 for c in range(3)]
        for j in range(4):
            idx = ids[j, pl.ds(base, 8), :]
            lo, hi = idx & 127, idx >> 7
            masks = [hi == h for h in range(1, 8)]
            for c in range(3):
                acc = lane_take(jnp.broadcast_to(u_s[c, 0:1, 0:128], (8, 128)), lo)
                for h in range(1, 8):
                    acc = jnp.where(masks[h - 1], lane_take(jnp.broadcast_to(u_s[c, h:h + 1, 0:128], (8, 128)), lo), acc)
                sums[c] = [sums[c][m] + weights[j][m] * acc for m in range(4)]
        for c in range(3):
            p0, q0, p1, q1 = sums[c]
            outb[pl.ds(base, 8), 2 * c, :] = p0 + pltpu.roll(q0, 64, 1)
            outb[pl.ds(base, 8), 2 * c + 1, :] = p1 + pltpu.roll(q1, 64, 1)
        for s in range(8):
            i = lax.rem(base + s + n - me, n)

            @pl.when(i != 0)
            def _():
                ret(i).start()
        return 0
    lax.fori_loop(0, tiles, back, 0)
    ret_ref[me] = outb[me]

    def drain(i, _):
        fwd(i).wait_send()
        ret(i).wait()
        return 0
    lax.fori_loop(1, n, drain, 0)
    unpack_part(tgt_ref, slot_s, ret_ref, lhs, fd_ref)


def solid(face_block, pressure, local, weight, area, nodes, target, stiffness, connect, halo, mass, disp, vel, nx, ny, shapes):
    n = nx * ny
    V = pl.BlockSpec(memory_space=pltpu.VMEM)
    A = pl.BlockSpec(memory_space=pl.ANY)
    D = pltpu.SemaphoreType.DMA
    M = pltpu.VMEM
    I32 = jnp.int32
    return pl.pallas_call(
        functools.partial(solid_kernel, nx, ny, shapes),
        out_shape=(jax.ShapeDtypeStruct(disp.shape, F32), jax.ShapeDtypeStruct((12, target.shape[1]), F32)),
        in_specs=[pl.BlockSpec(memory_space=pltpu.SMEM), A, A, A, A, A, V, A, V, V, V, V, V],
        out_specs=(V, V),
        scratch_shapes=[
            M(pressure.shape, BF16), M(local.shape, I32), M(weight.shape, F32), M(area.shape, F32), M(nodes.shape, I32),
            M(area.shape, F32), M((16 * STRIDE, 128), F32), M((256, 32, 128), BF16), M((1024, 128), I32), M((1024, 128), F32),
            M((1024, 128), F32), M(target.shape, I32), M((128, 256), F32), M((640, 256), F32),
            M((n, 10, 128), F32), M((n, 6, 128), F32), M((768, 256), BF16),
            M((n, 10, 128), F32), M((n, 6, 128), F32), M((60, 60, 256), F32),
            M((4, n, 128), I32), M((24, 256), I32), M((24, 256), I32),
            M((3, 24, 256), F32), M((60, 256), F32), M((60, 256), F32),
            M((96, 5120), BF16), M((5120, 128), BF16), M((256, 128), BF16),
            M((128, 4096), BF16), M((48, 4096), BF16),
            M((SUBSTEPS, 2, 8, 128), F32), M((SUBSTEPS, 2, 8, 128), F32),
            M((SUBSTEPS, 2, 8, 128), F32), M((SUBSTEPS, 2, 8, 128), F32),
            D((5,)), D, D((n,)), D((n,)), D((n,)), D((n,)), D((SUBSTEPS, 2)), D((SUBSTEPS, 2)), D((SUBSTEPS, 2)), D((SUBSTEPS, 2))],
        compiler_params=pltpu.CompilerParams(collective_id=0, has_side_effects=True, vmem_limit_bytes=56 * 2**20),
        name="solid",
    )(face_block, pressure, local, weight, area, nodes, target, stiffness, connect, halo, mass.reshape(1, -1), disp, vel)


def shape_table():
    corner_u = [-1, 1, 1, -1, 0, 1, 0, -1]
    corner_v = [-1, -1, 1, 1, -1, 0, 1, 0]
    gauss_point = 1.0 / math.sqrt(3.0)
    points = [
        (-gauss_point, -gauss_point),
        (gauss_point, -gauss_point),
        (gauss_point, gauss_point),
        (-gauss_point, gauss_point),
    ]
    shape_values = np.zeros((4, 8), np.float32)
    for position, (coord_u, coord_v) in enumerate(points):
        for corner in range(8):
            node_u = corner_u[corner]
            node_v = corner_v[corner]
            if corner < 4:
                entry_value = (
                    0.25
                    * (1 + coord_u * node_u)
                    * (1 + coord_v * node_v)
                    * (coord_u * node_u + coord_v * node_v - 1)
                )
            elif node_u == 0:
                entry_value = 0.5 * (1 - coord_u * coord_u) * (1 + coord_v * node_v)
            else:
                entry_value = 0.5 * (1 + coord_u * node_u) * (1 - coord_v * coord_v)
            shape_values[position, corner] = entry_value
    return shape_values


def shards(
    pressure,
    face_block,
    stencil_local,
    stencil_weight,
    area_normal,
    face_part,
    face_nodes,
    stiffness,
    connect,
    halo_nodes,
    node_mass,
    displacement,
    velocity,
):
    gx_size = lax.axis_size("gx")
    yz_size = lax.axis_size("yz")
    return solid(
        face_block, pressure, stencil_local, stencil_weight, area_normal, face_nodes, face_part.reshape(1, -1),
        stiffness, connect, halo_nodes, node_mass, displacement, velocity, gx_size, yz_size, shape_table()
    )


def solution(mesh):
    in_specs = (
        P(("gx", "yz"), None),
        P(("gx", "yz")),
        P(None, ("gx", "yz")),
        P(None, ("gx", "yz")),
        P(None, ("gx", "yz")),
        P(("gx", "yz"), None),
        P(None, ("gx", "yz")),
        P(None, None, ("gx", "yz")),
        P(None, ("gx", "yz")),
        P(None, ("gx", "yz")),
        P(("gx", "yz")),
        P(None, ("gx", "yz")),
        P(None, ("gx", "yz")),
    )
    out_specs = (P(None, ("gx", "yz")), P(None, ("gx", "yz")))
    return jax.shard_map(shards, mesh=mesh, in_specs=in_specs, out_specs=out_specs, check_vma=False)
```

```python
import functools
import math

import jax
import jax.numpy as jnp
import numpy as np
from jax import lax
from jax.experimental import pallas as pl
from jax.experimental.pallas import tpu as pltpu
from jax.sharding import PartitionSpec as P

MESH = pl.DeviceIdType.MESH
F32 = jnp.float32
BF16 = jnp.bfloat16
SUBSTEPS = 4

def half_lanes(left, right):
    lane = lax.broadcasted_iota(jnp.int32, (8, 128), 1)
    return jnp.where(lane < 64, F32(left), F32(right))

def mix_weights(shapes):
    pick = lambda q, a: float(shapes[q, a])
    out = []
    for j in range(4):
        e, o = 2 * j, 2 * j + 1
        out.append((
            half_lanes(pick(0, e), pick(1, o)), half_lanes(pick(1, e), pick(0, o)),
            half_lanes(pick(2, e), pick(3, o)), half_lanes(pick(3, e), pick(2, o))))
    return out

STRIDE = 40
UNR = 32
TAKE = lax.GatherDimensionNumbers(
    offset_dims=(), collapsed_slice_dims=(1,), start_index_map=(1,), operand_batching_dims=(0,), start_indices_batching_dims=(0,)
)

def lane_take(x, idx):
    return lax.gather(x, idx[..., None], TAKE, slice_sizes=(1, 1), mode=lax.GatherScatterMode.PROMISE_IN_BOUNDS)

def stencil_part(fb_ref, pr_ref, loc_ref, w_ref, an_ref, out_ref, tab32, tab, idxt, wt, res, arrive_lists, arrive_blocks):
    arrive_lists()
    for i in range(8):
        idxt[128 * i:128 * i + 128, :] = jnp.concatenate(
            [loc_ref[:, a * 1024 + 128 * i:a * 1024 + 128 * i + 128] for a in range(4)], axis=0).T
        wt[128 * i:128 * i + 128, :] = jnp.concatenate(
            [w_ref[:, a * 1024 + 128 * i:a * 1024 + 128 * i + 128] for a in range(4)], axis=0).T
    arrive_blocks()

    def relayout(b, _):
        r0 = pl.multiple_of(b * 16, 16)
        for t in range(32):
            x = pr_ref[pl.ds(r0, 16), 128 * t:128 * t + 128].astype(jnp.float32)
            tab32[pl.ds(t, 8, stride=STRIDE), :] = x[:8]
            tab32[pl.ds(8 * STRIDE + t, 8, stride=STRIDE), :] = x[8:]
        for n in range(16):
            tab[r0 + n] = tab32[n * STRIDE:n * STRIDE + 32, :].astype(jnp.bfloat16)
        return 0
    lax.fori_loop(0, 16, relayout, 0)
    lane = lax.broadcasted_iota(jnp.int32, (16, 128), 1)
    sub = lax.broadcasted_iota(jnp.int32, (16, 128), 0).astype(jnp.int16)
    grp = (lane // 32).astype(jnp.int16)
    m_lo = grp < 2
    m0 = grp == 0
    m2 = grp == 2

    def main(gg, _):
        for uu in range(UNR // 8):
            base = pl.multiple_of(gg * UNR + 8 * uu, 8)
            rows = []
            for u in range(8):
                g = base + u
                row = jnp.broadcast_to(idxt[pl.ds(g, 1), :], (16, 128))
                lo = (row & 127).astype(jnp.int16)
                hi = (row >> 7).astype(jnp.int16)
                cl = hi < 16
                mine = (hi & 15) == sub
                xs = []
                for a in range(4):
                    block = tab[fb_ref[a * 1024 + g]]
                    xs.append(jnp.where(cl, lane_take(block[:16], lo), lane_take(block[16:], lo)))
                x = jnp.where(m_lo, jnp.where(m0, xs[0], xs[1]), jnp.where(m2, xs[2], xs[3]))
                x = jnp.where(mine, x, jnp.bfloat16(0)).astype(jnp.float32)
                rows.append(jnp.sum(x[:8] + x[8:], axis=0, keepdims=True))
            res[pl.ds(base, 8), :] = jnp.concatenate(rows, axis=0) * wt[pl.ds(base, 8), :]
        return 0
    lax.fori_loop(0, 1024 // UNR, main, 0)
    for i in range(8):
        rt = res[128 * i:128 * i + 128, :].T
        for a in range(4):
            f0 = a * 1024 + 128 * i
            fp = jnp.concatenate([jnp.sum(rt[a * 32 + 8 * q:a * 32 + 8 * q + 8], axis=0, keepdims=True) for q in range(4)], axis=0)
            fp3 = jnp.concatenate([fp, fp, fp], axis=0)
            out_ref[:, f0:f0 + 128] = -(an_ref[:, f0:f0 + 128] * fp3)


def pack_part(tgt_ref, fn_ref, trac, slot_s, carry, acc, send_ref):
    wide = 1024
    rows128 = lax.broadcasted_iota(jnp.int32, (128, 256), 0)
    rows256 = lax.broadcasted_iota(jnp.int32, (256, 256), 0)
    cols256 = lax.broadcasted_iota(jnp.int32, (256, 256), 1)
    rows256w = lax.broadcasted_iota(jnp.int32, (256, wide), 0)
    rows32 = lax.broadcasted_iota(jnp.int32, (32, wide), 0)
    one_if = lambda m: jnp.where(m, F32(1), F32(0)).astype(BF16)
    upper = one_if(rows256 < cols256)
    ones = jnp.ones((256, 256), BF16)
    carry[...] = jnp.zeros_like(carry)
    acc[...] = jnp.zeros_like(acc)

    def rank(kt, _):
        before = carry[...]
        for m in range(4):
            at = pl.ds(pl.multiple_of(kt * wide + 256 * m, 256), 256)
            hit = jnp.broadcast_to(tgt_ref[:, at], (128, 256)) == rows128
            hot = one_if(hit)
            within = jnp.dot(hot, upper, preferred_element_type=F32) + before
            slot_s[:, at] = jnp.sum(jnp.where(hit, within, F32(0)), axis=0, keepdims=True).astype(jnp.int32)
            before = before + jnp.dot(hot, ones, preferred_element_type=F32)
        carry[...] = before
        return 0
    lax.fori_loop(0, 4, rank, 0)

    def tile(kt, _):
        at = pl.ds(pl.multiple_of(kt * wide, wide), wide)
        slot = slot_s[:, at]
        place = jnp.broadcast_to(tgt_ref[:, at] + 128 * (slot >> 5), (256, wide))
        weights = one_if(place == rows256w)
        mask = jnp.broadcast_to(slot & 31, (32, wide)) == rows32
        values = [trac[:, at], fn_ref[:, at].astype(F32)]
        total = None
        highs = [v.astype(BF16).astype(F32) for v in values]
        for part in (highs, [v - h for v, h in zip(values, highs)]):
            x = [
                jnp.where(mask, jnp.broadcast_to(p[r:r + 1, :], (32, wide)), F32(0)).astype(BF16)
                for p in part
                for r in range(p.shape[0])
            ]
            y = lax.dot_general(jnp.concatenate(x, axis=0), weights, (((1,), (1,)), ((), ())), preferred_element_type=F32)
            total = y if total is None else total + y
        acc[...] += total
        return 0
    lax.fori_loop(0, 4, tile, 0)
    for r in range(10):
        block = [acc[32 * v:32 * v + 32, 128 * h:128 * h + 128] for v in (2 * r, 2 * r + 1) for h in range(2)]
        send_ref[:, r, :] = jnp.concatenate(block, axis=0).T


def unpack_part(tgt_ref, slot_s, ret_ref, lhs, fd_ref):
    wide = 512
    rows128 = lax.broadcasted_iota(jnp.int32, (128, wide), 0)
    rows64 = lax.broadcasted_iota(jnp.int32, (64, wide), 0)
    for r in range(6):
        x = ret_ref[:, r, :].T
        xh = x.astype(BF16).astype(F32)
        lhs[128 * r:128 * r + 128, :] = jnp.concatenate([xh, x - xh], axis=1).astype(BF16)

    def tile(kt, _):
        at = pl.ds(pl.multiple_of(kt * wide, wide), wide)
        hot = jnp.where(jnp.broadcast_to(tgt_ref[:, at], (128, wide)) == rows128, F32(1), F32(0)).astype(BF16)
        y = jnp.dot(lhs[...], jnp.concatenate([hot, hot], axis=0), preferred_element_type=F32)
        mask = jnp.broadcast_to(slot_s[:, at], (64, wide)) == rows64
        fd_ref[:, at] = jnp.concatenate(
            [jnp.sum(jnp.where(mask, y[64 * v:64 * v + 64, :], F32(0)), axis=0, keepdims=True) for v in range(12)], axis=0
        )
        return 0
    lax.fori_loop(0, 8, tile, 0)


def solid_kernel(nx, ny, shapes, fb_ref, pr_hbm, loc_hbm, w_hbm, an_hbm, fn_hbm, tgt_ref, k_hbm, con_ref, halo_ref, mass_ref, disp_ref, vel_ref,
                 nd_ref, fd_ref,
                 pr_ref, loc_ref, w_ref, an_ref, fn_ref, trac, tab32, tab, idxt, wt, res, slot_s, carry, acc_s, s_ref, ret_ref, lhs,
                 recv, outb, kmat, ids, con_lo, con_hi, u_s, fh_s, fl_s, v_s, oh_e, oh_h,
                 dsend, drecv, fsend, frecv,
                 in_sem, k_sem, fs_sem, fr_sem, rs_sem, rr_sem, ds_sem, dr_sem, gs_sem, gr_sem):
    n = nx * ny
    gx = lax.axis_index("gx")
    yz = lax.axis_index("yz")
    me = gx * ny + yz
    dev = lambda t: (t // ny, lax.rem(t, ny))
    nxt = lax.rem(me + 1, n)
    prv = lax.rem(me + n - 1, n)
    ins = [pltpu.make_async_copy(src, dst, in_sem.at[k]) for k, (src, dst) in enumerate(
        ((loc_hbm, loc_ref), (w_hbm, w_ref), (pr_hbm, pr_ref), (an_hbm, an_ref), (fn_hbm, fn_ref)))]
    for cp in ins:
        cp.start()
    kcopy = pltpu.make_async_copy(k_hbm, kmat, k_sem)
    kcopy.start()
    barrier = pltpu.get_barrier_semaphore()

    gx_at = [lax.rem(gx + a, nx) for a in range(nx)]

    def greet(b, _):
        y = lax.rem(yz + b, ny)
        for a in range(nx):
            pl.semaphore_signal(barrier, inc=1, device_id=(gx_at[a], y), device_id_type=MESH)
        return 0
    lax.fori_loop(1, ny, greet, 0)
    for a in range(1, nx):
        pl.semaphore_signal(barrier, inc=1, device_id=(gx_at[a], yz), device_id_type=MESH)

    sub8 = lax.broadcasted_iota(jnp.int32, (8, 128), 0)
    sub128 = lax.broadcasted_iota(jnp.int32, (128, 128), 0)
    weights = mix_weights(shapes)

    halo_lo = [jnp.broadcast_to(halo_ref[r:r + 1, :] & 127, (8, 128)) for r in range(2)]
    halo_hi = [jnp.broadcast_to(halo_ref[r:r + 1, :] >> 7, (8, 128)) for r in range(2)]
    stack = lambda ref, c: jnp.concatenate([ref[c:c + 1, 128 * h:128 * h + 128] for h in range(8)], axis=0)
    disp = [stack(disp_ref, c) for c in range(3)]
    vel = [stack(vel_ref, c) for c in range(3)]
    mass = stack(mass_ref, 0)

    def arrive_lists():
        ins[0].wait()
        ins[1].wait()

    def arrive_blocks():
        for cp in ins[2:]:
            cp.wait()
    stencil_part(fb_ref, pr_ref, loc_ref, w_ref, an_ref, trac, tab32, tab, idxt, wt, res, arrive_lists, arrive_blocks)
    pack_part(tgt_ref, fn_ref, trac, slot_s, carry, acc_s, s_ref)
    pl.semaphore_wait(barrier, n - 1)

    def near(src, dst, ss, rs, t):
        return pltpu.make_async_remote_copy(src_ref=src, dst_ref=dst, send_sem=ss, recv_sem=rs, device_id=dev(t), device_id_type=MESH)

    def disp_copies(step):
        return [near(dsend.at[step, 1], drecv.at[step, 0], ds_sem.at[step, 1], dr_sem.at[step, 0], nxt),
                near(dsend.at[step, 0], drecv.at[step, 1], ds_sem.at[step, 0], dr_sem.at[step, 1], prv)]

    def force_copies(step):
        return [near(fsend.at[step, 0], frecv.at[step, 1], gs_sem.at[step, 0], gr_sem.at[step, 1], prv),
                near(fsend.at[step, 1], frecv.at[step, 0], gs_sem.at[step, 1], gr_sem.at[step, 0], nxt)]

    def start_both(copies):
        up, down = copies

        @pl.when(me < n - 1)
        def _():
            up.start()

        @pl.when(me > 0)
        def _():
            down.start()

    def wait_both(copies):
        up, down = copies

        @pl.when(me < n - 1)
        def _():
            up.wait_send()
            down.wait_recv()

        @pl.when(me > 0)
        def _():
            down.wait_send()
            up.wait_recv()

    def send_disp(step, disp):
        for r in range(2):
            for c in range(3):
                g = jnp.where(halo_hi[r] == sub8, lane_take(disp[c], halo_lo[r]), F32(0))
                dsend[step, r, c:c + 1, :] = jnp.sum(g, axis=0, keepdims=True)
        start_both(disp_copies(step))

    def internal(step, disp):
        wait_both(disp_copies(step))
        ghost = [jnp.where(me > 0, drecv[step, 0, 0:3, :], F32(0)), jnp.where(me < n - 1, drecv[step, 1, 0:3, :], F32(0))]
        for c in range(3):
            rows = [disp[c][h:h + 1, :] for h in range(8)] + [ghost[0][c:c + 1, :], ghost[1][c:c + 1, :]]
            rows = [jnp.broadcast_to(r, (8, 128)) for r in rows]
            for at in range(3):
                for e in range(2):
                    lo = con_lo[8 * at:8 * at + 8, 128 * e:128 * e + 128]
                    hi = con_hi[8 * at:8 * at + 8, 128 * e:128 * e + 128]
                    acc = lane_take(rows[0], lo)
                    for h in range(1, 10):
                        acc = jnp.where(hi == h, lane_take(rows[h], lo), acc)
                    u_s[c, 8 * at:8 * at + 8, 128 * e:128 * e + 128] = acc

        def multiply(a, acc):
            for c in range(3):
                acc = acc + kmat[c * 20 + a] * u_s[c, pl.ds(a, 1), :]
            return acc
        force = lax.fori_loop(0, 20, multiply, jnp.zeros((60, 256), F32))
        fh = force.astype(BF16).astype(F32)
        fh_s[...] = fh
        fl_s[...] = force - fh
        sub16 = lax.broadcasted_iota(jnp.int32, (16, 256), 0)
        for a in range(20):
            mask = jnp.broadcast_to(con_hi[a:a + 1, :], (16, 256)) == sub16
            for c in range(3):
                for k, part in enumerate((fh_s, fl_s)):
                    row = jnp.broadcast_to(part[20 * c + a:20 * c + a + 1, :], (16, 256))
                    v_s[48 * k + 16 * c:48 * k + 16 * c + 16, a * 256:a * 256 + 256] = jnp.where(mask, row, F32(0)).astype(BF16)
        both = jnp.dot(v_s[...], oh_e[...], preferred_element_type=F32)
        total = both[:48] + both[48:]
        for k in range(2):
            for c in range(3):
                fsend[step, k, c:c + 1, :] = total[16 * c + 8 + k:16 * c + 9 + k, :]
        start_both(force_copies(step)[::-1])
        return [total[16 * c:16 * c + 8, :] for c in range(3)]

    def advance(step, own, ext, disp, vel):
        wait_both(force_copies(step)[::-1])
        got = [jnp.where(me > 0, frecv[step, 0, 0:3, :], F32(0)), jnp.where(me < n - 1, frecv[step, 1, 0:3, :], F32(0))]
        parts = []
        for c in range(3):
            cols = []
            for r in range(2):
                x = jnp.where(halo_hi[r] == sub8, jnp.broadcast_to(got[r][c:c + 1, :], (8, 128)), F32(0))
                cols.append(x)
            parts.append(jnp.concatenate(cols, axis=1))
        x = jnp.concatenate(parts, axis=0)
        xh = x.astype(BF16).astype(F32)
        lhs = jnp.concatenate([xh, x - xh], axis=0).astype(BF16)
        both = jnp.dot(lhs, oh_h[...], preferred_element_type=F32)
        add = both[:24] + both[24:]
        vel = [vel[c] + (ext[c] - (own[c] + add[8 * c:8 * c + 8, :])) / mass for c in range(3)]
        disp = [disp[c] + vel[c] for c in range(3)]
        return disp, vel

    send_disp(0, disp)

    def fwd(a, b, g, y):
        return pltpu.make_async_remote_copy(
            src_ref=s_ref.at[g * ny + y], dst_ref=recv.at[me], send_sem=fs_sem.at[a * ny + b], recv_sem=fr_sem.at[a * ny + b],
            device_id=(g, y), device_id_type=MESH)

    def fwd_start(b, _):
        y = lax.rem(yz + b, ny)
        for a in range(nx):
            fwd(a, b, gx_at[a], y).start()
        return 0
    lax.fori_loop(1, ny, fwd_start, 0)
    for a in range(1, nx):
        fwd(a, 0, gx_at[a], yz).start()
    recv[me] = s_ref[me]
    for dst in (con_lo, con_hi):
        dst[16:24, :] = jnp.zeros((8, 256), jnp.int32)
    con_lo[0:20, :] = con_ref[...] & 127
    con_hi[0:20, :] = con_ref[...] >> 7
    for a in range(20):
        for e in range(2):
            row = jnp.broadcast_to(con_lo[a:a + 1, 128 * e:128 * e + 128], (128, 128))
            oh_e[a * 256 + 128 * e:a * 256 + 128 * e + 128, :] = jnp.where(row == sub128, F32(1), F32(0)).T.astype(BF16)
    for r in range(2):
        row = jnp.broadcast_to(halo_ref[r:r + 1, :] & 127, (128, 128))
        oh_h[128 * r:128 * r + 128, :] = jnp.where(row == sub128, F32(1), F32(0)).T.astype(BF16)
    kcopy.wait()
    own = internal(0, disp)


    sub128h = lax.broadcasted_iota(jnp.int32, (128, 128), 0).astype(jnp.int16)

    tiles = n // 8
    mine = me // 8

    def gather_load(k, acc):
        base = pl.multiple_of(lax.rem(mine + tiles - k, tiles) * 8, 8)
        a = lax.rem(gx + nx - base // ny, nx)
        for s in range(8):
            b = lax.rem(yz + ny - lax.rem(base, ny) - s, ny)

            @pl.when(base + s != me)
            def _():
                fwd(a, b, gx, yz).wait_recv()
        get = lambda r: recv[pl.ds(base, 8), r, :]
        loads = []
        for c in range(3):
            t0, t1 = get(2 * c), get(2 * c + 1)
            r0, r1 = pltpu.roll(t0, 64, 1), pltpu.roll(t1, 64, 1)
            loads.append([weights[j][0] * t0 + weights[j][1] * r0 + weights[j][2] * t1 + weights[j][3] * r1 for j in range(4)])
        total = jnp.zeros((48, 128), F32)
        for j in range(4):
            idx = get(6 + j).astype(jnp.int32)
            ids[j, pl.ds(base, 8), :] = idx
            lo, hi = idx & 127, idx >> 7
            highs = [loads[c][j].astype(BF16).astype(F32) for c in range(3)]
            lows = [loads[c][j] - highs[c] for c in range(3)]
            for s in range(0, 8, 2):
                hots, vals = [], []
                for k in (s, s + 1):
                    row = jnp.broadcast_to(lo[k:k + 1, :], (128, 128)).astype(jnp.int16)
                    hots.append(jnp.where(row == sub128h, BF16(1), BF16(0)))
                    mask = jnp.broadcast_to(hi[k:k + 1, :], (8, 128)) == sub8
                    vals.append(jnp.concatenate(
                        [jnp.where(mask, jnp.broadcast_to(p[k:k + 1, :], (8, 128)), F32(0)) for p in highs + lows], axis=0).astype(BF16))
                total = total + lax.dot_general(
                    jnp.concatenate(vals, axis=1), jnp.concatenate(hots, axis=1), (((1,), (1,)), ((), ())), preferred_element_type=F32)
        return acc + total
    both = lax.fori_loop(0, tiles, gather_load, jnp.zeros((48, 128), F32))
    ext = [both[8 * c:8 * c + 8] + both[24 + 8 * c:32 + 8 * c] for c in range(3)]

    disp, vel = advance(0, own, ext, disp, vel)
    for step in range(1, SUBSTEPS):
        send_disp(step, disp)
        own = internal(step, disp)
        disp, vel = advance(step, own, ext, disp, vel)
    for c in range(3):
        for h in range(8):
            nd_ref[c:c + 1, 128 * h:128 * h + 128] = disp[c][h:h + 1, :]
            u_s[c, h:h + 1, 0:128] = disp[c][h:h + 1, :]

    def ret(i):
        t = lax.rem(me + i, n)
        return near(outb.at[t], ret_ref.at[me], rs_sem.at[i], rr_sem.at[i], t)

    def back(k, _):
        base = pl.multiple_of(lax.rem(mine + k, tiles) * 8, 8)
        sums = [[jnp.zeros((8, 128), F32)] * 4 for c in range(3)]
        for j in range(4):
            idx = ids[j, pl.ds(base, 8), :]
            lo, hi = idx & 127, idx >> 7
            masks = [hi == h for h in range(1, 8)]
            for c in range(3):
                acc = lane_take(jnp.broadcast_to(u_s[c, 0:1, 0:128], (8, 128)), lo)
                for h in range(1, 8):
                    acc = jnp.where(masks[h - 1], lane_take(jnp.broadcast_to(u_s[c, h:h + 1, 0:128], (8, 128)), lo), acc)
                sums[c] = [sums[c][m] + weights[j][m] * acc for m in range(4)]
        for c in range(3):
            p0, q0, p1, q1 = sums[c]
            outb[pl.ds(base, 8), 2 * c, :] = p0 + pltpu.roll(q0, 64, 1)
            outb[pl.ds(base, 8), 2 * c + 1, :] = p1 + pltpu.roll(q1, 64, 1)
        for s in range(8):
            i = lax.rem(base + s + n - me, n)

            @pl.when(i != 0)
            def _():
                ret(i).start()
        return 0
    lax.fori_loop(0, tiles, back, 0)
    ret_ref[me] = outb[me]

    def drain(i, _):
        fwd(i // ny, lax.rem(i, ny), gx, yz).wait_send()
        ret(i).wait()
        return 0
    lax.fori_loop(1, n, drain, 0)
    unpack_part(tgt_ref, slot_s, ret_ref, lhs, fd_ref)


def solid(face_block, pressure, local, weight, area, nodes, target, stiffness, connect, halo, mass, disp, vel, nx, ny, shapes):
    n = nx * ny
    V = pl.BlockSpec(memory_space=pltpu.VMEM)
    A = pl.BlockSpec(memory_space=pl.ANY)
    D = pltpu.SemaphoreType.DMA
    M = pltpu.VMEM
    I32 = jnp.int32
    return pl.pallas_call(
        functools.partial(solid_kernel, nx, ny, shapes),
        out_shape=(jax.ShapeDtypeStruct(disp.shape, F32), jax.ShapeDtypeStruct((12, target.shape[1]), F32)),
        in_specs=[pl.BlockSpec(memory_space=pltpu.SMEM), A, A, A, A, A, V, A, V, V, V, V, V],
        out_specs=(V, V),
        scratch_shapes=[
            M(pressure.shape, BF16), M(local.shape, I32), M(weight.shape, F32), M(area.shape, F32), M(nodes.shape, I32),
            M(area.shape, F32), M((16 * STRIDE, 128), F32), M((256, 32, 128), BF16), M((1024, 128), I32), M((1024, 128), F32),
            M((1024, 128), F32), M(target.shape, I32), M((128, 256), F32), M((640, 256), F32),
            M((n, 10, 128), F32), M((n, 6, 128), F32), M((768, 256), BF16),
            M((n, 10, 128), F32), M((n, 6, 128), F32), M((60, 60, 256), F32),
            M((4, n, 128), I32), M((24, 256), I32), M((24, 256), I32),
            M((3, 24, 256), F32), M((60, 256), F32), M((60, 256), F32),
            M((96, 5120), BF16), M((5120, 128), BF16), M((256, 128), BF16),
            M((SUBSTEPS, 2, 8, 128), F32), M((SUBSTEPS, 2, 8, 128), F32),
            M((SUBSTEPS, 2, 8, 128), F32), M((SUBSTEPS, 2, 8, 128), F32),
            D((5,)), D, D((n,)), D((n,)), D((n,)), D((n,)), D((SUBSTEPS, 2)), D((SUBSTEPS, 2)), D((SUBSTEPS, 2)), D((SUBSTEPS, 2))],
        compiler_params=pltpu.CompilerParams(collective_id=0, has_side_effects=True, vmem_limit_bytes=56 * 2**20),
        name="solid",
    )(face_block, pressure, local, weight, area, nodes, target, stiffness, connect, halo, mass.reshape(1, -1), disp, vel)


def shape_table():
    corner_u = [-1, 1, 1, -1, 0, 1, 0, -1]
    corner_v = [-1, -1, 1, 1, -1, 0, 1, 0]
    gauss_point = 1.0 / math.sqrt(3.0)
    points = [
        (-gauss_point, -gauss_point),
        (gauss_point, -gauss_point),
        (gauss_point, gauss_point),
        (-gauss_point, gauss_point),
    ]
    shape_values = np.zeros((4, 8), np.float32)
    for position, (coord_u, coord_v) in enumerate(points):
        for corner in range(8):
            node_u = corner_u[corner]
            node_v = corner_v[corner]
            if corner < 4:
                entry_value = (
                    0.25
                    * (1 + coord_u * node_u)
                    * (1 + coord_v * node_v)
                    * (coord_u * node_u + coord_v * node_v - 1)
                )
            elif node_u == 0:
                entry_value = 0.5 * (1 - coord_u * coord_u) * (1 + coord_v * node_v)
            else:
                entry_value = 0.5 * (1 + coord_u * node_u) * (1 - coord_v * coord_v)
            shape_values[position, corner] = entry_value
    return shape_values


def shards(
    pressure,
    face_block,
    stencil_local,
    stencil_weight,
    area_normal,
    face_part,
    face_nodes,
    stiffness,
    connect,
    halo_nodes,
    node_mass,
    displacement,
    velocity,
):
    gx_size = lax.axis_size("gx")
    yz_size = lax.axis_size("yz")
    return solid(
        face_block, pressure, stencil_local, stencil_weight, area_normal, face_nodes, face_part.reshape(1, -1),
        stiffness, connect, halo_nodes, node_mass, displacement, velocity, gx_size, yz_size, shape_table()
    )


def solution(mesh):
    in_specs = (
        P(("gx", "yz"), None),
        P(("gx", "yz")),
        P(None, ("gx", "yz")),
        P(None, ("gx", "yz")),
        P(None, ("gx", "yz")),
        P(("gx", "yz"), None),
        P(None, ("gx", "yz")),
        P(None, None, ("gx", "yz")),
        P(None, ("gx", "yz")),
        P(None, ("gx", "yz")),
        P(("gx", "yz")),
        P(None, ("gx", "yz")),
        P(None, ("gx", "yz")),
    )
    out_specs = (P(None, ("gx", "yz")), P(None, ("gx", "yz")))
    return jax.shard_map(shards, mesh=mesh, in_specs=in_specs, out_specs=out_specs, check_vma=False)
```

```python
import functools
import math

import jax
import jax.numpy as jnp
import numpy as np
from jax import lax
from jax.experimental import pallas as pl
from jax.experimental.pallas import tpu as pltpu
from jax.sharding import PartitionSpec as P

MESH = pl.DeviceIdType.MESH
F32 = jnp.float32
BF16 = jnp.bfloat16
SUBSTEPS = 4

def half_lanes(left, right):
    lane = lax.broadcasted_iota(jnp.int32, (8, 128), 1)
    return jnp.where(lane < 64, F32(left), F32(right))

def mix_weights(shapes):
    pick = lambda q, a: float(shapes[q, a])
    out = []
    for j in range(4):
        e, o = 2 * j, 2 * j + 1
        out.append((
            half_lanes(pick(0, e), pick(1, o)), half_lanes(pick(1, e), pick(0, o)),
            half_lanes(pick(2, e), pick(3, o)), half_lanes(pick(3, e), pick(2, o))))
    return out

STRIDE = 40
UNR = 32
TAKE = lax.GatherDimensionNumbers(
    offset_dims=(), collapsed_slice_dims=(1,), start_index_map=(1,), operand_batching_dims=(0,), start_indices_batching_dims=(0,)
)

def lane_take(x, idx):
    return lax.gather(x, idx[..., None], TAKE, slice_sizes=(1, 1), mode=lax.GatherScatterMode.PROMISE_IN_BOUNDS)

def stencil_part(fb_ref, pr_ref, loc_ref, w_ref, an_ref, out_ref, tab32, tab, idxt, wt, res, arrive_lists, arrive_blocks):
    arrive_lists()
    for i in range(8):
        idxt[128 * i:128 * i + 128, :] = jnp.concatenate(
            [loc_ref[:, a * 1024 + 128 * i:a * 1024 + 128 * i + 128] for a in range(4)], axis=0).T
        wt[128 * i:128 * i + 128, :] = jnp.concatenate(
            [w_ref[:, a * 1024 + 128 * i:a * 1024 + 128 * i + 128] for a in range(4)], axis=0).T
    arrive_blocks()

    def relayout(b, _):
        r0 = pl.multiple_of(b * 16, 16)
        for t in range(32):
            x = pr_ref[pl.ds(r0, 16), 128 * t:128 * t + 128].astype(jnp.float32)
            tab32[pl.ds(t, 8, stride=STRIDE), :] = x[:8]
            tab32[pl.ds(8 * STRIDE + t, 8, stride=STRIDE), :] = x[8:]
        for n in range(16):
            tab[r0 + n] = tab32[n * STRIDE:n * STRIDE + 32, :].astype(jnp.bfloat16)
        return 0
    lax.fori_loop(0, 16, relayout, 0)
    lane = lax.broadcasted_iota(jnp.int32, (16, 128), 1)
    sub = lax.broadcasted_iota(jnp.int32, (16, 128), 0).astype(jnp.int16)
    grp = (lane // 32).astype(jnp.int16)
    m_lo = grp < 2
    m0 = grp == 0
    m2 = grp == 2

    def main(gg, _):
        for uu in range(UNR // 8):
            base = pl.multiple_of(gg * UNR + 8 * uu, 8)
            rows = []
            for u in range(8):
                g = base + u
                row = jnp.broadcast_to(idxt[pl.ds(g, 1), :], (16, 128))
                lo = (row & 127).astype(jnp.int16)
                hi = (row >> 7).astype(jnp.int16)
                cl = hi < 16
                mine = (hi & 15) == sub
                xs = []
                for a in range(4):
                    block = tab[fb_ref[a * 1024 + g]]
                    xs.append(jnp.where(cl, lane_take(block[:16], lo), lane_take(block[16:], lo)))
                x = jnp.where(m_lo, jnp.where(m0, xs[0], xs[1]), jnp.where(m2, xs[2], xs[3]))
                x = jnp.where(mine, x, jnp.bfloat16(0)).astype(jnp.float32)
                rows.append(jnp.sum(x[:8] + x[8:], axis=0, keepdims=True))
            res[pl.ds(base, 8), :] = jnp.concatenate(rows, axis=0) * wt[pl.ds(base, 8), :]
        return 0
    lax.fori_loop(0, 1024 // UNR, main, 0)
    for i in range(8):
        rt = res[128 * i:128 * i + 128, :].T
        for a in range(4):
            f0 = a * 1024 + 128 * i
            fp = jnp.concatenate([jnp.sum(rt[a * 32 + 8 * q:a * 32 + 8 * q + 8], axis=0, keepdims=True) for q in range(4)], axis=0)
            fp3 = jnp.concatenate([fp, fp, fp], axis=0)
            out_ref[:, f0:f0 + 128] = -(an_ref[:, f0:f0 + 128] * fp3)


def pack_part(tgt_ref, fn_ref, trac, slot_s, carry, acc, send_ref):
    wide = 1024
    rows128 = lax.broadcasted_iota(jnp.int32, (128, 256), 0)
    rows256 = lax.broadcasted_iota(jnp.int32, (256, 256), 0)
    cols256 = lax.broadcasted_iota(jnp.int32, (256, 256), 1)
    rows256w = lax.broadcasted_iota(jnp.int32, (256, wide), 0)
    rows32 = lax.broadcasted_iota(jnp.int32, (32, wide), 0)
    one_if = lambda m: jnp.where(m, F32(1), F32(0)).astype(BF16)
    upper = one_if(rows256 < cols256)
    ones = jnp.ones((256, 256), BF16)
    carry[...] = jnp.zeros_like(carry)
    acc[...] = jnp.zeros_like(acc)

    def rank(kt, _):
        before = carry[...]
        for m in range(4):
            at = pl.ds(pl.multiple_of(kt * wide + 256 * m, 256), 256)
            hit = jnp.broadcast_to(tgt_ref[:, at], (128, 256)) == rows128
            hot = one_if(hit)
            within = jnp.dot(hot, upper, preferred_element_type=F32) + before
            slot_s[:, at] = jnp.sum(jnp.where(hit, within, F32(0)), axis=0, keepdims=True).astype(jnp.int32)
            before = before + jnp.dot(hot, ones, preferred_element_type=F32)
        carry[...] = before
        return 0
    lax.fori_loop(0, 4, rank, 0)

    def tile(kt, _):
        at = pl.ds(pl.multiple_of(kt * wide, wide), wide)
        slot = slot_s[:, at]
        place = jnp.broadcast_to(tgt_ref[:, at] + 128 * (slot >> 5), (256, wide))
        weights = one_if(place == rows256w)
        mask = jnp.broadcast_to(slot & 31, (32, wide)) == rows32
        values = [trac[:, at], fn_ref[:, at].astype(F32)]
        total = None
        highs = [v.astype(BF16).astype(F32) for v in values]
        for part in (highs, [v - h for v, h in zip(values, highs)]):
            x = [
                jnp.where(mask, jnp.broadcast_to(p[r:r + 1, :], (32, wide)), F32(0)).astype(BF16)
                for p in part
                for r in range(p.shape[0])
            ]
            y = lax.dot_general(jnp.concatenate(x, axis=0), weights, (((1,), (1,)), ((), ())), preferred_element_type=F32)
            total = y if total is None else total + y
        acc[...] += total
        return 0
    lax.fori_loop(0, 4, tile, 0)
    for r in range(10):
        block = [acc[32 * v:32 * v + 32, 128 * h:128 * h + 128] for v in (2 * r, 2 * r + 1) for h in range(2)]
        send_ref[:, r, :] = jnp.concatenate(block, axis=0).T


def unpack_kernel(tgt_ref, slot_s, ret_ref, nd_in, nd_ref, fd_ref, lhs):
    nd_ref[...] = nd_in[...]
    wide = 512
    rows128 = lax.broadcasted_iota(jnp.int32, (128, wide), 0)
    rows64 = lax.broadcasted_iota(jnp.int32, (64, wide), 0)
    for r in range(6):
        x = ret_ref[:, r, :].T
        xh = x.astype(BF16).astype(F32)
        lhs[128 * r:128 * r + 128, :] = jnp.concatenate([xh, x - xh], axis=1).astype(BF16)

    def tile(kt, _):
        at = pl.ds(pl.multiple_of(kt * wide, wide), wide)
        hot = jnp.where(jnp.broadcast_to(tgt_ref[:, at], (128, wide)) == rows128, F32(1), F32(0)).astype(BF16)
        y = jnp.dot(lhs[...], jnp.concatenate([hot, hot], axis=0), preferred_element_type=F32)
        mask = jnp.broadcast_to(slot_s[:, at], (64, wide)) == rows64
        fd_ref[:, at] = jnp.concatenate(
            [jnp.sum(jnp.where(mask, y[64 * v:64 * v + 64, :], F32(0)), axis=0, keepdims=True) for v in range(12)], axis=0
        )
        return 0
    lax.fori_loop(0, 8, tile, 0)


def solid_kernel(nx, ny, shapes, fb_ref, pr_hbm, loc_hbm, w_hbm, an_hbm, fn_hbm, tgt_ref, k_hbm, con_ref, halo_ref, mass_ref, disp_ref, vel_ref,
                 nd_ref, ret_ref, slot_s,
                 pr_ref, loc_ref, w_ref, an_ref, fn_ref, trac, tab32, tab, idxt, wt, res, carry, acc_s, s_ref,
                 recv, outb, kmat, ids, con_lo, con_hi, u_s, fh_s, fl_s, v_s, oh_e, oh_h,
                 dsend, drecv, fsend, frecv,
                 in_sem, k_sem, fs_sem, fr_sem, rs_sem, rr_sem, ds_sem, dr_sem, gs_sem, gr_sem):
    n = nx * ny
    gx = lax.axis_index("gx")
    yz = lax.axis_index("yz")
    me = gx * ny + yz
    dev = lambda t: (t // ny, lax.rem(t, ny))
    nxt = lax.rem(me + 1, n)
    prv = lax.rem(me + n - 1, n)
    ins = [pltpu.make_async_copy(src, dst, in_sem.at[k]) for k, (src, dst) in enumerate(
        ((loc_hbm, loc_ref), (w_hbm, w_ref), (pr_hbm, pr_ref), (an_hbm, an_ref), (fn_hbm, fn_ref)))]
    for cp in ins:
        cp.start()
    kcopy = pltpu.make_async_copy(k_hbm, kmat, k_sem)
    kcopy.start()
    barrier = pltpu.get_barrier_semaphore()

    gx_at = [lax.rem(gx + a, nx) for a in range(nx)]

    def greet(b, _):
        y = lax.rem(yz + b, ny)
        for a in range(nx):
            pl.semaphore_signal(barrier, inc=1, device_id=(gx_at[a], y), device_id_type=MESH)
        return 0
    lax.fori_loop(1, ny, greet, 0)
    for a in range(1, nx):
        pl.semaphore_signal(barrier, inc=1, device_id=(gx_at[a], yz), device_id_type=MESH)

    sub8 = lax.broadcasted_iota(jnp.int32, (8, 128), 0)
    sub128 = lax.broadcasted_iota(jnp.int32, (128, 128), 0)
    weights = mix_weights(shapes)

    halo_lo = [jnp.broadcast_to(halo_ref[r:r + 1, :] & 127, (8, 128)) for r in range(2)]
    halo_hi = [jnp.broadcast_to(halo_ref[r:r + 1, :] >> 7, (8, 128)) for r in range(2)]
    stack = lambda ref, c: jnp.concatenate([ref[c:c + 1, 128 * h:128 * h + 128] for h in range(8)], axis=0)
    disp = [stack(disp_ref, c) for c in range(3)]
    vel = [stack(vel_ref, c) for c in range(3)]
    mass = stack(mass_ref, 0)

    def arrive_lists():
        ins[0].wait()
        ins[1].wait()

    def arrive_blocks():
        for cp in ins[2:]:
            cp.wait()
    stencil_part(fb_ref, pr_ref, loc_ref, w_ref, an_ref, trac, tab32, tab, idxt, wt, res, arrive_lists, arrive_blocks)
    pack_part(tgt_ref, fn_ref, trac, slot_s, carry, acc_s, s_ref)
    pl.semaphore_wait(barrier, n - 1)

    def near(src, dst, ss, rs, t):
        return pltpu.make_async_remote_copy(src_ref=src, dst_ref=dst, send_sem=ss, recv_sem=rs, device_id=dev(t), device_id_type=MESH)

    def disp_copies(step):
        return [near(dsend.at[step, 1], drecv.at[step, 0], ds_sem.at[step, 1], dr_sem.at[step, 0], nxt),
                near(dsend.at[step, 0], drecv.at[step, 1], ds_sem.at[step, 0], dr_sem.at[step, 1], prv)]

    def force_copies(step):
        return [near(fsend.at[step, 0], frecv.at[step, 1], gs_sem.at[step, 0], gr_sem.at[step, 1], prv),
                near(fsend.at[step, 1], frecv.at[step, 0], gs_sem.at[step, 1], gr_sem.at[step, 0], nxt)]

    def start_both(copies):
        up, down = copies

        @pl.when(me < n - 1)
        def _():
            up.start()

        @pl.when(me > 0)
        def _():
            down.start()

    def wait_both(copies):
        up, down = copies

        @pl.when(me < n - 1)
        def _():
            up.wait_send()
            down.wait_recv()

        @pl.when(me > 0)
        def _():
            down.wait_send()
            up.wait_recv()

    def send_disp(step, disp):
        for r in range(2):
            for c in range(3):
                g = jnp.where(halo_hi[r] == sub8, lane_take(disp[c], halo_lo[r]), F32(0))
                dsend[step, r, c:c + 1, :] = jnp.sum(g, axis=0, keepdims=True)
        start_both(disp_copies(step))

    def internal(step, disp):
        wait_both(disp_copies(step))
        ghost = [jnp.where(me > 0, drecv[step, 0, 0:3, :], F32(0)), jnp.where(me < n - 1, drecv[step, 1, 0:3, :], F32(0))]
        for c in range(3):
            rows = [disp[c][h:h + 1, :] for h in range(8)] + [ghost[0][c:c + 1, :], ghost[1][c:c + 1, :]]
            rows = [jnp.broadcast_to(r, (8, 128)) for r in rows]
            for at in range(3):
                for e in range(2):
                    lo = con_lo[8 * at:8 * at + 8, 128 * e:128 * e + 128]
                    hi = con_hi[8 * at:8 * at + 8, 128 * e:128 * e + 128]
                    acc = lane_take(rows[0], lo)
                    for h in range(1, 10):
                        acc = jnp.where(hi == h, lane_take(rows[h], lo), acc)
                    u_s[c, 8 * at:8 * at + 8, 128 * e:128 * e + 128] = acc

        def multiply(a, acc):
            for c in range(3):
                acc = acc + kmat[c * 20 + a] * u_s[c, pl.ds(a, 1), :]
            return acc
        force = lax.fori_loop(0, 20, multiply, jnp.zeros((60, 256), F32))
        fh = force.astype(BF16).astype(F32)
        fh_s[...] = fh
        fl_s[...] = force - fh
        sub16 = lax.broadcasted_iota(jnp.int32, (16, 256), 0)
        for a in range(20):
            mask = jnp.broadcast_to(con_hi[a:a + 1, :], (16, 256)) == sub16
            for c in range(3):
                for k, part in enumerate((fh_s, fl_s)):
                    row = jnp.broadcast_to(part[20 * c + a:20 * c + a + 1, :], (16, 256))
                    v_s[48 * k + 16 * c:48 * k + 16 * c + 16, a * 256:a * 256 + 256] = jnp.where(mask, row, F32(0)).astype(BF16)
        both = jnp.dot(v_s[...], oh_e[...], preferred_element_type=F32)
        total = both[:48] + both[48:]
        for k in range(2):
            for c in range(3):
                fsend[step, k, c:c + 1, :] = total[16 * c + 8 + k:16 * c + 9 + k, :]
        start_both(force_copies(step)[::-1])
        return [total[16 * c:16 * c + 8, :] for c in range(3)]

    def advance(step, own, ext, disp, vel):
        wait_both(force_copies(step)[::-1])
        got = [jnp.where(me > 0, frecv[step, 0, 0:3, :], F32(0)), jnp.where(me < n - 1, frecv[step, 1, 0:3, :], F32(0))]
        parts = []
        for c in range(3):
            cols = []
            for r in range(2):
                x = jnp.where(halo_hi[r] == sub8, jnp.broadcast_to(got[r][c:c + 1, :], (8, 128)), F32(0))
                cols.append(x)
            parts.append(jnp.concatenate(cols, axis=1))
        x = jnp.concatenate(parts, axis=0)
        xh = x.astype(BF16).astype(F32)
        lhs = jnp.concatenate([xh, x - xh], axis=0).astype(BF16)
        both = jnp.dot(lhs, oh_h[...], preferred_element_type=F32)
        add = both[:24] + both[24:]
        vel = [vel[c] + (ext[c] - (own[c] + add[8 * c:8 * c + 8, :])) / mass for c in range(3)]
        disp = [disp[c] + vel[c] for c in range(3)]
        return disp, vel

    tiles = n // 8
    mine = me // 8

    def tile_at(k):
        d = k // 4
        step = lax.rem(2 + d + (d // 2) * (2 * d - 3), 4)
        g = lax.rem(gx + 2 * step, nx)
        g = g + (1 - 2 * lax.rem(g, 2)) * (1 - lax.rem(k // 2, 2))
        half = lax.rem(yz // 8 + 1 - lax.rem(k, 2), 2)
        return g, half

    send_disp(0, disp)

    def fwd(g, y):
        return pltpu.make_async_remote_copy(
            src_ref=s_ref.at[g * ny + y], dst_ref=recv.at[me], send_sem=fs_sem, recv_sem=fr_sem.at[mine],
            device_id=(g, y), device_id_type=MESH)

    def fwd_start(k, _):
        g, half = tile_at(k)
        for s in range(8):
            y = half * 8 + lax.rem(yz + s, 8)

            @pl.when(g * ny + y != me)
            def _():
                fwd(g, y).start()
        return 0
    lax.fori_loop(0, tiles, fwd_start, 0)
    recv[me] = s_ref[me]
    for dst in (con_lo, con_hi):
        dst[16:24, :] = jnp.zeros((8, 256), jnp.int32)
    con_lo[0:20, :] = con_ref[...] & 127
    con_hi[0:20, :] = con_ref[...] >> 7
    for a in range(20):
        for e in range(2):
            row = jnp.broadcast_to(con_lo[a:a + 1, 128 * e:128 * e + 128], (128, 128))
            oh_e[a * 256 + 128 * e:a * 256 + 128 * e + 128, :] = jnp.where(row == sub128, F32(1), F32(0)).T.astype(BF16)
    for r in range(2):
        row = jnp.broadcast_to(halo_ref[r:r + 1, :] & 127, (128, 128))
        oh_h[128 * r:128 * r + 128, :] = jnp.where(row == sub128, F32(1), F32(0)).T.astype(BF16)
    kcopy.wait()
    own = internal(0, disp)


    sub128h = lax.broadcasted_iota(jnp.int32, (128, 128), 0).astype(jnp.int16)

    def gather_load(k, acc):
        g, half = tile_at(k)
        source = g * 2 + half
        base = pl.multiple_of(source * 8, 8)
        def arrive(count):
            pltpu.make_async_remote_copy(
                src_ref=s_ref.at[pl.ds(0, count)], dst_ref=recv.at[pl.ds(0, count)], send_sem=fs_sem, recv_sem=fr_sem.at[source],
                device_id=(gx, yz), device_id_type=MESH).wait_recv()

        @pl.when(source == mine)
        def _():
            arrive(7)

        @pl.when(source != mine)
        def _():
            arrive(8)
        get = lambda r: recv[pl.ds(base, 8), r, :]
        loads = []
        for c in range(3):
            t0, t1 = get(2 * c), get(2 * c + 1)
            r0, r1 = pltpu.roll(t0, 64, 1), pltpu.roll(t1, 64, 1)
            loads.append([weights[j][0] * t0 + weights[j][1] * r0 + weights[j][2] * t1 + weights[j][3] * r1 for j in range(4)])
        total = jnp.zeros((48, 128), F32)
        for j in range(4):
            idx = get(6 + j).astype(jnp.int32)
            ids[j, pl.ds(base, 8), :] = idx
            lo, hi = idx & 127, idx >> 7
            highs = [loads[c][j].astype(BF16).astype(F32) for c in range(3)]
            lows = [loads[c][j] - highs[c] for c in range(3)]
            for s in range(0, 8, 2):
                hots, vals = [], []
                for k in (s, s + 1):
                    row = jnp.broadcast_to(lo[k:k + 1, :], (128, 128)).astype(jnp.int16)
                    hots.append(jnp.where(row == sub128h, BF16(1), BF16(0)))
                    mask = jnp.broadcast_to(hi[k:k + 1, :], (8, 128)) == sub8
                    vals.append(jnp.concatenate(
                        [jnp.where(mask, jnp.broadcast_to(p[k:k + 1, :], (8, 128)), F32(0)) for p in highs + lows], axis=0).astype(BF16))
                total = total + lax.dot_general(
                    jnp.concatenate(vals, axis=1), jnp.concatenate(hots, axis=1), (((1,), (1,)), ((), ())), preferred_element_type=F32)
        return acc + total
    both = lax.fori_loop(0, tiles, gather_load, jnp.zeros((48, 128), F32))
    ext = [both[8 * c:8 * c + 8] + both[24 + 8 * c:32 + 8 * c] for c in range(3)]

    disp, vel = advance(0, own, ext, disp, vel)
    for step in range(1, SUBSTEPS):
        send_disp(step, disp)
        own = internal(step, disp)
        disp, vel = advance(step, own, ext, disp, vel)
    for c in range(3):
        for h in range(8):
            nd_ref[c:c + 1, 128 * h:128 * h + 128] = disp[c][h:h + 1, :]
            u_s[c, h:h + 1, 0:128] = disp[c][h:h + 1, :]

    def ret(g, y):
        return pltpu.make_async_remote_copy(
            src_ref=outb.at[g * ny + y], dst_ref=ret_ref.at[me], send_sem=rs_sem, recv_sem=rr_sem,
            device_id=(g, y), device_id_type=MESH)

    def back(k, _):
        g, half = tile_at(k)
        base = pl.multiple_of((g * 2 + half) * 8, 8)
        sums = [[jnp.zeros((8, 128), F32)] * 4 for c in range(3)]
        for j in range(4):
            idx = ids[j, pl.ds(base, 8), :]
            lo, hi = idx & 127, idx >> 7
            masks = [hi == h for h in range(1, 8)]
            for c in range(3):
                acc = lane_take(jnp.broadcast_to(u_s[c, 0:1, 0:128], (8, 128)), lo)
                for h in range(1, 8):
                    acc = jnp.where(masks[h - 1], lane_take(jnp.broadcast_to(u_s[c, h:h + 1, 0:128], (8, 128)), lo), acc)
                sums[c] = [sums[c][m] + weights[j][m] * acc for m in range(4)]
        for c in range(3):
            p0, q0, p1, q1 = sums[c]
            outb[pl.ds(base, 8), 2 * c, :] = p0 + pltpu.roll(q0, 64, 1)
            outb[pl.ds(base, 8), 2 * c + 1, :] = p1 + pltpu.roll(q1, 64, 1)
        for s in range(8):
            y = half * 8 + lax.rem(yz + s, 8)

            @pl.when(g * ny + y != me)
            def _():
                ret(g, y).start()
        return 0
    lax.fori_loop(0, tiles, back, 0)
    ret_ref[me] = outb[me]

    def every(src, dst, ss, rs):
        return pltpu.make_async_remote_copy(
            src_ref=src.at[pl.ds(0, n - 1)], dst_ref=dst.at[pl.ds(0, n - 1)], send_sem=ss, recv_sem=rs,
            device_id=(gx, yz), device_id_type=MESH)
    every(s_ref, recv, fs_sem, fr_sem.at[0]).wait_send()
    last = every(outb, ret_ref, rs_sem, rr_sem)
    last.wait_send()
    last.wait_recv()


def solid(face_block, pressure, local, weight, area, nodes, target, stiffness, connect, halo, mass, disp, vel, nx, ny, shapes):
    n = nx * ny
    V = pl.BlockSpec(memory_space=pltpu.VMEM)
    A = pl.BlockSpec(memory_space=pl.ANY)
    D = pltpu.SemaphoreType.DMA
    M = pltpu.VMEM
    I32 = jnp.int32
    node_disp, back, slot = pl.pallas_call(
        functools.partial(solid_kernel, nx, ny, shapes),
        out_shape=(jax.ShapeDtypeStruct(disp.shape, F32), jax.ShapeDtypeStruct((n, 6, 128), F32), jax.ShapeDtypeStruct(target.shape, I32)),
        in_specs=[pl.BlockSpec(memory_space=pltpu.SMEM), A, A, A, A, A, V, A, V, V, V, V, V],
        out_specs=(V, V, V),
        scratch_shapes=[
            M(pressure.shape, BF16), M(local.shape, I32), M(weight.shape, F32), M(area.shape, F32), M(nodes.shape, I32),
            M(area.shape, F32), M((16 * STRIDE, 128), F32), M((256, 32, 128), BF16), M((1024, 128), I32), M((1024, 128), F32),
            M((1024, 128), F32), M((128, 256), F32), M((640, 256), F32),
            M((n, 10, 128), F32),
            M((n, 10, 128), F32), M((n, 6, 128), F32), M((60, 60, 256), F32),
            M((4, n, 128), I32), M((24, 256), I32), M((24, 256), I32),
            M((3, 24, 256), F32), M((60, 256), F32), M((60, 256), F32),
            M((96, 5120), BF16), M((5120, 128), BF16), M((256, 128), BF16),
            M((SUBSTEPS, 2, 8, 128), F32), M((SUBSTEPS, 2, 8, 128), F32),
            M((SUBSTEPS, 2, 8, 128), F32), M((SUBSTEPS, 2, 8, 128), F32),
            D((5,)), D, D, D((n // 8,)), D, D, D((SUBSTEPS, 2)), D((SUBSTEPS, 2)), D((SUBSTEPS, 2)), D((SUBSTEPS, 2))],
        compiler_params=pltpu.CompilerParams(collective_id=0, has_side_effects=True, vmem_limit_bytes=56 * 2**20),
        name="solid",
    )(face_block, pressure, local, weight, area, nodes, target, stiffness, connect, halo, mass.reshape(1, -1), disp, vel)
    return pl.pallas_call(
        unpack_kernel,
        out_shape=(jax.ShapeDtypeStruct(disp.shape, F32), jax.ShapeDtypeStruct((12, target.shape[1]), F32)),
        in_specs=[V, V, V, V],
        out_specs=(V, V),
        scratch_shapes=[M((768, 256), BF16)],
        compiler_params=pltpu.CompilerParams(vmem_limit_bytes=24 * 2**20),
        name="unpack",
    )(target, slot, back, node_disp)


def shape_table():
    corner_u = [-1, 1, 1, -1, 0, 1, 0, -1]
    corner_v = [-1, -1, 1, 1, -1, 0, 1, 0]
    gauss_point = 1.0 / math.sqrt(3.0)
    points = [
        (-gauss_point, -gauss_point),
        (gauss_point, -gauss_point),
        (gauss_point, gauss_point),
        (-gauss_point, gauss_point),
    ]
    shape_values = np.zeros((4, 8), np.float32)
    for position, (coord_u, coord_v) in enumerate(points):
        for corner in range(8):
            node_u = corner_u[corner]
            node_v = corner_v[corner]
            if corner < 4:
                entry_value = (
                    0.25
                    * (1 + coord_u * node_u)
                    * (1 + coord_v * node_v)
                    * (coord_u * node_u + coord_v * node_v - 1)
                )
            elif node_u == 0:
                entry_value = 0.5 * (1 - coord_u * coord_u) * (1 + coord_v * node_v)
            else:
                entry_value = 0.5 * (1 + coord_u * node_u) * (1 - coord_v * coord_v)
            shape_values[position, corner] = entry_value
    return shape_values


def shards(
    pressure,
    face_block,
    stencil_local,
    stencil_weight,
    area_normal,
    face_part,
    face_nodes,
    stiffness,
    connect,
    halo_nodes,
    node_mass,
    displacement,
    velocity,
):
    gx_size = lax.axis_size("gx")
    yz_size = lax.axis_size("yz")
    return solid(
        face_block, pressure, stencil_local, stencil_weight, area_normal, face_nodes, face_part.reshape(1, -1),
        stiffness, connect, halo_nodes, node_mass, displacement, velocity, gx_size, yz_size, shape_table()
    )


def solution(mesh):
    in_specs = (
        P(("gx", "yz"), None),
        P(("gx", "yz")),
        P(None, ("gx", "yz")),
        P(None, ("gx", "yz")),
        P(None, ("gx", "yz")),
        P(("gx", "yz"), None),
        P(None, ("gx", "yz")),
        P(None, None, ("gx", "yz")),
        P(None, ("gx", "yz")),
        P(None, ("gx", "yz")),
        P(("gx", "yz")),
        P(None, ("gx", "yz")),
        P(None, ("gx", "yz")),
    )
    out_specs = (P(None, ("gx", "yz")), P(None, ("gx", "yz")))
    return jax.shard_map(shards, mesh=mesh, in_specs=in_specs, out_specs=out_specs, check_vma=False)
```

```python
import functools
import math

import jax
import jax.numpy as jnp
import numpy as np
from jax import lax
from jax.experimental import pallas as pl
from jax.experimental.pallas import tpu as pltpu
from jax.sharding import PartitionSpec as P

MESH = pl.DeviceIdType.MESH
F32 = jnp.float32
BF16 = jnp.bfloat16
SUBSTEPS = 4

def half_lanes(left, right):
    lane = lax.broadcasted_iota(jnp.int32, (8, 128), 1)
    return jnp.where(lane < 64, F32(left), F32(right))

def mix_weights(shapes):
    pick = lambda q, a: float(shapes[q, a])
    out = []
    for j in range(4):
        e, o = 2 * j, 2 * j + 1
        out.append((
            half_lanes(pick(0, e), pick(1, o)), half_lanes(pick(1, e), pick(0, o)),
            half_lanes(pick(2, e), pick(3, o)), half_lanes(pick(3, e), pick(2, o))))
    return out

STRIDE = 40
UNR = 32
TAKE = lax.GatherDimensionNumbers(
    offset_dims=(), collapsed_slice_dims=(1,), start_index_map=(1,), operand_batching_dims=(0,), start_indices_batching_dims=(0,)
)

def lane_take(x, idx):
    return lax.gather(x, idx[..., None], TAKE, slice_sizes=(1, 1), mode=lax.GatherScatterMode.PROMISE_IN_BOUNDS)

def stencil_part(fb_ref, pr_ref, loc_ref, w_ref, an_ref, out_ref, tab32, tab, idxt, wt, res, arrive_lists, arrive_blocks):
    arrive_lists()
    for i in range(8):
        idxt[128 * i:128 * i + 128, :] = jnp.concatenate(
            [loc_ref[:, a * 1024 + 128 * i:a * 1024 + 128 * i + 128] for a in range(4)], axis=0).T
        wt[128 * i:128 * i + 128, :] = jnp.concatenate(
            [w_ref[:, a * 1024 + 128 * i:a * 1024 + 128 * i + 128] for a in range(4)], axis=0).T
    arrive_blocks()

    def relayout(b, _):
        r0 = pl.multiple_of(b * 16, 16)
        for t in range(32):
            x = pr_ref[pl.ds(r0, 16), 128 * t:128 * t + 128].astype(jnp.float32)
            tab32[pl.ds(t, 8, stride=STRIDE), :] = x[:8]
            tab32[pl.ds(8 * STRIDE + t, 8, stride=STRIDE), :] = x[8:]
        for n in range(16):
            tab[r0 + n] = tab32[n * STRIDE:n * STRIDE + 32, :].astype(jnp.bfloat16)
        return 0
    lax.fori_loop(0, 16, relayout, 0)
    lane = lax.broadcasted_iota(jnp.int32, (16, 128), 1)
    sub = lax.broadcasted_iota(jnp.int32, (16, 128), 0).astype(jnp.int16)
    grp = (lane // 32).astype(jnp.int16)
    m_lo = grp < 2
    m0 = grp == 0
    m2 = grp == 2

    def main(gg, _):
        for uu in range(UNR // 8):
            base = pl.multiple_of(gg * UNR + 8 * uu, 8)
            rows = []
            for u in range(8):
                g = base + u
                row = jnp.broadcast_to(idxt[pl.ds(g, 1), :], (16, 128))
                lo = (row & 127).astype(jnp.int16)
                hi = (row >> 7).astype(jnp.int16)
                cl = hi < 16
                mine = (hi & 15) == sub
                xs = []
                for a in range(4):
                    block = tab[fb_ref[a * 1024 + g]]
                    xs.append(jnp.where(cl, lane_take(block[:16], lo), lane_take(block[16:], lo)))
                x = jnp.where(m_lo, jnp.where(m0, xs[0], xs[1]), jnp.where(m2, xs[2], xs[3]))
                x = jnp.where(mine, x, jnp.bfloat16(0)).astype(jnp.float32)
                rows.append(jnp.sum(x[:8] + x[8:], axis=0, keepdims=True))
            res[pl.ds(base, 8), :] = jnp.concatenate(rows, axis=0) * wt[pl.ds(base, 8), :]
        return 0
    lax.fori_loop(0, 1024 // UNR, main, 0)
    for i in range(8):
        rt = res[128 * i:128 * i + 128, :].T
        for a in range(4):
            f0 = a * 1024 + 128 * i
            fp = jnp.concatenate([jnp.sum(rt[a * 32 + 8 * q:a * 32 + 8 * q + 8], axis=0, keepdims=True) for q in range(4)], axis=0)
            fp3 = jnp.concatenate([fp, fp, fp], axis=0)
            out_ref[:, f0:f0 + 128] = -(an_ref[:, f0:f0 + 128] * fp3)


def pack_part(tgt_ref, fn_ref, trac, slot_s, carry, acc, send_ref):
    wide = 1024
    rows128 = lax.broadcasted_iota(jnp.int32, (128, 256), 0)
    rows256 = lax.broadcasted_iota(jnp.int32, (256, 256), 0)
    cols256 = lax.broadcasted_iota(jnp.int32, (256, 256), 1)
    rows256w = lax.broadcasted_iota(jnp.int32, (256, wide), 0)
    rows32 = lax.broadcasted_iota(jnp.int32, (32, wide), 0)
    one_if = lambda m: jnp.where(m, F32(1), F32(0)).astype(BF16)
    upper = one_if(rows256 < cols256)
    ones = jnp.ones((256, 256), BF16)
    carry[...] = jnp.zeros_like(carry)
    acc[...] = jnp.zeros_like(acc)

    def rank(kt, _):
        before = carry[...]
        for m in range(4):
            at = pl.ds(pl.multiple_of(kt * wide + 256 * m, 256), 256)
            hit = jnp.broadcast_to(tgt_ref[:, at], (128, 256)) == rows128
            hot = one_if(hit)
            within = jnp.dot(hot, upper, preferred_element_type=F32) + before
            slot_s[:, at] = jnp.sum(jnp.where(hit, within, F32(0)), axis=0, keepdims=True).astype(jnp.int32)
            before = before + jnp.dot(hot, ones, preferred_element_type=F32)
        carry[...] = before
        return 0
    lax.fori_loop(0, 4, rank, 0)

    def tile(kt, _):
        at = pl.ds(pl.multiple_of(kt * wide, wide), wide)
        slot = slot_s[:, at]
        place = jnp.broadcast_to(tgt_ref[:, at] + 128 * (slot >> 5), (256, wide))
        weights = one_if(place == rows256w)
        mask = jnp.broadcast_to(slot & 31, (32, wide)) == rows32
        values = [trac[:, at], fn_ref[:, at].astype(F32)]
        total = None
        highs = [v.astype(BF16).astype(F32) for v in values]
        for part in (highs, [v - h for v, h in zip(values, highs)]):
            x = [
                jnp.where(mask, jnp.broadcast_to(p[r:r + 1, :], (32, wide)), F32(0)).astype(BF16)
                for p in part
                for r in range(p.shape[0])
            ]
            y = lax.dot_general(jnp.concatenate(x, axis=0), weights, (((1,), (1,)), ((), ())), preferred_element_type=F32)
            total = y if total is None else total + y
        acc[...] += total
        return 0
    lax.fori_loop(0, 4, tile, 0)
    for r in range(10):
        block = [acc[32 * v:32 * v + 32, 128 * h:128 * h + 128] for v in (2 * r, 2 * r + 1) for h in range(2)]
        send_ref[:, r, :] = jnp.concatenate(block, axis=0).T


def unpack_kernel(tgt_ref, slot_s, ret_ref, nd_in, nd_ref, fd_ref, lhs):
    nd_ref[...] = nd_in[...]
    wide = 512
    rows128 = lax.broadcasted_iota(jnp.int32, (128, wide), 0)
    rows64 = lax.broadcasted_iota(jnp.int32, (64, wide), 0)
    for r in range(6):
        x = ret_ref[:, r, :].T
        xh = x.astype(BF16).astype(F32)
        lhs[128 * r:128 * r + 128, :] = jnp.concatenate([xh, x - xh], axis=1).astype(BF16)

    def tile(kt, _):
        at = pl.ds(pl.multiple_of(kt * wide, wide), wide)
        hot = jnp.where(jnp.broadcast_to(tgt_ref[:, at], (128, wide)) == rows128, F32(1), F32(0)).astype(BF16)
        y = jnp.dot(lhs[...], jnp.concatenate([hot, hot], axis=0), preferred_element_type=F32)
        mask = jnp.broadcast_to(slot_s[:, at], (64, wide)) == rows64
        fd_ref[:, at] = jnp.concatenate(
            [jnp.sum(jnp.where(mask, y[64 * v:64 * v + 64, :], F32(0)), axis=0, keepdims=True) for v in range(12)], axis=0
        )
        return 0
    lax.fori_loop(0, 8, tile, 0)


def solid_kernel(nx, ny, shapes, fb_ref, pr_hbm, loc_hbm, w_hbm, an_hbm, fn_hbm, tgt_ref, k_hbm, con_ref, halo_ref, mass_ref, disp_ref, vel_ref,
                 nd_ref, ret_ref, slot_s,
                 pr_ref, loc_ref, w_ref, an_ref, fn_ref, trac, tab32, tab, idxt, wt, res, carry, acc_s, s_ref,
                 recv, outb, kmat, ids, con_lo, con_hi, u_s, fh_s, fl_s, v_s, oh_e, oh_h,
                 dsend, drecv, esend, erecv, fsend, frecv, ffar, eq_s,
                 in_sem, k_sem, fs_sem, fr_sem, rs_sem, rr_sem, ds_sem, dr_sem, es_sem, er_sem, gs_sem, gr_sem, hs_sem, hr_sem):
    n = nx * ny
    gx = lax.axis_index("gx")
    yz = lax.axis_index("yz")
    me = gx * ny + yz
    dev = lambda t: (t // ny, lax.rem(t, ny))
    ins = [pltpu.make_async_copy(src, dst, in_sem.at[k]) for k, (src, dst) in enumerate(
        ((loc_hbm, loc_ref), (w_hbm, w_ref), (pr_hbm, pr_ref), (an_hbm, an_ref), (fn_hbm, fn_ref)))]
    for cp in ins:
        cp.start()
    kcopy = pltpu.make_async_copy(k_hbm, kmat, k_sem)
    kcopy.start()
    barrier = pltpu.get_barrier_semaphore()

    gx_at = [lax.rem(gx + a, nx) for a in range(nx)]

    def greet(b, _):
        y = lax.rem(yz + b, ny)
        for a in range(nx):
            pl.semaphore_signal(barrier, inc=1, device_id=(gx_at[a], y), device_id_type=MESH)
        return 0
    lax.fori_loop(1, ny, greet, 0)
    for a in range(1, nx):
        pl.semaphore_signal(barrier, inc=1, device_id=(gx_at[a], yz), device_id_type=MESH)

    sub8 = lax.broadcasted_iota(jnp.int32, (8, 128), 0)
    sub128 = lax.broadcasted_iota(jnp.int32, (128, 128), 0)
    weights = mix_weights(shapes)

    halo_lo = [jnp.broadcast_to(halo_ref[r:r + 1, :] & 127, (8, 128)) for r in range(2)]
    halo_hi = [jnp.broadcast_to(halo_ref[r:r + 1, :] >> 7, (8, 128)) for r in range(2)]
    stack = lambda ref, c: jnp.concatenate([ref[c:c + 1, 128 * h:128 * h + 128] for h in range(8)], axis=0)
    disp = [stack(disp_ref, c) for c in range(3)]
    vel = [stack(vel_ref, c) for c in range(3)]
    mass = stack(mass_ref, 0)

    def arrive_lists():
        ins[0].wait()
        ins[1].wait()

    def arrive_blocks():
        for cp in ins[2:]:
            cp.wait()
    stencil_part(fb_ref, pr_ref, loc_ref, w_ref, an_ref, trac, tab32, tab, idxt, wt, res, arrive_lists, arrive_blocks)
    pack_part(tgt_ref, fn_ref, trac, slot_s, carry, acc_s, s_ref)
    pl.semaphore_wait(barrier, n - 1)

    def near(src, dst, ss, rs, t):
        return pltpu.make_async_remote_copy(src_ref=src, dst_ref=dst, send_sem=ss, recv_sem=rs, device_id=dev(t), device_id_type=MESH)

    def hop(send, recv, ss, rs, dist):
        return (near(send(1), recv(0), ss(1), rs(0), lax.rem(me + dist, n)),
                near(send(0), recv(1), ss(0), rs(1), lax.rem(me + n - dist, n)), dist)

    def start_both(copies):
        up, down, dist = copies

        @pl.when(me < n - dist)
        def _():
            up.start()

        @pl.when(me >= dist)
        def _():
            down.start()

    def wait_both(copies):
        up, down, dist = copies

        @pl.when(me < n - dist)
        def _():
            up.wait_send()
            down.wait_recv()

        @pl.when(me >= dist)
        def _():
            down.wait_send()
            up.wait_recv()

    at = lambda ref, *lead: lambda side: ref.at[(*lead, side)]
    state_copies = hop(at(dsend), at(drecv), at(ds_sem), at(dr_sem), 1)
    load_copies = hop(at(esend), at(erecv), at(es_sem), at(er_sem), 1)
    force_copies = lambda step: hop(at(fsend, step), at(frecv, step), at(gs_sem, step), at(gr_sem, step), 1)
    far_copies = lambda step: hop(at(fsend, step), at(ffar, step), at(hs_sem, step), at(hr_sem, step), 2)
    exists = [me > 0, me < n - 1]
    exists_far = [me > 1, me < n - 2]

    def pick(r, x):
        g = jnp.where(halo_hi[r] == sub8, lane_take(x, halo_lo[r]), F32(0))
        return jnp.sum(g, axis=0, keepdims=True)

    def send_state():
        for r in range(2):
            for c in range(3):
                dsend[r, c:c + 1, :] = pick(r, disp[c])
                dsend[r, 3 + c:4 + c, :] = pick(r, vel[c])
            dsend[r, 6:7, :] = pick(r, mass)
            dsend[r, 8:10, :] = halo_ref[...].astype(F32)
        start_both(state_copies)

    def ghost_state():
        wait_both(state_copies)
        gd = [jnp.where(exists[k], drecv[k, 0:3, :], F32(0)) for k in range(2)]
        gv = [jnp.where(exists[k], drecv[k, 3:6, :], F32(0)) for k in range(2)]
        gm = [jnp.where(exists[k], drecv[k, 6:7, :], F32(1)) for k in range(2)]
        for k in range(2):
            held, other = drecv[k, 9 - k:10 - k, :], drecv[k, 8 + k:9 + k, :]
            for m, x in enumerate((held, other)):
                same = jnp.broadcast_to(x, (128, 128)).T == jnp.broadcast_to(held, (128, 128))
                eq_s[k, 128 * m:128 * m + 128, :] = jnp.where(same, F32(1), F32(0)).astype(BF16)
        return gd, gv, gm

    def advance_ghosts(step, ge, gd, gv, gm):
        wait_both(far_copies(step))
        for k in range(2):
            x = jnp.concatenate([fsend[step, k], jnp.where(exists_far[k], ffar[step, k], F32(0))], axis=1)
            xh = x.astype(BF16).astype(F32)
            both = jnp.dot(jnp.concatenate([xh, x - xh], axis=0).astype(BF16), eq_s[k], preferred_element_type=F32)
            total = frecv[step, k, 3:6, :] + (both[0:3] + both[8:11])
            v = gv[k] + (ge[k] - total) / gm[k]
            gv[k] = jnp.where(exists[k], v, F32(0))
            gd[k] = gd[k] + gv[k]

    def internal(step, disp, ghost):
        for c in range(3):
            rows = [disp[c][h:h + 1, :] for h in range(8)] + [ghost[0][c:c + 1, :], ghost[1][c:c + 1, :]]
            rows = [jnp.broadcast_to(r, (8, 128)) for r in rows]
            for at in range(3):
                for e in range(2):
                    lo = con_lo[8 * at:8 * at + 8, 128 * e:128 * e + 128]
                    hi = con_hi[8 * at:8 * at + 8, 128 * e:128 * e + 128]
                    acc = lane_take(rows[0], lo)
                    for h in range(1, 10):
                        acc = jnp.where(hi == h, lane_take(rows[h], lo), acc)
                    u_s[c, 8 * at:8 * at + 8, 128 * e:128 * e + 128] = acc

        def multiply(a, acc):
            for c in range(3):
                acc = acc + kmat[c * 20 + a] * u_s[c, pl.ds(a, 1), :]
            return acc
        force = lax.fori_loop(0, 20, multiply, jnp.zeros((60, 256), F32))
        fh = force.astype(BF16).astype(F32)
        fh_s[...] = fh
        fl_s[...] = force - fh
        sub16 = lax.broadcasted_iota(jnp.int32, (16, 256), 0)
        for a in range(20):
            mask = jnp.broadcast_to(con_hi[a:a + 1, :], (16, 256)) == sub16
            for c in range(3):
                for k, part in enumerate((fh_s, fl_s)):
                    row = jnp.broadcast_to(part[20 * c + a:20 * c + a + 1, :], (16, 256))
                    v_s[48 * k + 16 * c:48 * k + 16 * c + 16, a * 256:a * 256 + 256] = jnp.where(mask, row, F32(0)).astype(BF16)
        both = jnp.dot(v_s[...], oh_e[...], preferred_element_type=F32)
        total = both[:48] + both[48:]
        own = [total[16 * c:16 * c + 8, :] for c in range(3)]
        for k in range(2):
            for c in range(3):
                fsend[step, k, c:c + 1, :] = total[16 * c + 8 + k:16 * c + 9 + k, :]
                fsend[step, k, 3 + c:4 + c, :] = pick(k, own[c])
            fsend[step, k, 6:8, :] = jnp.zeros((2, 128), F32)
        start_both(force_copies(step))
        if step < SUBSTEPS - 1:
            start_both(far_copies(step))
        return own

    def advance(step, own, ext, disp, vel):
        wait_both(force_copies(step))
        got = [jnp.where(me > 0, frecv[step, 0, 0:3, :], F32(0)), jnp.where(me < n - 1, frecv[step, 1, 0:3, :], F32(0))]
        parts = []
        for c in range(3):
            cols = []
            for r in range(2):
                x = jnp.where(halo_hi[r] == sub8, jnp.broadcast_to(got[r][c:c + 1, :], (8, 128)), F32(0))
                cols.append(x)
            parts.append(jnp.concatenate(cols, axis=1))
        x = jnp.concatenate(parts, axis=0)
        xh = x.astype(BF16).astype(F32)
        lhs = jnp.concatenate([xh, x - xh], axis=0).astype(BF16)
        both = jnp.dot(lhs, oh_h[...], preferred_element_type=F32)
        add = both[:24] + both[24:]
        vel = [vel[c] + (ext[c] - (own[c] + add[8 * c:8 * c + 8, :])) / mass for c in range(3)]
        disp = [disp[c] + vel[c] for c in range(3)]
        return disp, vel

    tiles = n // 8
    mine = me // 8

    def tile_at(k):
        d = k // 4
        step = lax.rem(2 + d + (d // 2) * (2 * d - 3), 4)
        g = lax.rem(gx + 2 * step, nx)
        g = g + (1 - 2 * lax.rem(g, 2)) * (1 - lax.rem(k // 2, 2))
        half = lax.rem(yz // 8 + 1 - lax.rem(k, 2), 2)
        return g, half

    send_state()

    def fwd(g, y):
        return pltpu.make_async_remote_copy(
            src_ref=s_ref.at[g * ny + y], dst_ref=recv.at[me], send_sem=fs_sem, recv_sem=fr_sem.at[mine],
            device_id=(g, y), device_id_type=MESH)

    def fwd_start(k, _):
        g, half = tile_at(k)
        for s in range(8):
            y = half * 8 + lax.rem(yz + s, 8)

            @pl.when(g * ny + y != me)
            def _():
                fwd(g, y).start()
        return 0
    lax.fori_loop(0, tiles, fwd_start, 0)
    recv[me] = s_ref[me]
    for dst in (con_lo, con_hi):
        dst[16:24, :] = jnp.zeros((8, 256), jnp.int32)
    con_lo[0:20, :] = con_ref[...] & 127
    con_hi[0:20, :] = con_ref[...] >> 7
    for a in range(20):
        for e in range(2):
            row = jnp.broadcast_to(con_lo[a:a + 1, 128 * e:128 * e + 128], (128, 128))
            oh_e[a * 256 + 128 * e:a * 256 + 128 * e + 128, :] = jnp.where(row == sub128, F32(1), F32(0)).T.astype(BF16)
    for r in range(2):
        row = jnp.broadcast_to(halo_ref[r:r + 1, :] & 127, (128, 128))
        oh_h[128 * r:128 * r + 128, :] = jnp.where(row == sub128, F32(1), F32(0)).T.astype(BF16)
    kcopy.wait()
    gd, gv, gm = ghost_state()
    own = internal(0, disp, gd)


    sub128h = lax.broadcasted_iota(jnp.int32, (128, 128), 0).astype(jnp.int16)

    def gather_load(k, acc):
        g, half = tile_at(k)
        source = g * 2 + half
        base = pl.multiple_of(source * 8, 8)
        def arrive(count):
            pltpu.make_async_remote_copy(
                src_ref=s_ref.at[pl.ds(0, count)], dst_ref=recv.at[pl.ds(0, count)], send_sem=fs_sem, recv_sem=fr_sem.at[source],
                device_id=(gx, yz), device_id_type=MESH).wait_recv()

        @pl.when(source == mine)
        def _():
            arrive(7)

        @pl.when(source != mine)
        def _():
            arrive(8)
        get = lambda r: recv[pl.ds(base, 8), r, :]
        loads = []
        for c in range(3):
            t0, t1 = get(2 * c), get(2 * c + 1)
            r0, r1 = pltpu.roll(t0, 64, 1), pltpu.roll(t1, 64, 1)
            loads.append([weights[j][0] * t0 + weights[j][1] * r0 + weights[j][2] * t1 + weights[j][3] * r1 for j in range(4)])
        total = jnp.zeros((48, 128), F32)
        for j in range(4):
            idx = get(6 + j).astype(jnp.int32)
            ids[j, pl.ds(base, 8), :] = idx
            lo, hi = idx & 127, idx >> 7
            highs = [loads[c][j].astype(BF16).astype(F32) for c in range(3)]
            lows = [loads[c][j] - highs[c] for c in range(3)]
            for s in range(0, 8, 2):
                hots, vals = [], []
                for k in (s, s + 1):
                    row = jnp.broadcast_to(lo[k:k + 1, :], (128, 128)).astype(jnp.int16)
                    hots.append(jnp.where(row == sub128h, BF16(1), BF16(0)))
                    mask = jnp.broadcast_to(hi[k:k + 1, :], (8, 128)) == sub8
                    vals.append(jnp.concatenate(
                        [jnp.where(mask, jnp.broadcast_to(p[k:k + 1, :], (8, 128)), F32(0)) for p in highs + lows], axis=0).astype(BF16))
                total = total + lax.dot_general(
                    jnp.concatenate(vals, axis=1), jnp.concatenate(hots, axis=1), (((1,), (1,)), ((), ())), preferred_element_type=F32)
        return acc + total
    both = lax.fori_loop(0, tiles, gather_load, jnp.zeros((48, 128), F32))
    ext = [both[8 * c:8 * c + 8] + both[24 + 8 * c:32 + 8 * c] for c in range(3)]

    for r in range(2):
        for c in range(3):
            esend[r, c:c + 1, :] = pick(r, ext[c])
        esend[r, 3:8, :] = jnp.zeros((5, 128), F32)
    start_both(load_copies)
    disp, vel = advance(0, own, ext, disp, vel)
    wait_both(load_copies)
    ge = [jnp.where(exists[k], erecv[k, 0:3, :], F32(0)) for k in range(2)]
    advance_ghosts(0, ge, gd, gv, gm)
    for step in range(1, SUBSTEPS):
        own = internal(step, disp, gd)
        disp, vel = advance(step, own, ext, disp, vel)
        if step < SUBSTEPS - 1:
            advance_ghosts(step, ge, gd, gv, gm)
    for c in range(3):
        for h in range(8):
            nd_ref[c:c + 1, 128 * h:128 * h + 128] = disp[c][h:h + 1, :]
            u_s[c, h:h + 1, 0:128] = disp[c][h:h + 1, :]

    def ret(g, y):
        return pltpu.make_async_remote_copy(
            src_ref=outb.at[g * ny + y], dst_ref=ret_ref.at[me], send_sem=rs_sem, recv_sem=rr_sem,
            device_id=(g, y), device_id_type=MESH)

    def back(k, _):
        g, half = tile_at(k)
        base = pl.multiple_of((g * 2 + half) * 8, 8)
        sums = [[jnp.zeros((8, 128), F32)] * 4 for c in range(3)]
        for j in range(4):
            idx = ids[j, pl.ds(base, 8), :]
            lo, hi = idx & 127, idx >> 7
            masks = [hi == h for h in range(1, 8)]
            for c in range(3):
                acc = lane_take(jnp.broadcast_to(u_s[c, 0:1, 0:128], (8, 128)), lo)
                for h in range(1, 8):
                    acc = jnp.where(masks[h - 1], lane_take(jnp.broadcast_to(u_s[c, h:h + 1, 0:128], (8, 128)), lo), acc)
                sums[c] = [sums[c][m] + weights[j][m] * acc for m in range(4)]
        for c in range(3):
            p0, q0, p1, q1 = sums[c]
            outb[pl.ds(base, 8), 2 * c, :] = p0 + pltpu.roll(q0, 64, 1)
            outb[pl.ds(base, 8), 2 * c + 1, :] = p1 + pltpu.roll(q1, 64, 1)
        for s in range(8):
            y = half * 8 + lax.rem(yz + s, 8)

            @pl.when(g * ny + y != me)
            def _():
                ret(g, y).start()
        return 0
    lax.fori_loop(0, tiles, back, 0)
    ret_ref[me] = outb[me]

    def every(src, dst, ss, rs):
        return pltpu.make_async_remote_copy(
            src_ref=src.at[pl.ds(0, n - 1)], dst_ref=dst.at[pl.ds(0, n - 1)], send_sem=ss, recv_sem=rs,
            device_id=(gx, yz), device_id_type=MESH)
    every(s_ref, recv, fs_sem, fr_sem.at[0]).wait_send()
    last = every(outb, ret_ref, rs_sem, rr_sem)
    last.wait_send()
    last.wait_recv()


def solid(face_block, pressure, local, weight, area, nodes, target, stiffness, connect, halo, mass, disp, vel, nx, ny, shapes):
    n = nx * ny
    V = pl.BlockSpec(memory_space=pltpu.VMEM)
    A = pl.BlockSpec(memory_space=pl.ANY)
    D = pltpu.SemaphoreType.DMA
    M = pltpu.VMEM
    I32 = jnp.int32
    node_disp, back, slot = pl.pallas_call(
        functools.partial(solid_kernel, nx, ny, shapes),
        out_shape=(jax.ShapeDtypeStruct(disp.shape, F32), jax.ShapeDtypeStruct((n, 6, 128), F32), jax.ShapeDtypeStruct(target.shape, I32)),
        in_specs=[pl.BlockSpec(memory_space=pltpu.SMEM), A, A, A, A, A, V, A, V, V, V, V, V],
        out_specs=(V, V, V),
        scratch_shapes=[
            M(pressure.shape, BF16), M(local.shape, I32), M(weight.shape, F32), M(area.shape, F32), M(nodes.shape, I32),
            M(area.shape, F32), M((16 * STRIDE, 128), F32), M((256, 32, 128), BF16), M((1024, 128), I32), M((1024, 128), F32),
            M((1024, 128), F32), M((128, 256), F32), M((640, 256), F32),
            M((n, 10, 128), F32),
            M((n, 10, 128), F32), M((n, 6, 128), F32), M((60, 60, 256), F32),
            M((4, n, 128), I32), M((24, 256), I32), M((24, 256), I32),
            M((3, 24, 256), F32), M((60, 256), F32), M((60, 256), F32),
            M((96, 5120), BF16), M((5120, 128), BF16), M((256, 128), BF16),
            M((2, 16, 128), F32), M((2, 16, 128), F32), M((2, 8, 128), F32), M((2, 8, 128), F32),
            M((SUBSTEPS, 2, 8, 128), F32), M((SUBSTEPS, 2, 8, 128), F32), M((SUBSTEPS, 2, 8, 128), F32), M((2, 256, 128), BF16),
            D((5,)), D, D, D((n // 8,)), D, D, D((2,)), D((2,)), D((2,)), D((2,)),
            D((SUBSTEPS, 2)), D((SUBSTEPS, 2)), D((SUBSTEPS, 2)), D((SUBSTEPS, 2))],
        compiler_params=pltpu.CompilerParams(collective_id=0, has_side_effects=True, vmem_limit_bytes=56 * 2**20),
        name="solid",
    )(face_block, pressure, local, weight, area, nodes, target, stiffness, connect, halo, mass.reshape(1, -1), disp, vel)
    return pl.pallas_call(
        unpack_kernel,
        out_shape=(jax.ShapeDtypeStruct(disp.shape, F32), jax.ShapeDtypeStruct((12, target.shape[1]), F32)),
        in_specs=[V, V, V, V],
        out_specs=(V, V),
        scratch_shapes=[M((768, 256), BF16)],
        compiler_params=pltpu.CompilerParams(vmem_limit_bytes=24 * 2**20),
        name="unpack",
    )(target, slot, back, node_disp)


def shape_table():
    corner_u = [-1, 1, 1, -1, 0, 1, 0, -1]
    corner_v = [-1, -1, 1, 1, -1, 0, 1, 0]
    gauss_point = 1.0 / math.sqrt(3.0)
    points = [
        (-gauss_point, -gauss_point),
        (gauss_point, -gauss_point),
        (gauss_point, gauss_point),
        (-gauss_point, gauss_point),
    ]
    shape_values = np.zeros((4, 8), np.float32)
    for position, (coord_u, coord_v) in enumerate(points):
        for corner in range(8):
            node_u = corner_u[corner]
            node_v = corner_v[corner]
            if corner < 4:
                entry_value = (
                    0.25
                    * (1 + coord_u * node_u)
                    * (1 + coord_v * node_v)
                    * (coord_u * node_u + coord_v * node_v - 1)
                )
            elif node_u == 0:
                entry_value = 0.5 * (1 - coord_u * coord_u) * (1 + coord_v * node_v)
            else:
                entry_value = 0.5 * (1 + coord_u * node_u) * (1 - coord_v * coord_v)
            shape_values[position, corner] = entry_value
    return shape_values


def shards(
    pressure,
    face_block,
    stencil_local,
    stencil_weight,
    area_normal,
    face_part,
    face_nodes,
    stiffness,
    connect,
    halo_nodes,
    node_mass,
    displacement,
    velocity,
):
    gx_size = lax.axis_size("gx")
    yz_size = lax.axis_size("yz")
    return solid(
        face_block, pressure, stencil_local, stencil_weight, area_normal, face_nodes, face_part.reshape(1, -1),
        stiffness, connect, halo_nodes, node_mass, displacement, velocity, gx_size, yz_size, shape_table()
    )


def solution(mesh):
    in_specs = (
        P(("gx", "yz"), None),
        P(("gx", "yz")),
        P(None, ("gx", "yz")),
        P(None, ("gx", "yz")),
        P(None, ("gx", "yz")),
        P(("gx", "yz"), None),
        P(None, ("gx", "yz")),
        P(None, None, ("gx", "yz")),
        P(None, ("gx", "yz")),
        P(None, ("gx", "yz")),
        P(("gx", "yz")),
        P(None, ("gx", "yz")),
        P(None, ("gx", "yz")),
    )
    out_specs = (P(None, ("gx", "yz")), P(None, ("gx", "yz")))
    return jax.shard_map(shards, mesh=mesh, in_specs=in_specs, out_specs=out_specs, check_vma=False)
```

```python
import functools
import math

import jax
import jax.numpy as jnp
import numpy as np
from jax import lax
from jax.experimental import pallas as pl
from jax.experimental.pallas import tpu as pltpu
from jax.sharding import PartitionSpec as P

MESH = pl.DeviceIdType.MESH
F32 = jnp.float32
BF16 = jnp.bfloat16
SUBSTEPS = 4

def half_lanes(left, right):
    lane = lax.broadcasted_iota(jnp.int32, (8, 128), 1)
    return jnp.where(lane < 64, F32(left), F32(right))

def mix_weights(shapes):
    pick = lambda q, a: float(shapes[q, a])
    out = []
    for j in range(4):
        e, o = 2 * j, 2 * j + 1
        out.append((
            half_lanes(pick(0, e), pick(1, o)), half_lanes(pick(1, e), pick(0, o)),
            half_lanes(pick(2, e), pick(3, o)), half_lanes(pick(3, e), pick(2, o))))
    return out

STRIDE = 40
UNR = 64
TAKE = lax.GatherDimensionNumbers(
    offset_dims=(), collapsed_slice_dims=(1,), start_index_map=(1,), operand_batching_dims=(0,), start_indices_batching_dims=(0,)
)

def lane_take(x, idx):
    return lax.gather(x, idx[..., None], TAKE, slice_sizes=(1, 1), mode=lax.GatherScatterMode.PROMISE_IN_BOUNDS)

def stencil_part(fb_ref, pr_ref, loc_ref, w_ref, an_ref, out_ref, tab32, tab, idxt, wt, res, arrive_lists, arrive_blocks):
    arrive_lists()
    for i in range(8):
        idxt[128 * i:128 * i + 128, :] = jnp.concatenate(
            [loc_ref[:, a * 1024 + 128 * i:a * 1024 + 128 * i + 128] for a in range(4)], axis=0).T
        wt[128 * i:128 * i + 128, :] = jnp.concatenate(
            [w_ref[:, a * 1024 + 128 * i:a * 1024 + 128 * i + 128] for a in range(4)], axis=0).T
    arrive_blocks()

    def relayout(b, _):
        r0 = pl.multiple_of(b * 16, 16)
        for t in range(32):
            x = pr_ref[pl.ds(r0, 16), 128 * t:128 * t + 128].astype(jnp.float32)
            tab32[pl.ds(t, 8, stride=STRIDE), :] = x[:8]
            tab32[pl.ds(8 * STRIDE + t, 8, stride=STRIDE), :] = x[8:]
        for n in range(16):
            tab[r0 + n] = tab32[n * STRIDE:n * STRIDE + 32, :].astype(jnp.bfloat16)
        return 0
    lax.fori_loop(0, 16, relayout, 0)
    lane = lax.broadcasted_iota(jnp.int32, (16, 128), 1)
    sub = lax.broadcasted_iota(jnp.int32, (16, 128), 0).astype(jnp.int16)
    grp = (lane // 32).astype(jnp.int16)
    m_lo = grp < 2
    m0 = grp == 0
    m2 = grp == 2

    def main(gg, _):
        for uu in range(UNR // 8):
            base = pl.multiple_of(gg * UNR + 8 * uu, 8)
            rows = []
            for u in range(8):
                g = base + u
                row = jnp.broadcast_to(idxt[pl.ds(g, 1), :], (16, 128))
                lo = (row & 127).astype(jnp.int16)
                hi = (row >> 7).astype(jnp.int16)
                cl = hi < 16
                mine = (hi & 15) == sub
                xs = []
                for a in range(4):
                    block = tab[fb_ref[a * 1024 + g]]
                    xs.append(jnp.where(cl, lane_take(block[:16], lo), lane_take(block[16:], lo)))
                x = jnp.where(m_lo, jnp.where(m0, xs[0], xs[1]), jnp.where(m2, xs[2], xs[3]))
                x = jnp.where(mine, x, jnp.bfloat16(0)).astype(jnp.float32)
                rows.append(jnp.sum(x[:8] + x[8:], axis=0, keepdims=True))
            res[pl.ds(base, 8), :] = jnp.concatenate(rows, axis=0) * wt[pl.ds(base, 8), :]
        return 0
    lax.fori_loop(0, 1024 // UNR, main, 0)
    for i in range(8):
        rt = res[128 * i:128 * i + 128, :].T
        for a in range(4):
            f0 = a * 1024 + 128 * i
            fp = jnp.concatenate([jnp.sum(rt[a * 32 + 8 * q:a * 32 + 8 * q + 8], axis=0, keepdims=True) for q in range(4)], axis=0)
            fp3 = jnp.concatenate([fp, fp, fp], axis=0)
            out_ref[:, f0:f0 + 128] = -(an_ref[:, f0:f0 + 128] * fp3)


def pack_part(tgt_ref, fn_ref, trac, slot_s, carry, acc, send_ref):
    wide = 1024
    rows128 = lax.broadcasted_iota(jnp.int32, (128, 256), 0)
    rows256 = lax.broadcasted_iota(jnp.int32, (256, 256), 0)
    cols256 = lax.broadcasted_iota(jnp.int32, (256, 256), 1)
    rows256w = lax.broadcasted_iota(jnp.int32, (256, wide), 0)
    rows32 = lax.broadcasted_iota(jnp.int32, (32, wide), 0)
    one_if = lambda m: jnp.where(m, F32(1), F32(0)).astype(BF16)
    upper = one_if(rows256 < cols256)
    ones = jnp.ones((256, 256), BF16)
    carry[...] = jnp.zeros_like(carry)
    acc[...] = jnp.zeros_like(acc)

    def rank(kt, _):
        before = carry[...]
        for m in range(4):
            at = pl.ds(pl.multiple_of(kt * wide + 256 * m, 256), 256)
            hit = jnp.broadcast_to(tgt_ref[:, at], (128, 256)) == rows128
            hot = one_if(hit)
            within = jnp.dot(hot, upper, preferred_element_type=F32) + before
            slot_s[:, at] = jnp.sum(jnp.where(hit, within, F32(0)), axis=0, keepdims=True).astype(jnp.int32)
            before = before + jnp.dot(hot, ones, preferred_element_type=F32)
        carry[...] = before
        return 0
    lax.fori_loop(0, 4, rank, 0)

    def tile(kt, _):
        at = pl.ds(pl.multiple_of(kt * wide, wide), wide)
        slot = slot_s[:, at]
        place = jnp.broadcast_to(tgt_ref[:, at] + 128 * (slot >> 5), (256, wide))
        weights = one_if(place == rows256w)
        mask = jnp.broadcast_to(slot & 31, (32, wide)) == rows32
        values = [trac[:, at], fn_ref[:, at].astype(F32)]
        total = None
        highs = [v.astype(BF16).astype(F32) for v in values]
        for part in (highs, [v - h for v, h in zip(values, highs)]):
            x = [
                jnp.where(mask, jnp.broadcast_to(p[r:r + 1, :], (32, wide)), F32(0)).astype(BF16)
                for p in part
                for r in range(p.shape[0])
            ]
            y = lax.dot_general(jnp.concatenate(x, axis=0), weights, (((1,), (1,)), ((), ())), preferred_element_type=F32)
            total = y if total is None else total + y
        acc[...] += total
        return 0
    lax.fori_loop(0, 4, tile, 0)
    for r in range(10):
        block = [acc[32 * v:32 * v + 32, 128 * h:128 * h + 128] for v in (2 * r, 2 * r + 1) for h in range(2)]
        send_ref[:, r, :] = jnp.concatenate(block, axis=0).T


def unpack_kernel(n, tgt_ref, ret_ref, nd_ref, fd_ref, slot_s, lhs):
    for r in range(56):
        row = ret_ref[n + r // 6, r % 6:r % 6 + 1, :]
        if r < 32:
            slot_s[:, 128 * r:128 * r + 128] = row.astype(jnp.int32)
        else:
            c, h = divmod(r - 32, 8)
            nd_ref[c:c + 1, 128 * h:128 * h + 128] = row
    wide = 512
    rows128 = lax.broadcasted_iota(jnp.int32, (128, wide), 0)
    rows64 = lax.broadcasted_iota(jnp.int32, (64, wide), 0)
    for r in range(6):
        x = ret_ref[0:n, r, :].T
        xh = x.astype(BF16).astype(F32)
        lhs[128 * r:128 * r + 128, :] = jnp.concatenate([xh, x - xh], axis=1).astype(BF16)

    def tile(kt, _):
        at = pl.ds(pl.multiple_of(kt * wide, wide), wide)
        hot = jnp.where(jnp.broadcast_to(tgt_ref[:, at], (128, wide)) == rows128, F32(1), F32(0)).astype(BF16)
        y = jnp.dot(lhs[...], jnp.concatenate([hot, hot], axis=0), preferred_element_type=F32)
        mask = jnp.broadcast_to(slot_s[:, at], (64, wide)) == rows64
        fd_ref[:, at] = jnp.concatenate(
            [jnp.sum(jnp.where(mask, y[64 * v:64 * v + 64, :], F32(0)), axis=0, keepdims=True) for v in range(12)], axis=0
        )
        return 0
    lax.fori_loop(0, 8, tile, 0)


def solid_kernel(nx, ny, shapes, fb_ref, pr_hbm, loc_hbm, w_hbm, an_hbm, fn_hbm, tgt_ref, k_hbm, con_ref, halo_ref, mass_ref, disp_ref, vel_ref,
                 ret_ref,
                 pr_ref, loc_ref, w_ref, an_ref, fn_ref, trac, tab32, tab, idxt, wt, res, slot_s, carry, acc_s, s_ref,
                 recv, outb, kmat, ids, con_lo, con_hi, u_s, fh_s, fl_s, v_s, oh_e, oh_h,
                 dsend, drecv, esend, erecv, fsend, frecv, ffar, eq_s,
                 in_sem, k_sem, fs_sem, fr_sem, rs_sem, rr_sem, ds_sem, dr_sem, es_sem, er_sem, gs_sem, gr_sem, hs_sem, hr_sem):
    n = nx * ny
    gx = lax.axis_index("gx")
    yz = lax.axis_index("yz")
    me = gx * ny + yz
    dev = lambda t: (t // ny, lax.rem(t, ny))
    ins = [pltpu.make_async_copy(src, dst, in_sem.at[k]) for k, (src, dst) in enumerate(
        ((loc_hbm, loc_ref), (w_hbm, w_ref), (pr_hbm, pr_ref), (an_hbm, an_ref), (fn_hbm, fn_ref)))]
    for cp in ins:
        cp.start()
    kcopy = pltpu.make_async_copy(k_hbm, kmat, k_sem)
    kcopy.start()
    barrier = pltpu.get_barrier_semaphore()

    gx_at = [lax.rem(gx + a, nx) for a in range(nx)]

    def greet(b, _):
        y = lax.rem(yz + b, ny)
        for a in range(nx):
            pl.semaphore_signal(barrier, inc=1, device_id=(gx_at[a], y), device_id_type=MESH)
        return 0
    lax.fori_loop(1, ny, greet, 0)
    for a in range(1, nx):
        pl.semaphore_signal(barrier, inc=1, device_id=(gx_at[a], yz), device_id_type=MESH)

    sub8 = lax.broadcasted_iota(jnp.int32, (8, 128), 0)
    sub128 = lax.broadcasted_iota(jnp.int32, (128, 128), 0)
    weights = mix_weights(shapes)

    halo_lo = [jnp.broadcast_to(halo_ref[r:r + 1, :] & 127, (8, 128)) for r in range(2)]
    halo_hi = [jnp.broadcast_to(halo_ref[r:r + 1, :] >> 7, (8, 128)) for r in range(2)]
    stack = lambda ref, c: jnp.concatenate([ref[c:c + 1, 128 * h:128 * h + 128] for h in range(8)], axis=0)
    disp = [stack(disp_ref, c) for c in range(3)]
    vel = [stack(vel_ref, c) for c in range(3)]
    mass = stack(mass_ref, 0)

    def arrive_lists():
        ins[0].wait()
        ins[1].wait()

    def arrive_blocks():
        for cp in ins[2:]:
            cp.wait()
    stencil_part(fb_ref, pr_ref, loc_ref, w_ref, an_ref, trac, tab32, tab, idxt, wt, res, arrive_lists, arrive_blocks)
    pack_part(tgt_ref, fn_ref, trac, slot_s, carry, acc_s, s_ref)
    pl.semaphore_wait(barrier, n - 1)

    def near(src, dst, ss, rs, t):
        return pltpu.make_async_remote_copy(src_ref=src, dst_ref=dst, send_sem=ss, recv_sem=rs, device_id=dev(t), device_id_type=MESH)

    def hop(send, recv, ss, rs, dist):
        return (near(send(1), recv(0), ss(1), rs(0), lax.rem(me + dist, n)),
                near(send(0), recv(1), ss(0), rs(1), lax.rem(me + n - dist, n)), dist)

    def start_both(copies):
        up, down, dist = copies

        @pl.when(me < n - dist)
        def _():
            up.start()

        @pl.when(me >= dist)
        def _():
            down.start()

    def wait_both(copies):
        up, down, dist = copies

        @pl.when(me < n - dist)
        def _():
            up.wait_send()
            down.wait_recv()

        @pl.when(me >= dist)
        def _():
            down.wait_send()
            up.wait_recv()

    at = lambda ref, *lead: lambda side: ref.at[(*lead, side)]
    state_copies = hop(at(dsend), at(drecv), at(ds_sem), at(dr_sem), 1)
    load_copies = hop(at(esend), at(erecv), at(es_sem), at(er_sem), 1)
    force_copies = lambda step: hop(at(fsend, step), at(frecv, step), at(gs_sem, step), at(gr_sem, step), 1)
    far_copies = lambda step: hop(at(fsend, step), at(ffar, step), at(hs_sem, step), at(hr_sem, step), 2)
    exists = [me > 0, me < n - 1]
    exists_far = [me > 1, me < n - 2]

    def pick(r, x):
        g = jnp.where(halo_hi[r] == sub8, lane_take(x, halo_lo[r]), F32(0))
        return jnp.sum(g, axis=0, keepdims=True)

    def send_state():
        for r in range(2):
            for c in range(3):
                dsend[r, c:c + 1, :] = pick(r, disp[c])
                dsend[r, 3 + c:4 + c, :] = pick(r, vel[c])
            dsend[r, 6:7, :] = pick(r, mass)
            dsend[r, 8:10, :] = halo_ref[...].astype(F32)
        start_both(state_copies)

    def ghost_state():
        wait_both(state_copies)
        gd = [jnp.where(exists[k], drecv[k, 0:3, :], F32(0)) for k in range(2)]
        gv = [jnp.where(exists[k], drecv[k, 3:6, :], F32(0)) for k in range(2)]
        gm = [jnp.where(exists[k], drecv[k, 6:7, :], F32(1)) for k in range(2)]
        for k in range(2):
            held, other = drecv[k, 9 - k:10 - k, :], drecv[k, 8 + k:9 + k, :]
            for m, x in enumerate((held, other)):
                same = jnp.broadcast_to(x, (128, 128)).T == jnp.broadcast_to(held, (128, 128))
                eq_s[k, 128 * m:128 * m + 128, :] = jnp.where(same, F32(1), F32(0)).astype(BF16)
        return gd, gv, gm

    def advance_ghosts(step, ge, gd, gv, gm):
        wait_both(far_copies(step))
        for k in range(2):
            x = jnp.concatenate([fsend[step, k], jnp.where(exists_far[k], ffar[step, k], F32(0))], axis=1)
            xh = x.astype(BF16).astype(F32)
            both = jnp.dot(jnp.concatenate([xh, x - xh], axis=0).astype(BF16), eq_s[k], preferred_element_type=F32)
            total = frecv[step, k, 3:6, :] + (both[0:3] + both[8:11])
            v = gv[k] + (ge[k] - total) / gm[k]
            gv[k] = jnp.where(exists[k], v, F32(0))
            gd[k] = gd[k] + gv[k]

    def internal(step, disp, ghost):
        for c in range(3):
            rows = [disp[c][h:h + 1, :] for h in range(8)] + [ghost[0][c:c + 1, :], ghost[1][c:c + 1, :]]
            rows = [jnp.broadcast_to(r, (8, 128)) for r in rows]
            for at in range(3):
                for e in range(2):
                    lo = con_lo[8 * at:8 * at + 8, 128 * e:128 * e + 128]
                    hi = con_hi[8 * at:8 * at + 8, 128 * e:128 * e + 128]
                    acc = lane_take(rows[0], lo)
                    for h in range(1, 10):
                        acc = jnp.where(hi == h, lane_take(rows[h], lo), acc)
                    u_s[c, 8 * at:8 * at + 8, 128 * e:128 * e + 128] = acc

        def multiply(a, acc):
            for c in range(3):
                acc = acc + kmat[c * 20 + a] * u_s[c, pl.ds(a, 1), :]
            return acc
        force = lax.fori_loop(0, 20, multiply, jnp.zeros((60, 256), F32))
        fh = force.astype(BF16).astype(F32)
        fh_s[...] = fh
        fl_s[...] = force - fh
        sub16 = lax.broadcasted_iota(jnp.int32, (16, 256), 0)
        for a in range(20):
            mask = jnp.broadcast_to(con_hi[a:a + 1, :], (16, 256)) == sub16
            for c in range(3):
                for k, part in enumerate((fh_s, fl_s)):
                    row = jnp.broadcast_to(part[20 * c + a:20 * c + a + 1, :], (16, 256))
                    v_s[48 * k + 16 * c:48 * k + 16 * c + 16, a * 256:a * 256 + 256] = jnp.where(mask, row, F32(0)).astype(BF16)
        both = jnp.dot(v_s[...], oh_e[...], preferred_element_type=F32)
        total = both[:48] + both[48:]
        own = [total[16 * c:16 * c + 8, :] for c in range(3)]
        for k in range(2):
            for c in range(3):
                fsend[step, k, c:c + 1, :] = total[16 * c + 8 + k:16 * c + 9 + k, :]
                fsend[step, k, 3 + c:4 + c, :] = pick(k, own[c])
            fsend[step, k, 6:8, :] = jnp.zeros((2, 128), F32)
        start_both(force_copies(step))
        if step < SUBSTEPS - 1:
            start_both(far_copies(step))
        return own

    def advance(step, own, ext, disp, vel):
        wait_both(force_copies(step))
        got = [jnp.where(me > 0, frecv[step, 0, 0:3, :], F32(0)), jnp.where(me < n - 1, frecv[step, 1, 0:3, :], F32(0))]
        parts = []
        for c in range(3):
            cols = []
            for r in range(2):
                x = jnp.where(halo_hi[r] == sub8, jnp.broadcast_to(got[r][c:c + 1, :], (8, 128)), F32(0))
                cols.append(x)
            parts.append(jnp.concatenate(cols, axis=1))
        x = jnp.concatenate(parts, axis=0)
        xh = x.astype(BF16).astype(F32)
        lhs = jnp.concatenate([xh, x - xh], axis=0).astype(BF16)
        both = jnp.dot(lhs, oh_h[...], preferred_element_type=F32)
        add = both[:24] + both[24:]
        vel = [vel[c] + (ext[c] - (own[c] + add[8 * c:8 * c + 8, :])) / mass for c in range(3)]
        disp = [disp[c] + vel[c] for c in range(3)]
        return disp, vel

    tiles = n // 8
    mine = me // 8

    def tile_at(k):
        d = k // 4
        step = lax.rem(2 + d + (d // 2) * (2 * d - 3), 4)
        g = lax.rem(gx + 2 * step, nx)
        g = g + (1 - 2 * lax.rem(g, 2)) * (1 - lax.rem(k // 2, 2))
        half = lax.rem(yz // 8 + 1 - lax.rem(k, 2), 2)
        return g, half

    send_state()

    def fwd(g, y):
        return pltpu.make_async_remote_copy(
            src_ref=s_ref.at[g * ny + y], dst_ref=recv.at[me], send_sem=fs_sem, recv_sem=fr_sem.at[mine],
            device_id=(g, y), device_id_type=MESH)

    def fwd_start(k, _):
        g, half = tile_at(k)
        for s in range(8):
            y = half * 8 + lax.rem(yz + s, 8)

            @pl.when(g * ny + y != me)
            def _():
                fwd(g, y).start()
        return 0
    lax.fori_loop(0, tiles, fwd_start, 0)
    recv[me] = s_ref[me]
    for dst in (con_lo, con_hi):
        dst[16:24, :] = jnp.zeros((8, 256), jnp.int32)
    con_lo[0:20, :] = con_ref[...] & 127
    con_hi[0:20, :] = con_ref[...] >> 7
    for a in range(20):
        for e in range(2):
            row = jnp.broadcast_to(con_lo[a:a + 1, 128 * e:128 * e + 128], (128, 128))
            oh_e[a * 256 + 128 * e:a * 256 + 128 * e + 128, :] = jnp.where(row == sub128, F32(1), F32(0)).T.astype(BF16)
    for r in range(2):
        row = jnp.broadcast_to(halo_ref[r:r + 1, :] & 127, (128, 128))
        oh_h[128 * r:128 * r + 128, :] = jnp.where(row == sub128, F32(1), F32(0)).T.astype(BF16)
    kcopy.wait()
    gd, gv, gm = ghost_state()
    own = internal(0, disp, gd)


    sub128h = lax.broadcasted_iota(jnp.int32, (128, 128), 0).astype(jnp.int16)

    def gather_load(k, acc):
        g, half = tile_at(k)
        source = g * 2 + half
        base = pl.multiple_of(source * 8, 8)
        def arrive(count):
            pltpu.make_async_remote_copy(
                src_ref=s_ref.at[pl.ds(0, count)], dst_ref=recv.at[pl.ds(0, count)], send_sem=fs_sem, recv_sem=fr_sem.at[source],
                device_id=(gx, yz), device_id_type=MESH).wait_recv()

        @pl.when(source == mine)
        def _():
            arrive(7)

        @pl.when(source != mine)
        def _():
            arrive(8)
        get = lambda r: recv[pl.ds(base, 8), r, :]
        loads = []
        for c in range(3):
            t0, t1 = get(2 * c), get(2 * c + 1)
            r0, r1 = pltpu.roll(t0, 64, 1), pltpu.roll(t1, 64, 1)
            loads.append([weights[j][0] * t0 + weights[j][1] * r0 + weights[j][2] * t1 + weights[j][3] * r1 for j in range(4)])
        total = jnp.zeros((48, 128), F32)
        for j in range(4):
            idx = get(6 + j).astype(jnp.int32)
            ids[j, pl.ds(base, 8), :] = idx
            lo, hi = idx & 127, idx >> 7
            highs = [loads[c][j].astype(BF16).astype(F32) for c in range(3)]
            lows = [loads[c][j] - highs[c] for c in range(3)]
            for s in range(0, 8, 2):
                hots, vals = [], []
                for k in (s, s + 1):
                    row = jnp.broadcast_to(lo[k:k + 1, :], (128, 128)).astype(jnp.int16)
                    hots.append(jnp.where(row == sub128h, BF16(1), BF16(0)))
                    mask = jnp.broadcast_to(hi[k:k + 1, :], (8, 128)) == sub8
                    vals.append(jnp.concatenate(
                        [jnp.where(mask, jnp.broadcast_to(p[k:k + 1, :], (8, 128)), F32(0)) for p in highs + lows], axis=0).astype(BF16))
                total = total + lax.dot_general(
                    jnp.concatenate(vals, axis=1), jnp.concatenate(hots, axis=1), (((1,), (1,)), ((), ())), preferred_element_type=F32)
        return acc + total
    both = lax.fori_loop(0, tiles, gather_load, jnp.zeros((48, 128), F32))
    ext = [both[8 * c:8 * c + 8] + both[24 + 8 * c:32 + 8 * c] for c in range(3)]

    for r in range(2):
        for c in range(3):
            esend[r, c:c + 1, :] = pick(r, ext[c])
        esend[r, 3:8, :] = jnp.zeros((5, 128), F32)
    start_both(load_copies)
    disp, vel = advance(0, own, ext, disp, vel)
    wait_both(load_copies)
    ge = [jnp.where(exists[k], erecv[k, 0:3, :], F32(0)) for k in range(2)]
    advance_ghosts(0, ge, gd, gv, gm)
    for step in range(1, SUBSTEPS):
        own = internal(step, disp, gd)
        disp, vel = advance(step, own, ext, disp, vel)
        if step < SUBSTEPS - 1:
            advance_ghosts(step, ge, gd, gv, gm)
    for c in range(3):
        for h in range(8):
            at_row = 32 + 8 * c + h
            ret_ref[n + at_row // 6, at_row % 6:at_row % 6 + 1, :] = disp[c][h:h + 1, :]
            u_s[c, h:h + 1, 0:128] = disp[c][h:h + 1, :]
    for r in range(32):
        ret_ref[n + r // 6, r % 6:r % 6 + 1, :] = slot_s[:, 128 * r:128 * r + 128].astype(F32)

    def ret(g, y):
        return pltpu.make_async_remote_copy(
            src_ref=outb.at[g * ny + y], dst_ref=ret_ref.at[me], send_sem=rs_sem, recv_sem=rr_sem,
            device_id=(g, y), device_id_type=MESH)

    def back(k, _):
        pair = [tile_at(2 * k + m) for m in range(2)]
        for g, half in pair:
            base = pl.multiple_of((g * 2 + half) * 8, 8)
            sums = [[jnp.zeros((8, 128), F32)] * 4 for c in range(3)]
            for j in range(4):
                idx = ids[j, pl.ds(base, 8), :]
                lo, hi = idx & 127, idx >> 7
                masks = [hi == h for h in range(1, 8)]
                for c in range(3):
                    acc = lane_take(jnp.broadcast_to(u_s[c, 0:1, 0:128], (8, 128)), lo)
                    for h in range(1, 8):
                        acc = jnp.where(masks[h - 1], lane_take(jnp.broadcast_to(u_s[c, h:h + 1, 0:128], (8, 128)), lo), acc)
                    sums[c] = [sums[c][m] + weights[j][m] * acc for m in range(4)]
            for c in range(3):
                p0, q0, p1, q1 = sums[c]
                outb[pl.ds(base, 8), 2 * c, :] = p0 + pltpu.roll(q0, 64, 1)
                outb[pl.ds(base, 8), 2 * c + 1, :] = p1 + pltpu.roll(q1, 64, 1)
        for g, half in pair:
            for s in range(8):
                y = half * 8 + lax.rem(yz + s, 8)

                @pl.when(g * ny + y != me)
                def _():
                    ret(g, y).start()
        return 0
    lax.fori_loop(0, tiles // 2, back, 0)
    ret_ref[me] = outb[me]

    def every(src, dst, ss, rs):
        return pltpu.make_async_remote_copy(
            src_ref=src.at[pl.ds(0, n - 1)], dst_ref=dst.at[pl.ds(0, n - 1)], send_sem=ss, recv_sem=rs,
            device_id=(gx, yz), device_id_type=MESH)
    every(s_ref, recv, fs_sem, fr_sem.at[0]).wait_send()
    last = every(outb, ret_ref, rs_sem, rr_sem)
    last.wait_send()
    last.wait_recv()


def solid(face_block, pressure, local, weight, area, nodes, target, stiffness, connect, halo, mass, disp, vel, nx, ny, shapes):
    n = nx * ny
    V = pl.BlockSpec(memory_space=pltpu.VMEM)
    A = pl.BlockSpec(memory_space=pl.ANY)
    D = pltpu.SemaphoreType.DMA
    M = pltpu.VMEM
    I32 = jnp.int32
    back = pl.pallas_call(
        functools.partial(solid_kernel, nx, ny, shapes),
        out_shape=jax.ShapeDtypeStruct((n + 10, 6, 128), F32),
        in_specs=[pl.BlockSpec(memory_space=pltpu.SMEM), A, A, A, A, A, V, A, V, V, V, V, V],
        out_specs=V,
        scratch_shapes=[
            M(pressure.shape, BF16), M(local.shape, I32), M(weight.shape, F32), M(area.shape, F32), M(nodes.shape, I32),
            M(area.shape, F32), M((16 * STRIDE, 128), F32), M((256, 32, 128), BF16), M((1024, 128), I32), M((1024, 128), F32),
            M((1024, 128), F32), M(target.shape, I32), M((128, 256), F32), M((640, 256), F32),
            M((n, 10, 128), F32),
            M((n, 10, 128), F32), M((n, 6, 128), F32), M((60, 60, 256), F32),
            M((4, n, 128), I32), M((24, 256), I32), M((24, 256), I32),
            M((3, 24, 256), F32), M((60, 256), F32), M((60, 256), F32),
            M((96, 5120), BF16), M((5120, 128), BF16), M((256, 128), BF16),
            M((2, 16, 128), F32), M((2, 16, 128), F32), M((2, 8, 128), F32), M((2, 8, 128), F32),
            M((SUBSTEPS, 2, 8, 128), F32), M((SUBSTEPS, 2, 8, 128), F32), M((SUBSTEPS, 2, 8, 128), F32), M((2, 256, 128), BF16),
            D((5,)), D, D, D((n // 8,)), D, D, D((2,)), D((2,)), D((2,)), D((2,)),
            D((SUBSTEPS, 2)), D((SUBSTEPS, 2)), D((SUBSTEPS, 2)), D((SUBSTEPS, 2))],
        compiler_params=pltpu.CompilerParams(collective_id=0, has_side_effects=True, vmem_limit_bytes=56 * 2**20),
        name="solid",
    )(face_block, pressure, local, weight, area, nodes, target, stiffness, connect, halo, mass.reshape(1, -1), disp, vel)
    return pl.pallas_call(
        functools.partial(unpack_kernel, n),
        out_shape=(jax.ShapeDtypeStruct(disp.shape, F32), jax.ShapeDtypeStruct((12, target.shape[1]), F32)),
        in_specs=[V, V],
        out_specs=(V, V),
        scratch_shapes=[M(target.shape, I32), M((768, 256), BF16)],
        compiler_params=pltpu.CompilerParams(vmem_limit_bytes=24 * 2**20),
        name="unpack",
    )(target, back)


def shape_table():
    corner_u = [-1, 1, 1, -1, 0, 1, 0, -1]
    corner_v = [-1, -1, 1, 1, -1, 0, 1, 0]
    gauss_point = 1.0 / math.sqrt(3.0)
    points = [
        (-gauss_point, -gauss_point),
        (gauss_point, -gauss_point),
        (gauss_point, gauss_point),
        (-gauss_point, gauss_point),
    ]
    shape_values = np.zeros((4, 8), np.float32)
    for position, (coord_u, coord_v) in enumerate(points):
        for corner in range(8):
            node_u = corner_u[corner]
            node_v = corner_v[corner]
            if corner < 4:
                entry_value = (
                    0.25
                    * (1 + coord_u * node_u)
                    * (1 + coord_v * node_v)
                    * (coord_u * node_u + coord_v * node_v - 1)
                )
            elif node_u == 0:
                entry_value = 0.5 * (1 - coord_u * coord_u) * (1 + coord_v * node_v)
            else:
                entry_value = 0.5 * (1 + coord_u * node_u) * (1 - coord_v * coord_v)
            shape_values[position, corner] = entry_value
    return shape_values


def shards(
    pressure,
    face_block,
    stencil_local,
    stencil_weight,
    area_normal,
    face_part,
    face_nodes,
    stiffness,
    connect,
    halo_nodes,
    node_mass,
    displacement,
    velocity,
):
    gx_size = lax.axis_size("gx")
    yz_size = lax.axis_size("yz")
    return solid(
        face_block, pressure, stencil_local, stencil_weight, area_normal, face_nodes, face_part.reshape(1, -1),
        stiffness, connect, halo_nodes, node_mass, displacement, velocity, gx_size, yz_size, shape_table()
    )


def solution(mesh):
    in_specs = (
        P(("gx", "yz"), None),
        P(("gx", "yz")),
        P(None, ("gx", "yz")),
        P(None, ("gx", "yz")),
        P(None, ("gx", "yz")),
        P(("gx", "yz"), None),
        P(None, ("gx", "yz")),
        P(None, None, ("gx", "yz")),
        P(None, ("gx", "yz")),
        P(None, ("gx", "yz")),
        P(("gx", "yz")),
        P(None, ("gx", "yz")),
        P(None, ("gx", "yz")),
    )
    out_specs = (P(None, ("gx", "yz")), P(None, ("gx", "yz")))
    return jax.shard_map(shards, mesh=mesh, in_specs=in_specs, out_specs=out_specs, check_vma=False)
```

```python
import functools
import math

import jax
import jax.numpy as jnp
import numpy as np
from jax import lax
from jax.experimental import pallas as pl
from jax.experimental.pallas import tpu as pltpu
from jax.sharding import PartitionSpec as P

MESH = pl.DeviceIdType.MESH
F32 = jnp.float32
BF16 = jnp.bfloat16
SUBSTEPS = 4

def half_lanes(left, right):
    lane = lax.broadcasted_iota(jnp.int32, (8, 128), 1)
    return jnp.where(lane < 64, F32(left), F32(right))

def mix_weights(shapes):
    pick = lambda q, a: float(shapes[q, a])
    out = []
    for j in range(4):
        e, o = 2 * j, 2 * j + 1
        out.append((
            half_lanes(pick(0, e), pick(1, o)), half_lanes(pick(1, e), pick(0, o)),
            half_lanes(pick(2, e), pick(3, o)), half_lanes(pick(3, e), pick(2, o))))
    return out

STRIDE = 40
UNR = 128
TAKE = lax.GatherDimensionNumbers(
    offset_dims=(), collapsed_slice_dims=(1,), start_index_map=(1,), operand_batching_dims=(0,), start_indices_batching_dims=(0,)
)

def lane_take(x, idx):
    return lax.gather(x, idx[..., None], TAKE, slice_sizes=(1, 1), mode=lax.GatherScatterMode.PROMISE_IN_BOUNDS)

def stencil_part(fb_ref, pr_ref, loc_ref, w_ref, an_ref, out_ref, tab32, tab, idxt, wt, res, arrive_lists, arrive_blocks):
    arrive_lists()
    for i in range(8):
        idxt[128 * i:128 * i + 128, :] = jnp.concatenate(
            [loc_ref[:, a * 1024 + 128 * i:a * 1024 + 128 * i + 128] for a in range(4)], axis=0).T
        wt[128 * i:128 * i + 128, :] = jnp.concatenate(
            [w_ref[:, a * 1024 + 128 * i:a * 1024 + 128 * i + 128] for a in range(4)], axis=0).T
    arrive_blocks()

    def relayout(b, _):
        r0 = pl.multiple_of(b * 16, 16)
        for t in range(32):
            x = pr_ref[pl.ds(r0, 16), 128 * t:128 * t + 128].astype(jnp.float32)
            tab32[pl.ds(t, 8, stride=STRIDE), :] = x[:8]
            tab32[pl.ds(8 * STRIDE + t, 8, stride=STRIDE), :] = x[8:]
        for n in range(16):
            tab[r0 + n] = tab32[n * STRIDE:n * STRIDE + 32, :].astype(jnp.bfloat16)
        return 0
    lax.fori_loop(0, 16, relayout, 0)
    lane = lax.broadcasted_iota(jnp.int32, (16, 128), 1)
    sub = lax.broadcasted_iota(jnp.int32, (16, 128), 0).astype(jnp.int16)
    grp = (lane // 32).astype(jnp.int16)
    m_lo = grp < 2
    m0 = grp == 0
    m2 = grp == 2

    def main(gg, _):
        for uu in range(UNR // 8):
            base = pl.multiple_of(gg * UNR + 8 * uu, 8)
            rows = []
            for u in range(8):
                g = base + u
                row = jnp.broadcast_to(idxt[pl.ds(g, 1), :], (16, 128))
                lo = (row & 127).astype(jnp.int16)
                hi = (row >> 7).astype(jnp.int16)
                cl = hi < 16
                mine = (hi & 15) == sub
                xs = []
                for a in range(4):
                    block = tab[fb_ref[a * 1024 + g]]
                    xs.append(jnp.where(cl, lane_take(block[:16], lo), lane_take(block[16:], lo)))
                x = jnp.where(m_lo, jnp.where(m0, xs[0], xs[1]), jnp.where(m2, xs[2], xs[3]))
                x = jnp.where(mine, x, jnp.bfloat16(0)).astype(jnp.float32)
                rows.append(jnp.sum(x[:8] + x[8:], axis=0, keepdims=True))
            res[pl.ds(base, 8), :] = jnp.concatenate(rows, axis=0) * wt[pl.ds(base, 8), :]
        return 0
    lax.fori_loop(0, 1024 // UNR, main, 0)
    for i in range(8):
        rt = res[128 * i:128 * i + 128, :].T
        for a in range(4):
            f0 = a * 1024 + 128 * i
            fp = jnp.concatenate([jnp.sum(rt[a * 32 + 8 * q:a * 32 + 8 * q + 8], axis=0, keepdims=True) for q in range(4)], axis=0)
            fp3 = jnp.concatenate([fp, fp, fp], axis=0)
            out_ref[:, f0:f0 + 128] = -(an_ref[:, f0:f0 + 128] * fp3)


def pack_part(tgt_ref, fn_ref, trac, slot_s, carry, acc, send_ref):
    wide = 2048
    rows128 = lax.broadcasted_iota(jnp.int32, (128, 256), 0)
    rows256 = lax.broadcasted_iota(jnp.int32, (256, 256), 0)
    cols256 = lax.broadcasted_iota(jnp.int32, (256, 256), 1)
    rows256w = lax.broadcasted_iota(jnp.int32, (256, wide), 0)
    rows32 = lax.broadcasted_iota(jnp.int32, (32, wide), 0)
    one_if = lambda m: jnp.where(m, F32(1), F32(0)).astype(BF16)
    upper = one_if(rows256 < cols256)
    ones = jnp.ones((256, 256), BF16)
    carry[...] = jnp.zeros_like(carry)
    acc[...] = jnp.zeros_like(acc)

    def rank(kt, _):
        before = carry[...]
        for m in range(8):
            at = pl.ds(pl.multiple_of(kt * wide + 256 * m, 256), 256)
            hit = jnp.broadcast_to(tgt_ref[:, at], (128, 256)) == rows128
            hot = one_if(hit)
            within = jnp.dot(hot, upper, preferred_element_type=F32) + before
            slot_s[:, at] = jnp.sum(jnp.where(hit, within, F32(0)), axis=0, keepdims=True).astype(jnp.int32)
            before = before + jnp.dot(hot, ones, preferred_element_type=F32)
        carry[...] = before
        return 0
    lax.fori_loop(0, 2, rank, 0)

    def tile(kt, _):
        at = pl.ds(pl.multiple_of(kt * wide, wide), wide)
        slot = slot_s[:, at]
        place = jnp.broadcast_to(tgt_ref[:, at] + 128 * (slot >> 5), (256, wide))
        weights = one_if(place == rows256w)
        mask = jnp.broadcast_to(slot & 31, (32, wide)) == rows32
        values = [trac[:, at], fn_ref[:, at].astype(F32)]
        total = None
        highs = [v.astype(BF16).astype(F32) for v in values]
        for part in (highs, [v - h for v, h in zip(values, highs)]):
            x = [
                jnp.where(mask, jnp.broadcast_to(p[r:r + 1, :], (32, wide)), F32(0)).astype(BF16)
                for p in part
                for r in range(p.shape[0])
            ]
            y = lax.dot_general(jnp.concatenate(x, axis=0), weights, (((1,), (1,)), ((), ())), preferred_element_type=F32)
            total = y if total is None else total + y
        acc[...] += total
        return 0
    lax.fori_loop(0, 2, tile, 0)
    for r in range(10):
        block = [acc[32 * v:32 * v + 32, 128 * h:128 * h + 128] for v in (2 * r, 2 * r + 1) for h in range(2)]
        send_ref[:, r, :] = jnp.concatenate(block, axis=0).T


def unpack_kernel(n, tgt_ref, ret_ref, nd_ref, fd_ref, slot_s, lhs):
    for r in range(56):
        row = ret_ref[n + r // 6, r % 6:r % 6 + 1, :]
        if r < 32:
            slot_s[:, 128 * r:128 * r + 128] = row.astype(jnp.int32)
        else:
            c, h = divmod(r - 32, 8)
            nd_ref[c:c + 1, 128 * h:128 * h + 128] = row
    wide = 1024
    rows128 = lax.broadcasted_iota(jnp.int32, (128, wide), 0)
    rows64 = lax.broadcasted_iota(jnp.int32, (64, wide), 0)
    for r in range(6):
        x = ret_ref[0:n, r, :].T
        xh = x.astype(BF16).astype(F32)
        lhs[128 * r:128 * r + 128, :] = jnp.concatenate([xh, x - xh], axis=1).astype(BF16)

    def tile(kt, _):
        at = pl.ds(pl.multiple_of(kt * wide, wide), wide)
        hot = jnp.where(jnp.broadcast_to(tgt_ref[:, at], (128, wide)) == rows128, F32(1), F32(0)).astype(BF16)
        y = jnp.dot(lhs[...], jnp.concatenate([hot, hot], axis=0), preferred_element_type=F32)
        mask = jnp.broadcast_to(slot_s[:, at], (64, wide)) == rows64
        fd_ref[:, at] = jnp.concatenate(
            [jnp.sum(jnp.where(mask, y[64 * v:64 * v + 64, :], F32(0)), axis=0, keepdims=True) for v in range(12)], axis=0
        )
        return 0
    lax.fori_loop(0, 4, tile, 0)


def solid_kernel(nx, ny, shapes, fb_ref, pr_hbm, loc_hbm, w_hbm, an_hbm, fn_hbm, tgt_ref, k_hbm, con_ref, halo_ref, mass_ref, disp_ref, vel_ref,
                 ret_ref,
                 pr_ref, loc_ref, w_ref, an_ref, fn_ref, trac, tab32, tab, idxt, wt, res, slot_s, carry, acc_s, s_ref,
                 recv, outb, kmat, ids, con_lo, con_hi, u_s, fh_s, fl_s, v_s, oh_e, oh_h,
                 dsend, drecv, esend, erecv, fsend, frecv, ffar, eq_s,
                 in_sem, k_sem, fs_sem, fr_sem, rs_sem, rr_sem, ds_sem, dr_sem, es_sem, er_sem, gs_sem, gr_sem, hs_sem, hr_sem):
    n = nx * ny
    gx = lax.axis_index("gx")
    yz = lax.axis_index("yz")
    me = gx * ny + yz
    dev = lambda t: (t // ny, lax.rem(t, ny))
    ins = [pltpu.make_async_copy(src, dst, in_sem.at[k]) for k, (src, dst) in enumerate(
        ((loc_hbm, loc_ref), (w_hbm, w_ref), (pr_hbm, pr_ref), (an_hbm, an_ref), (fn_hbm, fn_ref)))]
    for cp in ins:
        cp.start()
    kcopy = pltpu.make_async_copy(k_hbm, kmat, k_sem)
    kcopy.start()
    barrier = pltpu.get_barrier_semaphore()

    gx_at = [lax.rem(gx + a, nx) for a in range(nx)]

    def greet(b, _):
        y = lax.rem(yz + b, ny)
        for a in range(nx):
            pl.semaphore_signal(barrier, inc=1, device_id=(gx_at[a], y), device_id_type=MESH)
        return 0
    lax.fori_loop(1, ny, greet, 0)
    for a in range(1, nx):
        pl.semaphore_signal(barrier, inc=1, device_id=(gx_at[a], yz), device_id_type=MESH)

    sub8 = lax.broadcasted_iota(jnp.int32, (8, 128), 0)
    sub128 = lax.broadcasted_iota(jnp.int32, (128, 128), 0)
    weights = mix_weights(shapes)

    halo_lo = [jnp.broadcast_to(halo_ref[r:r + 1, :] & 127, (8, 128)) for r in range(2)]
    halo_hi = [jnp.broadcast_to(halo_ref[r:r + 1, :] >> 7, (8, 128)) for r in range(2)]
    stack = lambda ref, c: jnp.concatenate([ref[c:c + 1, 128 * h:128 * h + 128] for h in range(8)], axis=0)
    disp = [stack(disp_ref, c) for c in range(3)]
    vel = [stack(vel_ref, c) for c in range(3)]
    mass = stack(mass_ref, 0)

    def arrive_lists():
        ins[0].wait()
        ins[1].wait()

    def arrive_blocks():
        for cp in ins[2:]:
            cp.wait()
    stencil_part(fb_ref, pr_ref, loc_ref, w_ref, an_ref, trac, tab32, tab, idxt, wt, res, arrive_lists, arrive_blocks)
    pack_part(tgt_ref, fn_ref, trac, slot_s, carry, acc_s, s_ref)
    pl.semaphore_wait(barrier, n - 1)

    def near(src, dst, ss, rs, t):
        return pltpu.make_async_remote_copy(src_ref=src, dst_ref=dst, send_sem=ss, recv_sem=rs, device_id=dev(t), device_id_type=MESH)

    def hop(send, recv, ss, rs, dist):
        return (near(send(1), recv(0), ss(1), rs(0), lax.rem(me + dist, n)),
                near(send(0), recv(1), ss(0), rs(1), lax.rem(me + n - dist, n)), dist)

    def start_both(copies):
        up, down, dist = copies

        @pl.when(me < n - dist)
        def _():
            up.start()

        @pl.when(me >= dist)
        def _():
            down.start()

    def wait_both(copies):
        up, down, dist = copies

        @pl.when(me < n - dist)
        def _():
            up.wait_send()
            down.wait_recv()

        @pl.when(me >= dist)
        def _():
            down.wait_send()
            up.wait_recv()

    at = lambda ref, *lead: lambda side: ref.at[(*lead, side)]
    state_copies = hop(at(dsend), at(drecv), at(ds_sem), at(dr_sem), 1)
    load_copies = hop(at(esend), at(erecv), at(es_sem), at(er_sem), 1)
    force_copies = lambda step: hop(at(fsend, step), at(frecv, step), at(gs_sem, step), at(gr_sem, step), 1)
    far_copies = lambda step: hop(at(fsend, step), at(ffar, step), at(hs_sem, step), at(hr_sem, step), 2)
    exists = [me > 0, me < n - 1]
    exists_far = [me > 1, me < n - 2]

    def pick(r, x):
        g = jnp.where(halo_hi[r] == sub8, lane_take(x, halo_lo[r]), F32(0))
        return jnp.sum(g, axis=0, keepdims=True)

    def send_state():
        for r in range(2):
            for c in range(3):
                dsend[r, c:c + 1, :] = pick(r, disp[c])
                dsend[r, 3 + c:4 + c, :] = pick(r, vel[c])
            dsend[r, 6:7, :] = pick(r, mass)
            dsend[r, 8:10, :] = halo_ref[...].astype(F32)
        start_both(state_copies)

    def ghost_state():
        wait_both(state_copies)
        gd = [jnp.where(exists[k], drecv[k, 0:3, :], F32(0)) for k in range(2)]
        gv = [jnp.where(exists[k], drecv[k, 3:6, :], F32(0)) for k in range(2)]
        gm = [jnp.where(exists[k], drecv[k, 6:7, :], F32(1)) for k in range(2)]
        for k in range(2):
            held, other = drecv[k, 9 - k:10 - k, :], drecv[k, 8 + k:9 + k, :]
            for m, x in enumerate((held, other)):
                same = jnp.broadcast_to(x, (128, 128)).T == jnp.broadcast_to(held, (128, 128))
                eq_s[k, 128 * m:128 * m + 128, :] = jnp.where(same, F32(1), F32(0)).astype(BF16)
        return gd, gv, gm

    def advance_ghosts(step, ge, gd, gv, gm):
        wait_both(far_copies(step))
        for k in range(2):
            x = jnp.concatenate([fsend[step, k], jnp.where(exists_far[k], ffar[step, k], F32(0))], axis=1)
            xh = x.astype(BF16).astype(F32)
            both = jnp.dot(jnp.concatenate([xh, x - xh], axis=0).astype(BF16), eq_s[k], preferred_element_type=F32)
            total = frecv[step, k, 3:6, :] + (both[0:3] + both[8:11])
            v = gv[k] + (ge[k] - total) / gm[k]
            gv[k] = jnp.where(exists[k], v, F32(0))
            gd[k] = gd[k] + gv[k]

    def internal(step, disp, ghost):
        for c in range(3):
            rows = [disp[c][h:h + 1, :] for h in range(8)] + [ghost[0][c:c + 1, :], ghost[1][c:c + 1, :]]
            rows = [jnp.broadcast_to(r, (8, 128)) for r in rows]
            for at in range(3):
                for e in range(2):
                    lo = con_lo[8 * at:8 * at + 8, 128 * e:128 * e + 128]
                    hi = con_hi[8 * at:8 * at + 8, 128 * e:128 * e + 128]
                    acc = lane_take(rows[0], lo)
                    for h in range(1, 10):
                        acc = jnp.where(hi == h, lane_take(rows[h], lo), acc)
                    u_s[c, 8 * at:8 * at + 8, 128 * e:128 * e + 128] = acc

        def multiply(a, acc):
            for c in range(3):
                acc = acc + kmat[c * 20 + a] * u_s[c, pl.ds(a, 1), :]
            return acc
        force = lax.fori_loop(0, 20, multiply, jnp.zeros((60, 256), F32))
        fh = force.astype(BF16).astype(F32)
        fh_s[...] = fh
        fl_s[...] = force - fh
        sub16 = lax.broadcasted_iota(jnp.int32, (16, 256), 0)
        for a in range(20):
            mask = jnp.broadcast_to(con_hi[a:a + 1, :], (16, 256)) == sub16
            for c in range(3):
                for k, part in enumerate((fh_s, fl_s)):
                    row = jnp.broadcast_to(part[20 * c + a:20 * c + a + 1, :], (16, 256))
                    v_s[48 * k + 16 * c:48 * k + 16 * c + 16, a * 256:a * 256 + 256] = jnp.where(mask, row, F32(0)).astype(BF16)
        both = jnp.dot(v_s[...], oh_e[...], preferred_element_type=F32)
        total = both[:48] + both[48:]
        own = [total[16 * c:16 * c + 8, :] for c in range(3)]
        for k in range(2):
            for c in range(3):
                fsend[step, k, c:c + 1, :] = total[16 * c + 8 + k:16 * c + 9 + k, :]
                fsend[step, k, 3 + c:4 + c, :] = pick(k, own[c])
            fsend[step, k, 6:8, :] = jnp.zeros((2, 128), F32)
        start_both(force_copies(step))
        if step < SUBSTEPS - 1:
            start_both(far_copies(step))
        return own

    def advance(step, own, ext, disp, vel):
        wait_both(force_copies(step))
        got = [jnp.where(me > 0, frecv[step, 0, 0:3, :], F32(0)), jnp.where(me < n - 1, frecv[step, 1, 0:3, :], F32(0))]
        parts = []
        for c in range(3):
            cols = []
            for r in range(2):
                x = jnp.where(halo_hi[r] == sub8, jnp.broadcast_to(got[r][c:c + 1, :], (8, 128)), F32(0))
                cols.append(x)
            parts.append(jnp.concatenate(cols, axis=1))
        x = jnp.concatenate(parts, axis=0)
        xh = x.astype(BF16).astype(F32)
        lhs = jnp.concatenate([xh, x - xh], axis=0).astype(BF16)
        both = jnp.dot(lhs, oh_h[...], preferred_element_type=F32)
        add = both[:24] + both[24:]
        vel = [vel[c] + (ext[c] - (own[c] + add[8 * c:8 * c + 8, :])) / mass for c in range(3)]
        disp = [disp[c] + vel[c] for c in range(3)]
        return disp, vel

    tiles = n // 8
    mine = me // 8

    spread = [lax.rem(yz + s, 8) for s in range(8)]
    own_half = yz // 8

    def tile_at(k):
        d = k // 4
        step = lax.rem(2 + d + (d // 2) * (2 * d - 3), 4)
        g = lax.rem(gx + 2 * step, nx)
        g = g + (1 - 2 * lax.rem(g, 2)) * (1 - lax.rem(k // 2, 2))
        half = lax.rem(yz // 8 + 1 - lax.rem(k, 2), 2)
        return g, half

    send_state()

    def fwd(g, y):
        return pltpu.make_async_remote_copy(
            src_ref=s_ref.at[g * ny + y], dst_ref=recv.at[me], send_sem=fs_sem, recv_sem=fr_sem.at[mine],
            device_id=(g, y), device_id_type=MESH)

    def fwd_start(k, _):
        g, half = tile_at(k)
        for s in range(8):
            fwd(g, half * 8 + spread[s]).start()
        return 0
    lax.fori_loop(0, tiles - 1, fwd_start, 0)
    for s in range(1, 8):
        fwd(gx, own_half * 8 + spread[s]).start()
    recv[me] = s_ref[me]
    for dst in (con_lo, con_hi):
        dst[16:24, :] = jnp.zeros((8, 256), jnp.int32)
    con_lo[0:20, :] = con_ref[...] & 127
    con_hi[0:20, :] = con_ref[...] >> 7
    for a in range(20):
        for e in range(2):
            row = jnp.broadcast_to(con_lo[a:a + 1, 128 * e:128 * e + 128], (128, 128))
            oh_e[a * 256 + 128 * e:a * 256 + 128 * e + 128, :] = jnp.where(row == sub128, F32(1), F32(0)).T.astype(BF16)
    for r in range(2):
        row = jnp.broadcast_to(halo_ref[r:r + 1, :] & 127, (128, 128))
        oh_h[128 * r:128 * r + 128, :] = jnp.where(row == sub128, F32(1), F32(0)).T.astype(BF16)
    kcopy.wait()
    gd, gv, gm = ghost_state()
    own = internal(0, disp, gd)


    sub128h = lax.broadcasted_iota(jnp.int32, (128, 128), 0).astype(jnp.int16)

    def arrive(source, count):
        pltpu.make_async_remote_copy(
            src_ref=s_ref.at[pl.ds(0, count)], dst_ref=recv.at[pl.ds(0, count)], send_sem=fs_sem, recv_sem=fr_sem.at[source],
            device_id=(gx, yz), device_id_type=MESH).wait_recv()

    def load_of(source, acc):
        base = pl.multiple_of(source * 8, 8)
        get = lambda r: recv[pl.ds(base, 8), r, :]
        loads = []
        for c in range(3):
            t0, t1 = get(2 * c), get(2 * c + 1)
            r0, r1 = pltpu.roll(t0, 64, 1), pltpu.roll(t1, 64, 1)
            loads.append([weights[j][0] * t0 + weights[j][1] * r0 + weights[j][2] * t1 + weights[j][3] * r1 for j in range(4)])
        total = jnp.zeros((48, 128), F32)
        for j in range(4):
            idx = get(6 + j).astype(jnp.int32)
            ids[j, pl.ds(base, 8), :] = idx
            lo, hi = idx & 127, idx >> 7
            highs = [loads[c][j].astype(BF16).astype(F32) for c in range(3)]
            lows = [loads[c][j] - highs[c] for c in range(3)]
            for s in range(0, 8, 2):
                hots, vals = [], []
                for k in (s, s + 1):
                    row = jnp.broadcast_to(lo[k:k + 1, :], (128, 128)).astype(jnp.int16)
                    hots.append(jnp.where(row == sub128h, BF16(1), BF16(0)))
                    mask = jnp.broadcast_to(hi[k:k + 1, :], (8, 128)) == sub8
                    vals.append(jnp.concatenate(
                        [jnp.where(mask, jnp.broadcast_to(p[k:k + 1, :], (8, 128)), F32(0)) for p in highs + lows], axis=0).astype(BF16))
                total = total + lax.dot_general(
                    jnp.concatenate(vals, axis=1), jnp.concatenate(hots, axis=1), (((1,), (1,)), ((), ())), preferred_element_type=F32)
        return acc + total
    def gather_load(k, acc):
        sources = []
        for m in range(3):
            g, half = tile_at(3 * k + m)
            sources.append(g * 2 + half)
            arrive(sources[m], 8)
        for source in sources:
            acc = load_of(source, acc)
        return acc

    both = lax.fori_loop(0, (tiles - 1) // 3, gather_load, jnp.zeros((48, 128), F32))
    arrive(mine, 7)
    both = load_of(mine, both)
    ext = [both[8 * c:8 * c + 8] + both[24 + 8 * c:32 + 8 * c] for c in range(3)]

    for r in range(2):
        for c in range(3):
            esend[r, c:c + 1, :] = pick(r, ext[c])
        esend[r, 3:8, :] = jnp.zeros((5, 128), F32)
    start_both(load_copies)
    disp, vel = advance(0, own, ext, disp, vel)
    wait_both(load_copies)
    ge = [jnp.where(exists[k], erecv[k, 0:3, :], F32(0)) for k in range(2)]
    advance_ghosts(0, ge, gd, gv, gm)
    for step in range(1, SUBSTEPS):
        own = internal(step, disp, gd)
        disp, vel = advance(step, own, ext, disp, vel)
        if step < SUBSTEPS - 1:
            advance_ghosts(step, ge, gd, gv, gm)
    for c in range(3):
        for h in range(8):
            at_row = 32 + 8 * c + h
            ret_ref[n + at_row // 6, at_row % 6:at_row % 6 + 1, :] = disp[c][h:h + 1, :]
            u_s[c, h:h + 1, 0:128] = disp[c][h:h + 1, :]
    for r in range(32):
        ret_ref[n + r // 6, r % 6:r % 6 + 1, :] = slot_s[:, 128 * r:128 * r + 128].astype(F32)

    def ret(g, y):
        return pltpu.make_async_remote_copy(
            src_ref=outb.at[g * ny + y], dst_ref=ret_ref.at[me], send_sem=rs_sem, recv_sem=rr_sem,
            device_id=(g, y), device_id_type=MESH)

    def back(k, _):
        pair = [tile_at(2 * k + m) for m in range(2)]
        for g, half in pair:
            base = pl.multiple_of((g * 2 + half) * 8, 8)
            sums = [[jnp.zeros((8, 128), F32)] * 4 for c in range(3)]
            for j in range(4):
                idx = ids[j, pl.ds(base, 8), :]
                lo, hi = idx & 127, idx >> 7
                masks = [hi == h for h in range(1, 8)]
                for c in range(3):
                    acc = lane_take(jnp.broadcast_to(u_s[c, 0:1, 0:128], (8, 128)), lo)
                    for h in range(1, 8):
                        acc = jnp.where(masks[h - 1], lane_take(jnp.broadcast_to(u_s[c, h:h + 1, 0:128], (8, 128)), lo), acc)
                    sums[c] = [sums[c][m] + weights[j][m] * acc for m in range(4)]
            for c in range(3):
                p0, q0, p1, q1 = sums[c]
                outb[pl.ds(base, 8), 2 * c, :] = p0 + pltpu.roll(q0, 64, 1)
                outb[pl.ds(base, 8), 2 * c + 1, :] = p1 + pltpu.roll(q1, 64, 1)
        for g, half in pair:
            for s in range(8):
                y = half * 8 + lax.rem(yz + s, 8)

                @pl.when(g * ny + y != me)
                def _():
                    ret(g, y).start()
        return 0
    lax.fori_loop(0, tiles // 2, back, 0)
    ret_ref[me] = outb[me]

    def every(src, dst, ss, rs):
        return pltpu.make_async_remote_copy(
            src_ref=src.at[pl.ds(0, n - 1)], dst_ref=dst.at[pl.ds(0, n - 1)], send_sem=ss, recv_sem=rs,
            device_id=(gx, yz), device_id_type=MESH)
    every(s_ref, recv, fs_sem, fr_sem.at[0]).wait_send()
    last = every(outb, ret_ref, rs_sem, rr_sem)
    last.wait_send()
    last.wait_recv()


def solid(face_block, pressure, local, weight, area, nodes, target, stiffness, connect, halo, mass, disp, vel, nx, ny, shapes):
    n = nx * ny
    V = pl.BlockSpec(memory_space=pltpu.VMEM)
    A = pl.BlockSpec(memory_space=pl.ANY)
    D = pltpu.SemaphoreType.DMA
    M = pltpu.VMEM
    I32 = jnp.int32
    back = pl.pallas_call(
        functools.partial(solid_kernel, nx, ny, shapes),
        out_shape=jax.ShapeDtypeStruct((n + 10, 6, 128), F32),
        in_specs=[pl.BlockSpec(memory_space=pltpu.SMEM), A, A, A, A, A, V, A, V, V, V, V, V],
        out_specs=V,
        scratch_shapes=[
            M(pressure.shape, BF16), M(local.shape, I32), M(weight.shape, F32), M(area.shape, F32), M(nodes.shape, I32),
            M(area.shape, F32), M((16 * STRIDE, 128), F32), M((256, 32, 128), BF16), M((1024, 128), I32), M((1024, 128), F32),
            M((1024, 128), F32), M(target.shape, I32), M((128, 256), F32), M((640, 256), F32),
            M((n, 10, 128), F32),
            M((n, 10, 128), F32), M((n, 6, 128), F32), M((60, 60, 256), F32),
            M((4, n, 128), I32), M((24, 256), I32), M((24, 256), I32),
            M((3, 24, 256), F32), M((60, 256), F32), M((60, 256), F32),
            M((96, 5120), BF16), M((5120, 128), BF16), M((256, 128), BF16),
            M((2, 16, 128), F32), M((2, 16, 128), F32), M((2, 8, 128), F32), M((2, 8, 128), F32),
            M((SUBSTEPS, 2, 8, 128), F32), M((SUBSTEPS, 2, 8, 128), F32), M((SUBSTEPS, 2, 8, 128), F32), M((2, 256, 128), BF16),
            D((5,)), D, D, D((n // 8,)), D, D, D((2,)), D((2,)), D((2,)), D((2,)),
            D((SUBSTEPS, 2)), D((SUBSTEPS, 2)), D((SUBSTEPS, 2)), D((SUBSTEPS, 2))],
        compiler_params=pltpu.CompilerParams(collective_id=0, has_side_effects=True, vmem_limit_bytes=56 * 2**20),
        name="solid",
    )(face_block, pressure, local, weight, area, nodes, target, stiffness, connect, halo, mass.reshape(1, -1), disp, vel)
    return pl.pallas_call(
        functools.partial(unpack_kernel, n),
        out_shape=(jax.ShapeDtypeStruct(disp.shape, F32), jax.ShapeDtypeStruct((12, target.shape[1]), F32)),
        in_specs=[V, V],
        out_specs=(V, V),
        scratch_shapes=[M(target.shape, I32), M((768, 256), BF16)],
        compiler_params=pltpu.CompilerParams(vmem_limit_bytes=24 * 2**20),
        name="unpack",
    )(target, back)


def shape_table():
    corner_u = [-1, 1, 1, -1, 0, 1, 0, -1]
    corner_v = [-1, -1, 1, 1, -1, 0, 1, 0]
    gauss_point = 1.0 / math.sqrt(3.0)
    points = [
        (-gauss_point, -gauss_point),
        (gauss_point, -gauss_point),
        (gauss_point, gauss_point),
        (-gauss_point, gauss_point),
    ]
    shape_values = np.zeros((4, 8), np.float32)
    for position, (coord_u, coord_v) in enumerate(points):
        for corner in range(8):
            node_u = corner_u[corner]
            node_v = corner_v[corner]
            if corner < 4:
                entry_value = (
                    0.25
                    * (1 + coord_u * node_u)
                    * (1 + coord_v * node_v)
                    * (coord_u * node_u + coord_v * node_v - 1)
                )
            elif node_u == 0:
                entry_value = 0.5 * (1 - coord_u * coord_u) * (1 + coord_v * node_v)
            else:
                entry_value = 0.5 * (1 + coord_u * node_u) * (1 - coord_v * coord_v)
            shape_values[position, corner] = entry_value
    return shape_values


def shards(
    pressure,
    face_block,
    stencil_local,
    stencil_weight,
    area_normal,
    face_part,
    face_nodes,
    stiffness,
    connect,
    halo_nodes,
    node_mass,
    displacement,
    velocity,
):
    gx_size = lax.axis_size("gx")
    yz_size = lax.axis_size("yz")
    return solid(
        face_block, pressure, stencil_local, stencil_weight, area_normal, face_nodes, face_part.reshape(1, -1),
        stiffness, connect, halo_nodes, node_mass, displacement, velocity, gx_size, yz_size, shape_table()
    )


def solution(mesh):
    in_specs = (
        P(("gx", "yz"), None),
        P(("gx", "yz")),
        P(None, ("gx", "yz")),
        P(None, ("gx", "yz")),
        P(None, ("gx", "yz")),
        P(("gx", "yz"), None),
        P(None, ("gx", "yz")),
        P(None, None, ("gx", "yz")),
        P(None, ("gx", "yz")),
        P(None, ("gx", "yz")),
        P(("gx", "yz")),
        P(None, ("gx", "yz")),
        P(None, ("gx", "yz")),
    )
    out_specs = (P(None, ("gx", "yz")), P(None, ("gx", "yz")))
    return jax.shard_map(shards, mesh=mesh, in_specs=in_specs, out_specs=out_specs, check_vma=False)
```

```python
import functools
import math

import jax
import jax.numpy as jnp
import numpy as np
from jax import lax
from jax.experimental import pallas as pl
from jax.experimental.pallas import tpu as pltpu
from jax.sharding import PartitionSpec as P

MESH = pl.DeviceIdType.MESH
F32 = jnp.float32
BF16 = jnp.bfloat16
SUBSTEPS = 4

def half_lanes(left, right):
    lane = lax.broadcasted_iota(jnp.int32, (8, 128), 1)
    return jnp.where(lane < 64, F32(left), F32(right))

def mix_weights(shapes):
    pick = lambda q, a: float(shapes[q, a])
    out = []
    for j in range(4):
        e, o = 2 * j, 2 * j + 1
        out.append((
            half_lanes(pick(0, e), pick(1, o)), half_lanes(pick(1, e), pick(0, o)),
            half_lanes(pick(2, e), pick(3, o)), half_lanes(pick(3, e), pick(2, o))))
    return out

STRIDE = 40
UNR = 128
TAKE = lax.GatherDimensionNumbers(
    offset_dims=(), collapsed_slice_dims=(1,), start_index_map=(1,), operand_batching_dims=(0,), start_indices_batching_dims=(0,)
)

def lane_take(x, idx):
    return lax.gather(x, idx[..., None], TAKE, slice_sizes=(1, 1), mode=lax.GatherScatterMode.PROMISE_IN_BOUNDS)

def stencil_part(fb_ref, pr_ref, loc_ref, w_ref, an_ref, out_ref, tab32, tab, idxt, wt, res, arrive_lists, arrive_blocks):
    arrive_lists()
    for i in range(8):
        idxt[128 * i:128 * i + 128, :] = jnp.concatenate(
            [loc_ref[:, a * 1024 + 128 * i:a * 1024 + 128 * i + 128] for a in range(4)], axis=0).T
        wt[128 * i:128 * i + 128, :] = jnp.concatenate(
            [w_ref[:, a * 1024 + 128 * i:a * 1024 + 128 * i + 128] for a in range(4)], axis=0).T
    arrive_blocks()

    def relayout(b, _):
        r0 = pl.multiple_of(b * 16, 16)
        for t in range(32):
            x = pr_ref[pl.ds(r0, 16), 128 * t:128 * t + 128].astype(jnp.float32)
            tab32[pl.ds(t, 8, stride=STRIDE), :] = x[:8]
            tab32[pl.ds(8 * STRIDE + t, 8, stride=STRIDE), :] = x[8:]
        for n in range(16):
            tab[r0 + n] = tab32[n * STRIDE:n * STRIDE + 32, :].astype(jnp.bfloat16)
        return 0
    lax.fori_loop(0, 16, relayout, 0)
    lane = lax.broadcasted_iota(jnp.int32, (16, 128), 1)
    sub = lax.broadcasted_iota(jnp.int32, (16, 128), 0).astype(jnp.int16)
    grp = (lane // 32).astype(jnp.int16)
    m_lo = grp < 2
    m0 = grp == 0
    m2 = grp == 2

    def main(gg, _):
        for uu in range(UNR // 8):
            base = pl.multiple_of(gg * UNR + 8 * uu, 8)
            rows = []
            for u in range(8):
                g = base + u
                row = jnp.broadcast_to(idxt[pl.ds(g, 1), :], (16, 128))
                lo = (row & 127).astype(jnp.int16)
                hi = (row >> 7).astype(jnp.int16)
                cl = hi < 16
                mine = (hi & 15) == sub
                xs = []
                for a in range(4):
                    block = tab[fb_ref[a * 1024 + g]]
                    xs.append(jnp.where(cl, lane_take(block[:16], lo), lane_take(block[16:], lo)))
                x = jnp.where(m_lo, jnp.where(m0, xs[0], xs[1]), jnp.where(m2, xs[2], xs[3]))
                x = jnp.where(mine, x, jnp.bfloat16(0)).astype(jnp.float32)
                rows.append(jnp.sum(x[:8] + x[8:], axis=0, keepdims=True))
            res[pl.ds(base, 8), :] = jnp.concatenate(rows, axis=0) * wt[pl.ds(base, 8), :]
        return 0
    lax.fori_loop(0, 1024 // UNR, main, 0)
    for i in range(8):
        rt = res[128 * i:128 * i + 128, :].T
        for a in range(4):
            f0 = a * 1024 + 128 * i
            fp = jnp.concatenate([jnp.sum(rt[a * 32 + 8 * q:a * 32 + 8 * q + 8], axis=0, keepdims=True) for q in range(4)], axis=0)
            fp3 = jnp.concatenate([fp, fp, fp], axis=0)
            out_ref[:, f0:f0 + 128] = -(an_ref[:, f0:f0 + 128] * fp3)


def rank_part(tgt_ref, slot_s, carry):
    wide = 2048
    rows128 = lax.broadcasted_iota(jnp.int32, (128, 256), 0)
    rows256 = lax.broadcasted_iota(jnp.int32, (256, 256), 0)
    cols256 = lax.broadcasted_iota(jnp.int32, (256, 256), 1)
    one_if = lambda m: jnp.where(m, F32(1), F32(0)).astype(BF16)
    upper = one_if(rows256 < cols256)
    ones = jnp.ones((256, 256), BF16)
    carry[...] = jnp.zeros_like(carry)

    def rank(kt, _):
        before = carry[...]
        for m in range(8):
            at = pl.ds(pl.multiple_of(kt * wide + 256 * m, 256), 256)
            hit = jnp.broadcast_to(tgt_ref[:, at], (128, 256)) == rows128
            hot = one_if(hit)
            within = jnp.dot(hot, upper, preferred_element_type=F32) + before
            slot_s[:, at] = jnp.sum(jnp.where(hit, within, F32(0)), axis=0, keepdims=True).astype(jnp.int32)
            before = before + jnp.dot(hot, ones, preferred_element_type=F32)
        carry[...] = before
        return 0
    lax.fori_loop(0, 2, rank, 0)


def pack_part(tgt_ref, fn_ref, trac, slot_s, acc, send_ref):
    wide = 2048
    rows128 = lax.broadcasted_iota(jnp.int32, (128, 256), 0)
    rows256 = lax.broadcasted_iota(jnp.int32, (256, 256), 0)
    cols256 = lax.broadcasted_iota(jnp.int32, (256, 256), 1)
    rows256w = lax.broadcasted_iota(jnp.int32, (256, wide), 0)
    rows32 = lax.broadcasted_iota(jnp.int32, (32, wide), 0)
    one_if = lambda m: jnp.where(m, F32(1), F32(0)).astype(BF16)
    acc[...] = jnp.zeros_like(acc)

    def tile(kt, _):
        at = pl.ds(pl.multiple_of(kt * wide, wide), wide)
        slot = slot_s[:, at]
        place = jnp.broadcast_to(tgt_ref[:, at] + 128 * (slot >> 5), (256, wide))
        weights = one_if(place == rows256w)
        mask = jnp.broadcast_to(slot & 31, (32, wide)) == rows32
        values = [trac[:, at], fn_ref[:, at].astype(F32)]
        total = None
        highs = [v.astype(BF16).astype(F32) for v in values]
        for part in (highs, [v - h for v, h in zip(values, highs)]):
            x = [
                jnp.where(mask, jnp.broadcast_to(p[r:r + 1, :], (32, wide)), F32(0)).astype(BF16)
                for p in part
                for r in range(p.shape[0])
            ]
            y = lax.dot_general(jnp.concatenate(x, axis=0), weights, (((1,), (1,)), ((), ())), preferred_element_type=F32)
            total = y if total is None else total + y
        acc[...] += total
        return 0
    lax.fori_loop(0, 2, tile, 0)
    for r in range(10):
        block = [acc[32 * v:32 * v + 32, 128 * h:128 * h + 128] for v in (2 * r, 2 * r + 1) for h in range(2)]
        send_ref[:, r, :] = jnp.concatenate(block, axis=0).T


def unpack_kernel(n, tgt_ref, ret_ref, nd_ref, fd_ref, slot_s, lhs):
    for r in range(56):
        row = ret_ref[n + r // 6, r % 6:r % 6 + 1, :]
        if r < 32:
            slot_s[:, 128 * r:128 * r + 128] = row.astype(jnp.int32)
        else:
            c, h = divmod(r - 32, 8)
            nd_ref[c:c + 1, 128 * h:128 * h + 128] = row
    wide = 1024
    rows128 = lax.broadcasted_iota(jnp.int32, (128, wide), 0)
    rows64 = lax.broadcasted_iota(jnp.int32, (64, wide), 0)
    for r in range(6):
        x = ret_ref[0:n, r, :].T
        xh = x.astype(BF16).astype(F32)
        lhs[128 * r:128 * r + 128, :] = jnp.concatenate([xh, x - xh], axis=1).astype(BF16)

    def tile(kt, _):
        at = pl.ds(pl.multiple_of(kt * wide, wide), wide)
        hot = jnp.where(jnp.broadcast_to(tgt_ref[:, at], (128, wide)) == rows128, F32(1), F32(0)).astype(BF16)
        y = jnp.dot(lhs[...], jnp.concatenate([hot, hot], axis=0), preferred_element_type=F32)
        mask = jnp.broadcast_to(slot_s[:, at], (64, wide)) == rows64
        fd_ref[:, at] = jnp.concatenate(
            [jnp.sum(jnp.where(mask, y[64 * v:64 * v + 64, :], F32(0)), axis=0, keepdims=True) for v in range(12)], axis=0
        )
        return 0
    lax.fori_loop(0, 4, tile, 0)


def solid_kernel(nx, ny, shapes, fb_ref, pr_hbm, loc_hbm, w_hbm, an_hbm, fn_hbm, tgt_ref, k_hbm, con_ref, halo_ref, mass_ref, disp_ref, vel_ref,
                 ret_ref,
                 pr_ref, loc_ref, w_ref, an_ref, fn_ref, trac, tab32, tab, idxt, wt, res, slot_s, carry, acc_s, s_ref,
                 recv, outb, kmat, ids, con_lo, con_hi, u_s, fh_s, fl_s, v_s, oh_e, oh_h,
                 dsend, drecv, esend, erecv, fsend, frecv, ffar, eq_s,
                 in_sem, k_sem, fs_sem, fr_sem, rs_sem, rr_sem, ds_sem, dr_sem, es_sem, er_sem, gs_sem, gr_sem, hs_sem, hr_sem):
    n = nx * ny
    gx = lax.axis_index("gx")
    yz = lax.axis_index("yz")
    me = gx * ny + yz
    dev = lambda t: (t // ny, lax.rem(t, ny))
    ins = [pltpu.make_async_copy(src, dst, in_sem.at[k]) for k, (src, dst) in enumerate(
        ((loc_hbm, loc_ref), (w_hbm, w_ref), (pr_hbm, pr_ref), (an_hbm, an_ref), (fn_hbm, fn_ref)))]
    for cp in ins:
        cp.start()
    kcopy = pltpu.make_async_copy(k_hbm, kmat, k_sem)
    barrier = pltpu.get_barrier_semaphore()

    gx_at = [lax.rem(gx + a, nx) for a in range(nx)]

    def greet(b, _):
        y = lax.rem(yz + b, ny)
        for a in range(nx):
            pl.semaphore_signal(barrier, inc=1, device_id=(gx_at[a], y), device_id_type=MESH)
        return 0
    lax.fori_loop(1, ny, greet, 0)
    for a in range(1, nx):
        pl.semaphore_signal(barrier, inc=1, device_id=(gx_at[a], yz), device_id_type=MESH)

    sub8 = lax.broadcasted_iota(jnp.int32, (8, 128), 0)
    sub128 = lax.broadcasted_iota(jnp.int32, (128, 128), 0)
    weights = mix_weights(shapes)

    halo_lo = [jnp.broadcast_to(halo_ref[r:r + 1, :] & 127, (8, 128)) for r in range(2)]
    halo_hi = [jnp.broadcast_to(halo_ref[r:r + 1, :] >> 7, (8, 128)) for r in range(2)]
    stack = lambda ref, c: jnp.concatenate([ref[c:c + 1, 128 * h:128 * h + 128] for h in range(8)], axis=0)
    disp = [stack(disp_ref, c) for c in range(3)]
    vel = [stack(vel_ref, c) for c in range(3)]
    mass = stack(mass_ref, 0)

    def arrive_lists():
        ins[0].wait()
        ins[1].wait()

    def arrive_blocks():
        for cp in ins[2:]:
            cp.wait()
        kcopy.start()
    rank_part(tgt_ref, slot_s, carry)
    stencil_part(fb_ref, pr_ref, loc_ref, w_ref, an_ref, trac, tab32, tab, idxt, wt, res, arrive_lists, arrive_blocks)
    pack_part(tgt_ref, fn_ref, trac, slot_s, acc_s, s_ref)
    pl.semaphore_wait(barrier, n - 1)

    def near(src, dst, ss, rs, t):
        return pltpu.make_async_remote_copy(src_ref=src, dst_ref=dst, send_sem=ss, recv_sem=rs, device_id=dev(t), device_id_type=MESH)

    def hop(send, recv, ss, rs, dist):
        return (near(send(1), recv(0), ss(1), rs(0), lax.rem(me + dist, n)),
                near(send(0), recv(1), ss(0), rs(1), lax.rem(me + n - dist, n)), dist)

    def start_both(copies):
        up, down, dist = copies

        @pl.when(me < n - dist)
        def _():
            up.start()

        @pl.when(me >= dist)
        def _():
            down.start()

    def wait_both(copies):
        up, down, dist = copies

        @pl.when(me < n - dist)
        def _():
            up.wait_send()
            down.wait_recv()

        @pl.when(me >= dist)
        def _():
            down.wait_send()
            up.wait_recv()

    at = lambda ref, *lead: lambda side: ref.at[(*lead, side)]
    state_copies = hop(at(dsend), at(drecv), at(ds_sem), at(dr_sem), 1)
    load_copies = hop(at(esend), at(erecv), at(es_sem), at(er_sem), 1)
    force_copies = lambda step: hop(at(fsend, step), at(frecv, step), at(gs_sem, step), at(gr_sem, step), 1)
    far_copies = lambda step: hop(at(fsend, step), at(ffar, step), at(hs_sem, step), at(hr_sem, step), 2)
    exists = [me > 0, me < n - 1]
    exists_far = [me > 1, me < n - 2]

    def pick(r, x):
        g = jnp.where(halo_hi[r] == sub8, lane_take(x, halo_lo[r]), F32(0))
        return jnp.sum(g, axis=0, keepdims=True)

    def send_state():
        for r in range(2):
            for c in range(3):
                dsend[r, c:c + 1, :] = pick(r, disp[c])
                dsend[r, 3 + c:4 + c, :] = pick(r, vel[c])
            dsend[r, 6:7, :] = pick(r, mass)
            dsend[r, 8:10, :] = halo_ref[...].astype(F32)
        start_both(state_copies)

    def ghost_state():
        wait_both(state_copies)
        gd = [jnp.where(exists[k], drecv[k, 0:3, :], F32(0)) for k in range(2)]
        gv = [jnp.where(exists[k], drecv[k, 3:6, :], F32(0)) for k in range(2)]
        gm = [jnp.where(exists[k], drecv[k, 6:7, :], F32(1)) for k in range(2)]
        for k in range(2):
            held, other = drecv[k, 9 - k:10 - k, :], drecv[k, 8 + k:9 + k, :]
            for m, x in enumerate((held, other)):
                same = jnp.broadcast_to(x, (128, 128)).T == jnp.broadcast_to(held, (128, 128))
                eq_s[k, 128 * m:128 * m + 128, :] = jnp.where(same, F32(1), F32(0)).astype(BF16)
        return gd, gv, gm

    def advance_ghosts(step, ge, gd, gv, gm):
        wait_both(far_copies(step))
        for k in range(2):
            x = jnp.concatenate([fsend[step, k], jnp.where(exists_far[k], ffar[step, k], F32(0))], axis=1)
            xh = x.astype(BF16).astype(F32)
            both = jnp.dot(jnp.concatenate([xh, x - xh], axis=0).astype(BF16), eq_s[k], preferred_element_type=F32)
            total = frecv[step, k, 3:6, :] + (both[0:3] + both[8:11])
            v = gv[k] + (ge[k] - total) / gm[k]
            gv[k] = jnp.where(exists[k], v, F32(0))
            gd[k] = gd[k] + gv[k]

    def internal(step, disp, ghost):
        for c in range(3):
            rows = [disp[c][h:h + 1, :] for h in range(8)] + [ghost[0][c:c + 1, :], ghost[1][c:c + 1, :]]
            rows = [jnp.broadcast_to(r, (8, 128)) for r in rows]
            for at in range(3):
                for e in range(2):
                    lo = con_lo[8 * at:8 * at + 8, 128 * e:128 * e + 128]
                    hi = con_hi[8 * at:8 * at + 8, 128 * e:128 * e + 128]
                    acc = lane_take(rows[0], lo)
                    for h in range(1, 10):
                        acc = jnp.where(hi == h, lane_take(rows[h], lo), acc)
                    u_s[c, 8 * at:8 * at + 8, 128 * e:128 * e + 128] = acc

        def multiply(a, acc):
            for c in range(3):
                acc = acc + kmat[c * 20 + a] * u_s[c, pl.ds(a, 1), :]
            return acc
        force = lax.fori_loop(0, 20, multiply, jnp.zeros((60, 256), F32))
        fh = force.astype(BF16).astype(F32)
        fh_s[...] = fh
        fl_s[...] = force - fh
        sub16 = lax.broadcasted_iota(jnp.int32, (16, 256), 0)
        for a in range(20):
            mask = jnp.broadcast_to(con_hi[a:a + 1, :], (16, 256)) == sub16
            for c in range(3):
                for k, part in enumerate((fh_s, fl_s)):
                    row = jnp.broadcast_to(part[20 * c + a:20 * c + a + 1, :], (16, 256))
                    v_s[48 * k + 16 * c:48 * k + 16 * c + 16, a * 256:a * 256 + 256] = jnp.where(mask, row, F32(0)).astype(BF16)
        both = jnp.dot(v_s[...], oh_e[...], preferred_element_type=F32)
        total = both[:48] + both[48:]
        own = [total[16 * c:16 * c + 8, :] for c in range(3)]
        for k in range(2):
            for c in range(3):
                fsend[step, k, c:c + 1, :] = total[16 * c + 8 + k:16 * c + 9 + k, :]
                fsend[step, k, 3 + c:4 + c, :] = pick(k, own[c])
            fsend[step, k, 6:8, :] = jnp.zeros((2, 128), F32)
        start_both(force_copies(step))
        if step < SUBSTEPS - 1:
            start_both(far_copies(step))
        return own

    def advance(step, own, ext, disp, vel):
        wait_both(force_copies(step))
        got = [jnp.where(me > 0, frecv[step, 0, 0:3, :], F32(0)), jnp.where(me < n - 1, frecv[step, 1, 0:3, :], F32(0))]
        parts = []
        for c in range(3):
            cols = []
            for r in range(2):
                x = jnp.where(halo_hi[r] == sub8, jnp.broadcast_to(got[r][c:c + 1, :], (8, 128)), F32(0))
                cols.append(x)
            parts.append(jnp.concatenate(cols, axis=1))
        x = jnp.concatenate(parts, axis=0)
        xh = x.astype(BF16).astype(F32)
        lhs = jnp.concatenate([xh, x - xh], axis=0).astype(BF16)
        both = jnp.dot(lhs, oh_h[...], preferred_element_type=F32)
        add = both[:24] + both[24:]
        vel = [vel[c] + (ext[c] - (own[c] + add[8 * c:8 * c + 8, :])) / mass for c in range(3)]
        disp = [disp[c] + vel[c] for c in range(3)]
        return disp, vel

    tiles = n // 8
    mine = me // 8

    spread = [lax.rem(yz + s, 8) for s in range(8)]
    own_half = yz // 8

    def tile_at(k):
        d = k // 4
        step = lax.rem(2 + d + (d // 2) * (2 * d - 3), 4)
        g = lax.rem(gx + 2 * step, nx)
        g = g + (1 - 2 * lax.rem(g, 2)) * (1 - lax.rem(k // 2, 2))
        half = lax.rem(yz // 8 + 1 - lax.rem(k, 2), 2)
        return g, half

    send_state()

    def fwd(g, y):
        return pltpu.make_async_remote_copy(
            src_ref=s_ref.at[g * ny + y], dst_ref=recv.at[me], send_sem=fs_sem, recv_sem=fr_sem.at[mine],
            device_id=(g, y), device_id_type=MESH)

    def fwd_start(k, _):
        g, half = tile_at(k)
        for s in range(8):
            fwd(g, half * 8 + spread[s]).start()
        return 0
    lax.fori_loop(0, tiles - 1, fwd_start, 0)
    for s in range(1, 8):
        fwd(gx, own_half * 8 + spread[s]).start()
    recv[me] = s_ref[me]
    for dst in (con_lo, con_hi):
        dst[16:24, :] = jnp.zeros((8, 256), jnp.int32)
    con_lo[0:20, :] = con_ref[...] & 127
    con_hi[0:20, :] = con_ref[...] >> 7
    for a in range(20):
        for e in range(2):
            row = jnp.broadcast_to(con_lo[a:a + 1, 128 * e:128 * e + 128], (128, 128))
            oh_e[a * 256 + 128 * e:a * 256 + 128 * e + 128, :] = jnp.where(row == sub128, F32(1), F32(0)).T.astype(BF16)
    for r in range(2):
        row = jnp.broadcast_to(halo_ref[r:r + 1, :] & 127, (128, 128))
        oh_h[128 * r:128 * r + 128, :] = jnp.where(row == sub128, F32(1), F32(0)).T.astype(BF16)
    kcopy.wait()
    gd, gv, gm = ghost_state()
    own = internal(0, disp, gd)


    sub128h = lax.broadcasted_iota(jnp.int32, (128, 128), 0).astype(jnp.int16)

    def arrive(source, count):
        pltpu.make_async_remote_copy(
            src_ref=s_ref.at[pl.ds(0, count)], dst_ref=recv.at[pl.ds(0, count)], send_sem=fs_sem, recv_sem=fr_sem.at[source],
            device_id=(gx, yz), device_id_type=MESH).wait_recv()

    def load_of(source, acc):
        base = pl.multiple_of(source * 8, 8)
        get = lambda r: recv[pl.ds(base, 8), r, :]
        loads = []
        for c in range(3):
            t0, t1 = get(2 * c), get(2 * c + 1)
            r0, r1 = pltpu.roll(t0, 64, 1), pltpu.roll(t1, 64, 1)
            loads.append([weights[j][0] * t0 + weights[j][1] * r0 + weights[j][2] * t1 + weights[j][3] * r1 for j in range(4)])
        total = jnp.zeros((48, 128), F32)
        for j in range(4):
            idx = get(6 + j).astype(jnp.int32)
            ids[j, pl.ds(base, 8), :] = idx
            lo, hi = idx & 127, idx >> 7
            highs = [loads[c][j].astype(BF16).astype(F32) for c in range(3)]
            lows = [loads[c][j] - highs[c] for c in range(3)]
            for s in range(0, 8, 2):
                hots, vals = [], []
                for k in (s, s + 1):
                    row = jnp.broadcast_to(lo[k:k + 1, :], (128, 128)).astype(jnp.int16)
                    hots.append(jnp.where(row == sub128h, BF16(1), BF16(0)))
                    mask = jnp.broadcast_to(hi[k:k + 1, :], (8, 128)) == sub8
                    vals.append(jnp.concatenate(
                        [jnp.where(mask, jnp.broadcast_to(p[k:k + 1, :], (8, 128)), F32(0)) for p in highs + lows], axis=0).astype(BF16))
                total = total + lax.dot_general(
                    jnp.concatenate(vals, axis=1), jnp.concatenate(hots, axis=1), (((1,), (1,)), ((), ())), preferred_element_type=F32)
        return acc + total
    def gather_load(k, acc):
        sources = []
        for m in range(3):
            g, half = tile_at(3 * k + m)
            sources.append(g * 2 + half)
            arrive(sources[m], 8)
        for source in sources:
            acc = load_of(source, acc)
        return acc

    both = lax.fori_loop(0, (tiles - 1) // 3, gather_load, jnp.zeros((48, 128), F32))
    arrive(mine, 7)
    both = load_of(mine, both)
    ext = [both[8 * c:8 * c + 8] + both[24 + 8 * c:32 + 8 * c] for c in range(3)]

    for r in range(2):
        for c in range(3):
            esend[r, c:c + 1, :] = pick(r, ext[c])
        esend[r, 3:8, :] = jnp.zeros((5, 128), F32)
    start_both(load_copies)
    disp, vel = advance(0, own, ext, disp, vel)
    wait_both(load_copies)
    ge = [jnp.where(exists[k], erecv[k, 0:3, :], F32(0)) for k in range(2)]
    advance_ghosts(0, ge, gd, gv, gm)
    for step in range(1, SUBSTEPS):
        own = internal(step, disp, gd)
        disp, vel = advance(step, own, ext, disp, vel)
        if step < SUBSTEPS - 1:
            advance_ghosts(step, ge, gd, gv, gm)
    for c in range(3):
        for h in range(8):
            at_row = 32 + 8 * c + h
            ret_ref[n + at_row // 6, at_row % 6:at_row % 6 + 1, :] = disp[c][h:h + 1, :]
            u_s[c, h:h + 1, 0:128] = disp[c][h:h + 1, :]
    for r in range(32):
        ret_ref[n + r // 6, r % 6:r % 6 + 1, :] = slot_s[:, 128 * r:128 * r + 128].astype(F32)

    def ret(g, y):
        return pltpu.make_async_remote_copy(
            src_ref=outb.at[g * ny + y], dst_ref=ret_ref.at[me], send_sem=rs_sem, recv_sem=rr_sem,
            device_id=(g, y), device_id_type=MESH)

    def back(k, _):
        pair = [tile_at(2 * k + m) for m in range(2)]
        for g, half in pair:
            base = pl.multiple_of((g * 2 + half) * 8, 8)
            sums = [[jnp.zeros((8, 128), F32)] * 4 for c in range(3)]
            for j in range(4):
                idx = ids[j, pl.ds(base, 8), :]
                lo, hi = idx & 127, idx >> 7
                masks = [hi == h for h in range(1, 8)]
                for c in range(3):
                    acc = lane_take(jnp.broadcast_to(u_s[c, 0:1, 0:128], (8, 128)), lo)
                    for h in range(1, 8):
                        acc = jnp.where(masks[h - 1], lane_take(jnp.broadcast_to(u_s[c, h:h + 1, 0:128], (8, 128)), lo), acc)
                    sums[c] = [sums[c][m] + weights[j][m] * acc for m in range(4)]
            for c in range(3):
                p0, q0, p1, q1 = sums[c]
                outb[pl.ds(base, 8), 2 * c, :] = p0 + pltpu.roll(q0, 64, 1)
                outb[pl.ds(base, 8), 2 * c + 1, :] = p1 + pltpu.roll(q1, 64, 1)
        for g, half in pair:
            for s in range(8):
                y = half * 8 + lax.rem(yz + s, 8)

                @pl.when(g * ny + y != me)
                def _():
                    ret(g, y).start()
        return 0
    lax.fori_loop(0, tiles // 2, back, 0)
    ret_ref[me] = outb[me]

    def every(src, dst, ss, rs):
        return pltpu.make_async_remote_copy(
            src_ref=src.at[pl.ds(0, n - 1)], dst_ref=dst.at[pl.ds(0, n - 1)], send_sem=ss, recv_sem=rs,
            device_id=(gx, yz), device_id_type=MESH)
    every(s_ref, recv, fs_sem, fr_sem.at[0]).wait_send()
    last = every(outb, ret_ref, rs_sem, rr_sem)
    last.wait_send()
    last.wait_recv()


def solid(face_block, pressure, local, weight, area, nodes, target, stiffness, connect, halo, mass, disp, vel, nx, ny, shapes):
    n = nx * ny
    V = pl.BlockSpec(memory_space=pltpu.VMEM)
    A = pl.BlockSpec(memory_space=pl.ANY)
    D = pltpu.SemaphoreType.DMA
    M = pltpu.VMEM
    I32 = jnp.int32
    back = pl.pallas_call(
        functools.partial(solid_kernel, nx, ny, shapes),
        out_shape=jax.ShapeDtypeStruct((n + 10, 6, 128), F32),
        in_specs=[pl.BlockSpec(memory_space=pltpu.SMEM), A, A, A, A, A, V, A, V, V, V, V, V],
        out_specs=V,
        scratch_shapes=[
            M(pressure.shape, BF16), M(local.shape, I32), M(weight.shape, F32), M(area.shape, F32), M(nodes.shape, I32),
            M(area.shape, F32), M((16 * STRIDE, 128), F32), M((256, 32, 128), BF16), M((1024, 128), I32), M((1024, 128), F32),
            M((1024, 128), F32), M(target.shape, I32), M((128, 256), F32), M((640, 256), F32),
            M((n, 10, 128), F32),
            M((n, 10, 128), F32), M((n, 6, 128), F32), M((60, 60, 256), F32),
            M((4, n, 128), I32), M((24, 256), I32), M((24, 256), I32),
            M((3, 24, 256), F32), M((60, 256), F32), M((60, 256), F32),
            M((96, 5120), BF16), M((5120, 128), BF16), M((256, 128), BF16),
            M((2, 16, 128), F32), M((2, 16, 128), F32), M((2, 8, 128), F32), M((2, 8, 128), F32),
            M((SUBSTEPS, 2, 8, 128), F32), M((SUBSTEPS, 2, 8, 128), F32), M((SUBSTEPS, 2, 8, 128), F32), M((2, 256, 128), BF16),
            D((5,)), D, D, D((n // 8,)), D, D, D((2,)), D((2,)), D((2,)), D((2,)),
            D((SUBSTEPS, 2)), D((SUBSTEPS, 2)), D((SUBSTEPS, 2)), D((SUBSTEPS, 2))],
        compiler_params=pltpu.CompilerParams(collective_id=0, has_side_effects=True, vmem_limit_bytes=56 * 2**20),
        name="solid",
    )(face_block, pressure, local, weight, area, nodes, target, stiffness, connect, halo, mass.reshape(1, -1), disp, vel)
    return pl.pallas_call(
        functools.partial(unpack_kernel, n),
        out_shape=(jax.ShapeDtypeStruct(disp.shape, F32), jax.ShapeDtypeStruct((12, target.shape[1]), F32)),
        in_specs=[V, V],
        out_specs=(V, V),
        scratch_shapes=[M(target.shape, I32), M((768, 256), BF16)],
        compiler_params=pltpu.CompilerParams(vmem_limit_bytes=24 * 2**20),
        name="unpack",
    )(target, back)


def shape_table():
    corner_u = [-1, 1, 1, -1, 0, 1, 0, -1]
    corner_v = [-1, -1, 1, 1, -1, 0, 1, 0]
    gauss_point = 1.0 / math.sqrt(3.0)
    points = [
        (-gauss_point, -gauss_point),
        (gauss_point, -gauss_point),
        (gauss_point, gauss_point),
        (-gauss_point, gauss_point),
    ]
    shape_values = np.zeros((4, 8), np.float32)
    for position, (coord_u, coord_v) in enumerate(points):
        for corner in range(8):
            node_u = corner_u[corner]
            node_v = corner_v[corner]
            if corner < 4:
                entry_value = (
                    0.25
                    * (1 + coord_u * node_u)
                    * (1 + coord_v * node_v)
                    * (coord_u * node_u + coord_v * node_v - 1)
                )
            elif node_u == 0:
                entry_value = 0.5 * (1 - coord_u * coord_u) * (1 + coord_v * node_v)
            else:
                entry_value = 0.5 * (1 + coord_u * node_u) * (1 - coord_v * coord_v)
            shape_values[position, corner] = entry_value
    return shape_values


def shards(
    pressure,
    face_block,
    stencil_local,
    stencil_weight,
    area_normal,
    face_part,
    face_nodes,
    stiffness,
    connect,
    halo_nodes,
    node_mass,
    displacement,
    velocity,
):
    gx_size = lax.axis_size("gx")
    yz_size = lax.axis_size("yz")
    return solid(
        face_block, pressure, stencil_local, stencil_weight, area_normal, face_nodes, face_part.reshape(1, -1),
        stiffness, connect, halo_nodes, node_mass, displacement, velocity, gx_size, yz_size, shape_table()
    )


def solution(mesh):
    in_specs = (
        P(("gx", "yz"), None),
        P(("gx", "yz")),
        P(None, ("gx", "yz")),
        P(None, ("gx", "yz")),
        P(None, ("gx", "yz")),
        P(("gx", "yz"), None),
        P(None, ("gx", "yz")),
        P(None, None, ("gx", "yz")),
        P(None, ("gx", "yz")),
        P(None, ("gx", "yz")),
        P(("gx", "yz")),
        P(None, ("gx", "yz")),
        P(None, ("gx", "yz")),
    )
    out_specs = (P(None, ("gx", "yz")), P(None, ("gx", "yz")))
    return jax.shard_map(shards, mesh=mesh, in_specs=in_specs, out_specs=out_specs, check_vma=False)
```

```python
import functools
import math

import jax
import jax.numpy as jnp
import numpy as np
from jax import lax
from jax.experimental import pallas as pl
from jax.experimental.pallas import tpu as pltpu
from jax.sharding import PartitionSpec as P

MESH = pl.DeviceIdType.MESH
F32 = jnp.float32
BF16 = jnp.bfloat16
SUBSTEPS = 4

def half_lanes(left, right):
    lane = lax.broadcasted_iota(jnp.int32, (8, 128), 1)
    return jnp.where(lane < 64, F32(left), F32(right))

def mix_weights(shapes):
    pick = lambda q, a: float(shapes[q, a])
    out = []
    for j in range(4):
        e, o = 2 * j, 2 * j + 1
        out.append((
            half_lanes(pick(0, e), pick(1, o)), half_lanes(pick(1, e), pick(0, o)),
            half_lanes(pick(2, e), pick(3, o)), half_lanes(pick(3, e), pick(2, o))))
    return out

STRIDE = 40
UNR = 128
TAKE = lax.GatherDimensionNumbers(
    offset_dims=(), collapsed_slice_dims=(1,), start_index_map=(1,), operand_batching_dims=(0,), start_indices_batching_dims=(0,)
)

def lane_take(x, idx):
    return lax.gather(x, idx[..., None], TAKE, slice_sizes=(1, 1), mode=lax.GatherScatterMode.PROMISE_IN_BOUNDS)

def stencil_part(fb_ref, pr_ref, loc_ref, w_ref, an_ref, out_ref, tab32, tab, idxt, wt, res, arrive_lists, arrive_blocks):
    arrive_lists()
    for i in range(8):
        idxt[128 * i:128 * i + 128, :] = jnp.concatenate(
            [loc_ref[:, a * 1024 + 128 * i:a * 1024 + 128 * i + 128] for a in range(4)], axis=0).T
        wt[128 * i:128 * i + 128, :] = jnp.concatenate(
            [w_ref[:, a * 1024 + 128 * i:a * 1024 + 128 * i + 128] for a in range(4)], axis=0).T
    arrive_blocks()

    def relayout(b, _):
        r0 = pl.multiple_of(b * 16, 16)
        for t in range(32):
            x = pr_ref[pl.ds(r0, 16), 128 * t:128 * t + 128].astype(jnp.float32)
            tab32[pl.ds(t, 8, stride=STRIDE), :] = x[:8]
            tab32[pl.ds(8 * STRIDE + t, 8, stride=STRIDE), :] = x[8:]
        for n in range(16):
            tab[r0 + n] = tab32[n * STRIDE:n * STRIDE + 32, :].astype(jnp.bfloat16)
        return 0
    lax.fori_loop(0, 16, relayout, 0)
    lane = lax.broadcasted_iota(jnp.int32, (16, 128), 1)
    sub = lax.broadcasted_iota(jnp.int32, (16, 128), 0).astype(jnp.int16)
    grp = (lane // 32).astype(jnp.int16)
    m_lo = grp < 2
    m0 = grp == 0
    m2 = grp == 2

    def main(gg, _):
        for uu in range(UNR // 8):
            base = pl.multiple_of(gg * UNR + 8 * uu, 8)
            rows = []
            for u in range(8):
                g = base + u
                row = jnp.broadcast_to(idxt[pl.ds(g, 1), :], (16, 128))
                lo = (row & 127).astype(jnp.int16)
                hi = (row >> 7).astype(jnp.int16)
                cl = hi < 16
                mine = (hi & 15) == sub
                xs = []
                for a in range(4):
                    block = tab[fb_ref[a * 1024 + g]]
                    xs.append(jnp.where(cl, lane_take(block[:16], lo), lane_take(block[16:], lo)))
                x = jnp.where(m_lo, jnp.where(m0, xs[0], xs[1]), jnp.where(m2, xs[2], xs[3]))
                x = jnp.where(mine, x, jnp.bfloat16(0)).astype(jnp.float32)
                rows.append(jnp.sum(x[:8] + x[8:], axis=0, keepdims=True))
            res[pl.ds(base, 8), :] = jnp.concatenate(rows, axis=0) * wt[pl.ds(base, 8), :]
        return 0
    lax.fori_loop(0, 1024 // UNR, main, 0)
    for i in range(8):
        rt = res[128 * i:128 * i + 128, :].T
        for a in range(4):
            f0 = a * 1024 + 128 * i
            fp = jnp.concatenate([jnp.sum(rt[a * 32 + 8 * q:a * 32 + 8 * q + 8], axis=0, keepdims=True) for q in range(4)], axis=0)
            fp3 = jnp.concatenate([fp, fp, fp], axis=0)
            out_ref[:, f0:f0 + 128] = -(an_ref[:, f0:f0 + 128] * fp3)


def rank_part(tgt_ref, slot_s, carry):
    wide = 2048
    rows128 = lax.broadcasted_iota(jnp.int32, (128, 256), 0)
    rows256 = lax.broadcasted_iota(jnp.int32, (256, 256), 0)
    cols256 = lax.broadcasted_iota(jnp.int32, (256, 256), 1)
    one_if = lambda m: jnp.where(m, F32(1), F32(0)).astype(BF16)
    upper = one_if(rows256 < cols256)
    ones = jnp.ones((256, 256), BF16)
    carry[...] = jnp.zeros_like(carry)

    def rank(kt, _):
        before = carry[...]
        for m in range(8):
            at = pl.ds(pl.multiple_of(kt * wide + 256 * m, 256), 256)
            hit = jnp.broadcast_to(tgt_ref[:, at], (128, 256)) == rows128
            hot = one_if(hit)
            within = jnp.dot(hot, upper, preferred_element_type=F32) + before
            slot_s[:, at] = jnp.sum(jnp.where(hit, within, F32(0)), axis=0, keepdims=True).astype(jnp.int32)
            before = before + jnp.dot(hot, ones, preferred_element_type=F32)
        carry[...] = before
        return 0
    lax.fori_loop(0, 2, rank, 0)


def pack_part(tgt_ref, fn_ref, trac, slot_s, acc, send_ref):
    wide = 2048
    rows128 = lax.broadcasted_iota(jnp.int32, (128, 256), 0)
    rows256 = lax.broadcasted_iota(jnp.int32, (256, 256), 0)
    cols256 = lax.broadcasted_iota(jnp.int32, (256, 256), 1)
    rows256w = lax.broadcasted_iota(jnp.int32, (256, wide), 0)
    rows32 = lax.broadcasted_iota(jnp.int32, (32, wide), 0)
    one_if = lambda m: jnp.where(m, F32(1), F32(0)).astype(BF16)
    acc[...] = jnp.zeros_like(acc)

    def tile(kt, _):
        at = pl.ds(pl.multiple_of(kt * wide, wide), wide)
        slot = slot_s[:, at]
        place = jnp.broadcast_to(tgt_ref[:, at] + 128 * (slot >> 5), (256, wide))
        weights = one_if(place == rows256w)
        mask = jnp.broadcast_to(slot & 31, (32, wide)) == rows32
        values = [trac[:, at], fn_ref[:, at].astype(F32)]
        total = None
        highs = [v.astype(BF16).astype(F32) for v in values]
        for part in (highs, [v - h for v, h in zip(values, highs)]):
            x = [
                jnp.where(mask, jnp.broadcast_to(p[r:r + 1, :], (32, wide)), F32(0)).astype(BF16)
                for p in part
                for r in range(p.shape[0])
            ]
            y = lax.dot_general(jnp.concatenate(x, axis=0), weights, (((1,), (1,)), ((), ())), preferred_element_type=F32)
            total = y if total is None else total + y
        acc[...] += total
        return 0
    lax.fori_loop(0, 2, tile, 0)
    for r in range(10):
        block = [acc[32 * v:32 * v + 32, 128 * h:128 * h + 128] for v in (2 * r, 2 * r + 1) for h in range(2)]
        send_ref[:, r, :] = jnp.concatenate(block, axis=0).T


def unpack_kernel(n, tgt_ref, ret_ref, nd_ref, fd_ref, slot_s, lhs):
    for r in range(56):
        row = ret_ref[n + r // 6, r % 6:r % 6 + 1, :]
        if r < 32:
            slot_s[:, 128 * r:128 * r + 128] = row.astype(jnp.int32)
        else:
            c, h = divmod(r - 32, 8)
            nd_ref[c:c + 1, 128 * h:128 * h + 128] = row
    wide = 2048
    rows128 = lax.broadcasted_iota(jnp.int32, (128, wide), 0)
    rows64 = lax.broadcasted_iota(jnp.int32, (64, wide), 0)
    for r in range(6):
        x = ret_ref[0:n, r, :].T
        xh = x.astype(BF16).astype(F32)
        lhs[128 * r:128 * r + 128, :] = jnp.concatenate([xh, x - xh], axis=1).astype(BF16)

    def tile(kt, _):
        at = pl.ds(pl.multiple_of(kt * wide, wide), wide)
        hot = jnp.where(jnp.broadcast_to(tgt_ref[:, at], (128, wide)) == rows128, F32(1), F32(0)).astype(BF16)
        y = jnp.dot(lhs[...], jnp.concatenate([hot, hot], axis=0), preferred_element_type=F32)
        mask = jnp.broadcast_to(slot_s[:, at], (64, wide)) == rows64
        fd_ref[:, at] = jnp.concatenate(
            [jnp.sum(jnp.where(mask, y[64 * v:64 * v + 64, :], F32(0)), axis=0, keepdims=True) for v in range(12)], axis=0
        )
        return 0
    lax.fori_loop(0, 2, tile, 0)


def solid_kernel(nx, ny, shapes, fb_ref, pr_hbm, loc_hbm, w_hbm, an_hbm, fn_hbm, tgt_ref, k_hbm, con_ref, halo_ref, mass_ref, disp_ref, vel_ref,
                 ret_ref,
                 pr_ref, loc_ref, w_ref, an_ref, fn_ref, trac, tab32, tab, idxt, wt, res, slot_s, carry, acc_s, s_ref,
                 recv, outb, kmat, ids, con_lo, con_hi, u_s, fh_s, fl_s, v_s, oh_e, oh_h,
                 dsend, drecv, esend, erecv, fsend, frecv, ffar, eq_s,
                 in_sem, k_sem, fs_sem, fr_sem, rs_sem, rr_sem, ds_sem, dr_sem, es_sem, er_sem, gs_sem, gr_sem, hs_sem, hr_sem):
    n = nx * ny
    gx = lax.axis_index("gx")
    yz = lax.axis_index("yz")
    me = gx * ny + yz
    dev = lambda t: (t // ny, lax.rem(t, ny))
    ins = [pltpu.make_async_copy(src, dst, in_sem.at[k]) for k, (src, dst) in enumerate(
        ((loc_hbm, loc_ref), (w_hbm, w_ref), (pr_hbm, pr_ref), (an_hbm, an_ref), (fn_hbm, fn_ref)))]
    for cp in ins:
        cp.start()
    kcopy = pltpu.make_async_copy(k_hbm, kmat, k_sem)
    barrier = pltpu.get_barrier_semaphore()

    gx_at = [lax.rem(gx + a, nx) for a in range(nx)]

    def greet(b, _):
        y = lax.rem(yz + b, ny)
        for a in range(nx):
            pl.semaphore_signal(barrier, inc=1, device_id=(gx_at[a], y), device_id_type=MESH)
        return 0
    lax.fori_loop(1, ny, greet, 0)
    for a in range(1, nx):
        pl.semaphore_signal(barrier, inc=1, device_id=(gx_at[a], yz), device_id_type=MESH)

    sub8 = lax.broadcasted_iota(jnp.int32, (8, 128), 0)
    sub128 = lax.broadcasted_iota(jnp.int32, (128, 128), 0)
    weights = mix_weights(shapes)

    halo_lo = [jnp.broadcast_to(halo_ref[r:r + 1, :] & 127, (8, 128)) for r in range(2)]
    halo_hi = [jnp.broadcast_to(halo_ref[r:r + 1, :] >> 7, (8, 128)) for r in range(2)]
    stack = lambda ref, c: jnp.concatenate([ref[c:c + 1, 128 * h:128 * h + 128] for h in range(8)], axis=0)
    disp = [stack(disp_ref, c) for c in range(3)]
    vel = [stack(vel_ref, c) for c in range(3)]
    mass = stack(mass_ref, 0)

    def arrive_lists():
        ins[0].wait()
        ins[1].wait()

    def arrive_blocks():
        for cp in ins[2:]:
            cp.wait()
        kcopy.start()
    rank_part(tgt_ref, slot_s, carry)
    stencil_part(fb_ref, pr_ref, loc_ref, w_ref, an_ref, trac, tab32, tab, idxt, wt, res, arrive_lists, arrive_blocks)
    pack_part(tgt_ref, fn_ref, trac, slot_s, acc_s, s_ref)
    pl.semaphore_wait(barrier, n - 1)

    def near(src, dst, ss, rs, t):
        return pltpu.make_async_remote_copy(src_ref=src, dst_ref=dst, send_sem=ss, recv_sem=rs, device_id=dev(t), device_id_type=MESH)

    def hop(send, recv, ss, rs, dist):
        return (near(send(1), recv(0), ss(1), rs(0), lax.rem(me + dist, n)),
                near(send(0), recv(1), ss(0), rs(1), lax.rem(me + n - dist, n)), dist)

    def start_both(copies):
        up, down, dist = copies

        @pl.when(me < n - dist)
        def _():
            up.start()

        @pl.when(me >= dist)
        def _():
            down.start()

    def wait_both(copies):
        up, down, dist = copies

        @pl.when(me < n - dist)
        def _():
            up.wait_send()
            down.wait_recv()

        @pl.when(me >= dist)
        def _():
            down.wait_send()
            up.wait_recv()

    at = lambda ref, *lead: lambda side: ref.at[(*lead, side)]
    state_copies = hop(at(dsend), at(drecv), at(ds_sem), at(dr_sem), 1)
    load_copies = hop(at(esend), at(erecv), at(es_sem), at(er_sem), 1)
    force_copies = lambda step: hop(at(fsend, step), at(frecv, step), at(gs_sem, step), at(gr_sem, step), 1)
    far_copies = lambda step: hop(at(fsend, step), at(ffar, step), at(hs_sem, step), at(hr_sem, step), 2)
    exists = [me > 0, me < n - 1]
    exists_far = [me > 1, me < n - 2]

    def pick(r, x):
        g = jnp.where(halo_hi[r] == sub8, lane_take(x, halo_lo[r]), F32(0))
        return jnp.sum(g, axis=0, keepdims=True)

    def send_state():
        for r in range(2):
            for c in range(3):
                dsend[r, c:c + 1, :] = pick(r, disp[c])
                dsend[r, 3 + c:4 + c, :] = pick(r, vel[c])
            dsend[r, 6:7, :] = pick(r, mass)
            dsend[r, 8:10, :] = halo_ref[...].astype(F32)
        start_both(state_copies)

    def ghost_state():
        wait_both(state_copies)
        gd = [jnp.where(exists[k], drecv[k, 0:3, :], F32(0)) for k in range(2)]
        gv = [jnp.where(exists[k], drecv[k, 3:6, :], F32(0)) for k in range(2)]
        gm = [jnp.where(exists[k], drecv[k, 6:7, :], F32(1)) for k in range(2)]
        for k in range(2):
            held, other = drecv[k, 9 - k:10 - k, :], drecv[k, 8 + k:9 + k, :]
            for m, x in enumerate((held, other)):
                same = jnp.broadcast_to(x, (128, 128)).T == jnp.broadcast_to(held, (128, 128))
                eq_s[k, 128 * m:128 * m + 128, :] = jnp.where(same, F32(1), F32(0)).astype(BF16)
        return gd, gv, gm

    def advance_ghosts(step, ge, gd, gv, gm):
        wait_both(far_copies(step))
        for k in range(2):
            x = jnp.concatenate([fsend[step, k], jnp.where(exists_far[k], ffar[step, k], F32(0))], axis=1)
            xh = x.astype(BF16).astype(F32)
            both = jnp.dot(jnp.concatenate([xh, x - xh], axis=0).astype(BF16), eq_s[k], preferred_element_type=F32)
            total = frecv[step, k, 3:6, :] + (both[0:3] + both[8:11])
            v = gv[k] + (ge[k] - total) / gm[k]
            gv[k] = jnp.where(exists[k], v, F32(0))
            gd[k] = gd[k] + gv[k]

    def internal(step, disp, ghost):
        for c in range(3):
            rows = [disp[c][h:h + 1, :] for h in range(8)] + [ghost[0][c:c + 1, :], ghost[1][c:c + 1, :]]
            rows = [jnp.broadcast_to(r, (8, 128)) for r in rows]
            for at in range(3):
                for e in range(2):
                    lo = con_lo[8 * at:8 * at + 8, 128 * e:128 * e + 128]
                    hi = con_hi[8 * at:8 * at + 8, 128 * e:128 * e + 128]
                    acc = lane_take(rows[0], lo)
                    for h in range(1, 10):
                        acc = jnp.where(hi == h, lane_take(rows[h], lo), acc)
                    u_s[c, 8 * at:8 * at + 8, 128 * e:128 * e + 128] = acc

        def multiply(a, acc):
            for c in range(3):
                acc = acc + kmat[c * 20 + a] * u_s[c, pl.ds(a, 1), :]
            return acc
        force = lax.fori_loop(0, 20, multiply, jnp.zeros((60, 256), F32))
        fh = force.astype(BF16).astype(F32)
        fh_s[...] = fh
        fl_s[...] = force - fh
        sub16 = lax.broadcasted_iota(jnp.int32, (16, 256), 0)
        for a in range(20):
            mask = jnp.broadcast_to(con_hi[a:a + 1, :], (16, 256)) == sub16
            for c in range(3):
                for k, part in enumerate((fh_s, fl_s)):
                    row = jnp.broadcast_to(part[20 * c + a:20 * c + a + 1, :], (16, 256))
                    v_s[48 * k + 16 * c:48 * k + 16 * c + 16, a * 256:a * 256 + 256] = jnp.where(mask, row, F32(0)).astype(BF16)
        both = jnp.dot(v_s[...], oh_e[...], preferred_element_type=F32)
        total = both[:48] + both[48:]
        own = [total[16 * c:16 * c + 8, :] for c in range(3)]
        for k in range(2):
            for c in range(3):
                fsend[step, k, c:c + 1, :] = total[16 * c + 8 + k:16 * c + 9 + k, :]
                fsend[step, k, 3 + c:4 + c, :] = pick(k, own[c])
            fsend[step, k, 6:8, :] = jnp.zeros((2, 128), F32)
        start_both(force_copies(step))
        if step < SUBSTEPS - 1:
            start_both(far_copies(step))
        return own

    def advance(step, own, ext, disp, vel):
        wait_both(force_copies(step))
        got = [jnp.where(me > 0, frecv[step, 0, 0:3, :], F32(0)), jnp.where(me < n - 1, frecv[step, 1, 0:3, :], F32(0))]
        parts = []
        for c in range(3):
            cols = []
            for r in range(2):
                x = jnp.where(halo_hi[r] == sub8, jnp.broadcast_to(got[r][c:c + 1, :], (8, 128)), F32(0))
                cols.append(x)
            parts.append(jnp.concatenate(cols, axis=1))
        x = jnp.concatenate(parts, axis=0)
        xh = x.astype(BF16).astype(F32)
        lhs = jnp.concatenate([xh, x - xh], axis=0).astype(BF16)
        both = jnp.dot(lhs, oh_h[...], preferred_element_type=F32)
        add = both[:24] + both[24:]
        vel = [vel[c] + (ext[c] - (own[c] + add[8 * c:8 * c + 8, :])) / mass for c in range(3)]
        disp = [disp[c] + vel[c] for c in range(3)]
        return disp, vel

    tiles = n // 8
    mine = me // 8

    spread = [lax.rem(yz + s, 8) for s in range(8)]
    own_half = yz // 8

    def tile_at(k):
        d = k // 4
        step = lax.rem(2 + d + (d // 2) * (2 * d - 3), 4)
        g = lax.rem(gx + 2 * step, nx)
        g = g + (1 - 2 * lax.rem(g, 2)) * (1 - lax.rem(k // 2, 2))
        half = lax.rem(yz // 8 + 1 - lax.rem(k, 2), 2)
        return g, half

    send_state()

    def fwd(g, y):
        return pltpu.make_async_remote_copy(
            src_ref=s_ref.at[g * ny + y], dst_ref=recv.at[me], send_sem=fs_sem, recv_sem=fr_sem.at[mine],
            device_id=(g, y), device_id_type=MESH)

    def fwd_start(k, _):
        g, half = tile_at(k)
        for s in range(8):
            fwd(g, half * 8 + spread[s]).start()
        return 0
    lax.fori_loop(0, tiles - 1, fwd_start, 0)
    for s in range(1, 8):
        fwd(gx, own_half * 8 + spread[s]).start()
    recv[me] = s_ref[me]
    for dst in (con_lo, con_hi):
        dst[16:24, :] = jnp.zeros((8, 256), jnp.int32)
    con_lo[0:20, :] = con_ref[...] & 127
    con_hi[0:20, :] = con_ref[...] >> 7
    for a in range(20):
        for e in range(2):
            row = jnp.broadcast_to(con_lo[a:a + 1, 128 * e:128 * e + 128], (128, 128))
            oh_e[a * 256 + 128 * e:a * 256 + 128 * e + 128, :] = jnp.where(row == sub128, F32(1), F32(0)).T.astype(BF16)
    for r in range(2):
        row = jnp.broadcast_to(halo_ref[r:r + 1, :] & 127, (128, 128))
        oh_h[128 * r:128 * r + 128, :] = jnp.where(row == sub128, F32(1), F32(0)).T.astype(BF16)
    kcopy.wait()
    gd, gv, gm = ghost_state()
    own = internal(0, disp, gd)


    sub128h = lax.broadcasted_iota(jnp.int32, (128, 128), 0).astype(jnp.int16)

    def arrive(source, count):
        pltpu.make_async_remote_copy(
            src_ref=s_ref.at[pl.ds(0, count)], dst_ref=recv.at[pl.ds(0, count)], send_sem=fs_sem, recv_sem=fr_sem.at[source],
            device_id=(gx, yz), device_id_type=MESH).wait_recv()

    def load_of(source, acc):
        base = pl.multiple_of(source * 8, 8)
        get = lambda r: recv[pl.ds(base, 8), r, :]
        loads = []
        for c in range(3):
            t0, t1 = get(2 * c), get(2 * c + 1)
            r0, r1 = pltpu.roll(t0, 64, 1), pltpu.roll(t1, 64, 1)
            loads.append([weights[j][0] * t0 + weights[j][1] * r0 + weights[j][2] * t1 + weights[j][3] * r1 for j in range(4)])
        total = jnp.zeros((48, 128), F32)
        for j in range(4):
            idx = get(6 + j).astype(jnp.int32)
            ids[j, pl.ds(base, 8), :] = idx
            lo, hi = idx & 127, idx >> 7
            highs = [loads[c][j].astype(BF16).astype(F32) for c in range(3)]
            lows = [loads[c][j] - highs[c] for c in range(3)]
            for s in range(0, 8, 2):
                hots, vals = [], []
                for k in (s, s + 1):
                    row = jnp.broadcast_to(lo[k:k + 1, :], (128, 128)).astype(jnp.int16)
                    hots.append(jnp.where(row == sub128h, BF16(1), BF16(0)))
                    mask = jnp.broadcast_to(hi[k:k + 1, :], (8, 128)) == sub8
                    vals.append(jnp.concatenate(
                        [jnp.where(mask, jnp.broadcast_to(p[k:k + 1, :], (8, 128)), F32(0)) for p in highs + lows], axis=0).astype(BF16))
                total = total + lax.dot_general(
                    jnp.concatenate(vals, axis=1), jnp.concatenate(hots, axis=1), (((1,), (1,)), ((), ())), preferred_element_type=F32)
        return acc + total
    def gather_load(k, acc):
        sources = []
        for m in range(3):
            g, half = tile_at(3 * k + m)
            sources.append(g * 2 + half)
            arrive(sources[m], 8)
        for source in sources:
            acc = load_of(source, acc)
        return acc

    both = lax.fori_loop(0, (tiles - 1) // 3, gather_load, jnp.zeros((48, 128), F32))
    arrive(mine, 7)
    both = load_of(mine, both)
    ext = [both[8 * c:8 * c + 8] + both[24 + 8 * c:32 + 8 * c] for c in range(3)]

    for r in range(2):
        for c in range(3):
            esend[r, c:c + 1, :] = pick(r, ext[c])
        esend[r, 3:8, :] = jnp.zeros((5, 128), F32)
    start_both(load_copies)
    disp, vel = advance(0, own, ext, disp, vel)
    wait_both(load_copies)
    ge = [jnp.where(exists[k], erecv[k, 0:3, :], F32(0)) for k in range(2)]
    advance_ghosts(0, ge, gd, gv, gm)
    for step in range(1, SUBSTEPS):
        own = internal(step, disp, gd)
        disp, vel = advance(step, own, ext, disp, vel)
        if step < SUBSTEPS - 1:
            advance_ghosts(step, ge, gd, gv, gm)
    for c in range(3):
        for h in range(8):
            at_row = 32 + 8 * c + h
            ret_ref[n + at_row // 6, at_row % 6:at_row % 6 + 1, :] = disp[c][h:h + 1, :]
            u_s[c, h:h + 1, 0:128] = disp[c][h:h + 1, :]
    for r in range(32):
        ret_ref[n + r // 6, r % 6:r % 6 + 1, :] = slot_s[:, 128 * r:128 * r + 128].astype(F32)

    def ret(g, y):
        return pltpu.make_async_remote_copy(
            src_ref=outb.at[g * ny + y], dst_ref=ret_ref.at[me], send_sem=rs_sem, recv_sem=rr_sem,
            device_id=(g, y), device_id_type=MESH)

    def back(k, _):
        pair = [tile_at(2 * k + m) for m in range(2)]
        for g, half in pair:
            base = pl.multiple_of((g * 2 + half) * 8, 8)
            sums = [[jnp.zeros((8, 128), F32)] * 4 for c in range(3)]
            for j in range(4):
                idx = ids[j, pl.ds(base, 8), :]
                lo, hi = idx & 127, idx >> 7
                masks = [hi == h for h in range(1, 8)]
                for c in range(3):
                    acc = lane_take(jnp.broadcast_to(u_s[c, 0:1, 0:128], (8, 128)), lo)
                    for h in range(1, 8):
                        acc = jnp.where(masks[h - 1], lane_take(jnp.broadcast_to(u_s[c, h:h + 1, 0:128], (8, 128)), lo), acc)
                    sums[c] = [sums[c][m] + weights[j][m] * acc for m in range(4)]
            for c in range(3):
                p0, q0, p1, q1 = sums[c]
                outb[pl.ds(base, 8), 2 * c, :] = p0 + pltpu.roll(q0, 64, 1)
                outb[pl.ds(base, 8), 2 * c + 1, :] = p1 + pltpu.roll(q1, 64, 1)
        for g, half in pair:
            for s in range(8):
                y = half * 8 + lax.rem(yz + s, 8)

                @pl.when(g * ny + y != me)
                def _():
                    ret(g, y).start()
        return 0
    lax.fori_loop(0, tiles // 2, back, 0)
    ret_ref[me] = outb[me]

    def every(src, dst, ss, rs):
        return pltpu.make_async_remote_copy(
            src_ref=src.at[pl.ds(0, n - 1)], dst_ref=dst.at[pl.ds(0, n - 1)], send_sem=ss, recv_sem=rs,
            device_id=(gx, yz), device_id_type=MESH)
    every(s_ref, recv, fs_sem, fr_sem.at[0]).wait_send()
    last = every(outb, ret_ref, rs_sem, rr_sem)
    last.wait_send()
    last.wait_recv()


def solid(face_block, pressure, local, weight, area, nodes, target, stiffness, connect, halo, mass, disp, vel, nx, ny, shapes):
    n = nx * ny
    V = pl.BlockSpec(memory_space=pltpu.VMEM)
    A = pl.BlockSpec(memory_space=pl.ANY)
    D = pltpu.SemaphoreType.DMA
    M = pltpu.VMEM
    I32 = jnp.int32
    back = pl.pallas_call(
        functools.partial(solid_kernel, nx, ny, shapes),
        out_shape=jax.ShapeDtypeStruct((n + 10, 6, 128), F32),
        in_specs=[pl.BlockSpec(memory_space=pltpu.SMEM), A, A, A, A, A, V, A, V, V, V, V, V],
        out_specs=V,
        scratch_shapes=[
            M(pressure.shape, BF16), M(local.shape, I32), M(weight.shape, F32), M(area.shape, F32), M(nodes.shape, I32),
            M(area.shape, F32), M((16 * STRIDE, 128), F32), M((256, 32, 128), BF16), M((1024, 128), I32), M((1024, 128), F32),
            M((1024, 128), F32), M(target.shape, I32), M((128, 256), F32), M((640, 256), F32),
            M((n, 10, 128), F32),
            M((n, 10, 128), F32), M((n, 6, 128), F32), M((60, 60, 256), F32),
            M((4, n, 128), I32), M((24, 256), I32), M((24, 256), I32),
            M((3, 24, 256), F32), M((60, 256), F32), M((60, 256), F32),
            M((96, 5120), BF16), M((5120, 128), BF16), M((256, 128), BF16),
            M((2, 16, 128), F32), M((2, 16, 128), F32), M((2, 8, 128), F32), M((2, 8, 128), F32),
            M((SUBSTEPS, 2, 8, 128), F32), M((SUBSTEPS, 2, 8, 128), F32), M((SUBSTEPS, 2, 8, 128), F32), M((2, 256, 128), BF16),
            D((5,)), D, D, D((n // 8,)), D, D, D((2,)), D((2,)), D((2,)), D((2,)),
            D((SUBSTEPS, 2)), D((SUBSTEPS, 2)), D((SUBSTEPS, 2)), D((SUBSTEPS, 2))],
        compiler_params=pltpu.CompilerParams(collective_id=0, has_side_effects=True, vmem_limit_bytes=56 * 2**20),
        name="solid",
    )(face_block, pressure, local, weight, area, nodes, target, stiffness, connect, halo, mass.reshape(1, -1), disp, vel)
    return pl.pallas_call(
        functools.partial(unpack_kernel, n),
        out_shape=(jax.ShapeDtypeStruct(disp.shape, F32), jax.ShapeDtypeStruct((12, target.shape[1]), F32)),
        in_specs=[V, V],
        out_specs=(V, V),
        scratch_shapes=[M(target.shape, I32), M((768, 256), BF16)],
        compiler_params=pltpu.CompilerParams(vmem_limit_bytes=24 * 2**20),
        name="unpack",
    )(target, back)


def shape_table():
    corner_u = [-1, 1, 1, -1, 0, 1, 0, -1]
    corner_v = [-1, -1, 1, 1, -1, 0, 1, 0]
    gauss_point = 1.0 / math.sqrt(3.0)
    points = [
        (-gauss_point, -gauss_point),
        (gauss_point, -gauss_point),
        (gauss_point, gauss_point),
        (-gauss_point, gauss_point),
    ]
    shape_values = np.zeros((4, 8), np.float32)
    for position, (coord_u, coord_v) in enumerate(points):
        for corner in range(8):
            node_u = corner_u[corner]
            node_v = corner_v[corner]
            if corner < 4:
                entry_value = (
                    0.25
                    * (1 + coord_u * node_u)
                    * (1 + coord_v * node_v)
                    * (coord_u * node_u + coord_v * node_v - 1)
                )
            elif node_u == 0:
                entry_value = 0.5 * (1 - coord_u * coord_u) * (1 + coord_v * node_v)
            else:
                entry_value = 0.5 * (1 + coord_u * node_u) * (1 - coord_v * coord_v)
            shape_values[position, corner] = entry_value
    return shape_values


def shards(
    pressure,
    face_block,
    stencil_local,
    stencil_weight,
    area_normal,
    face_part,
    face_nodes,
    stiffness,
    connect,
    halo_nodes,
    node_mass,
    displacement,
    velocity,
):
    gx_size = lax.axis_size("gx")
    yz_size = lax.axis_size("yz")
    return solid(
        face_block, pressure, stencil_local, stencil_weight, area_normal, face_nodes, face_part.reshape(1, -1),
        stiffness, connect, halo_nodes, node_mass, displacement, velocity, gx_size, yz_size, shape_table()
    )


def solution(mesh):
    in_specs = (
        P(("gx", "yz"), None),
        P(("gx", "yz")),
        P(None, ("gx", "yz")),
        P(None, ("gx", "yz")),
        P(None, ("gx", "yz")),
        P(("gx", "yz"), None),
        P(None, ("gx", "yz")),
        P(None, None, ("gx", "yz")),
        P(None, ("gx", "yz")),
        P(None, ("gx", "yz")),
        P(("gx", "yz")),
        P(None, ("gx", "yz")),
        P(None, ("gx", "yz")),
    )
    out_specs = (P(None, ("gx", "yz")), P(None, ("gx", "yz")))
    return jax.shard_map(shards, mesh=mesh, in_specs=in_specs, out_specs=out_specs, check_vma=False)
```
